16 devices in a mesh: cp: 4 (over z, y), fsdp: 4 (over x, core).
Axes of the slice: x: 2, y: 2, z: 2, core: 2. Of those that a mesh axis runs over, the one named last changes fastest.
Arguments:
- x_in: bfloat16 [16, 2048, 1152], P('fsdp', 'cp')
- grad_out: bfloat16 [16, 2048, 1152], P('fsdp', 'cp')
- seg_id: int32 [16, 2048], P('fsdp', 'cp')
- seg_pos: int32 [16, 2048], P('fsdp', 'cp')
- norm_scale: float32 [1152], P(('cp', 'fsdp'))
- w_q: float32 [1152, 1024], P(('cp', 'fsdp'))
- w_k: float32 [1152, 256], P(('cp', 'fsdp'))
- w_v: float32 [1152, 256], P(('cp', 'fsdp'))
- w_o: float32 [1024, 1152], P(('cp', 'fsdp'))
- b_o: float32 [1152], P(('cp', 'fsdp'))
- w_up1: float32 [1152, 6912], P(('cp', 'fsdp'))
- b_up1: float32 [6912], P(('cp', 'fsdp'))
- w_up2: float32 [1152, 6912], P(('cp', 'fsdp'))
- b_up2: float32 [6912], P(('cp', 'fsdp'))
- w_down: float32 [6912, 1152], P(('cp', 'fsdp'))
- b_down: float32 [1152], P(('cp', 'fsdp'))
Outputs:
- output 1: bfloat16 [16, 2048, 1152], P('fsdp', 'cp')
- output 2: bfloat16 [16, 2048, 1152], P('fsdp', 'cp')
- output 3: float32 [1152], P(('cp', 'fsdp'))
- output 4: float32 [1152, 1024], P(('cp', 'fsdp'))
- output 5: float32 [1152, 256], P(('cp', 'fsdp'))
- output 6: float32 [1152, 256], P(('cp', 'fsdp'))
- output 7: float32 [1024, 1152], P(('cp', 'fsdp'))
- output 8: float32 [1152], P(('cp', 'fsdp'))
- output 9: float32 [1152, 6912], P(('cp', 'fsdp'))
- output 10: float32 [6912], P(('cp', 'fsdp'))
- output 11: float32 [1152, 6912], P(('cp', 'fsdp'))
- output 12: float32 [6912], P(('cp', 'fsdp'))
- output 13: float32 [6912, 1152], P(('cp', 'fsdp'))
- output 14: float32 [1152], P(('cp', 'fsdp'))
All inputs are finite; a program needn't handle non-finite values.
Results may differ from the reference program's by a relative error of at most 0.0176682.
Values are sent between devices in bfloat16 or wider.
A program may use at most 1 GiB of HBM per device.

```python
import jax
import jax.numpy as jnp
from jax import lax

BATCH_ALL = 16
SEQ_LEN = 2048
MODEL_DIM = 1152
NUM_HEADS = 4
HEAD_DIM = 256
FFN_DIM = 6912
WINDOW = 2048
ROPE_DIMS = 128
DOC_SPREAD = 1536


def normal_draw(key, shape):
    return jax.random.normal(key, shape, jnp.float32)


def setup_inputs(seed: int = 0) -> dict:
    keys = jax.random.split(jax.random.key(seed), 16)
    qk_dim = NUM_HEADS * HEAD_DIM
    x_in = normal_draw(keys[0], (BATCH_ALL, SEQ_LEN, MODEL_DIM)).astype(jnp.bfloat16)
    grad_out = normal_draw(keys[1], (BATCH_ALL, SEQ_LEN, MODEL_DIM)).astype(jnp.bfloat16)
    positions = jnp.broadcast_to(jnp.arange(SEQ_LEN, dtype=jnp.int32), (BATCH_ALL, SEQ_LEN))
    doc_starts = (jax.random.randint(keys[2], (BATCH_ALL, SEQ_LEN), 0, DOC_SPREAD) == 0) | (positions == 0)
    seg_id = jnp.cumsum(doc_starts.astype(jnp.int32), axis=1)
    seg_pos = positions - lax.cummax(jnp.where(doc_starts, positions, 0), axis=1)
    return {
        'x_in': x_in,
        'grad_out': grad_out,
        'seg_id': seg_id,
        'seg_pos': seg_pos,
        'norm_scale': 0.3 * normal_draw(keys[3], (MODEL_DIM,)),
        'w_q': normal_draw(keys[4], (MODEL_DIM, qk_dim)) * MODEL_DIM ** -0.5,
        'w_k': normal_draw(keys[5], (MODEL_DIM, HEAD_DIM)) * MODEL_DIM ** -0.5,
        'w_v': normal_draw(keys[6], (MODEL_DIM, HEAD_DIM)) * MODEL_DIM ** -0.5,
        'w_o': normal_draw(keys[7], (qk_dim, MODEL_DIM)) * (2.0 * qk_dim ** -0.5),
        'b_o': 0.3 * normal_draw(keys[8], (MODEL_DIM,)),
        'w_up1': normal_draw(keys[9], (MODEL_DIM, FFN_DIM)) * MODEL_DIM ** -0.5,
        'b_up1': 0.5 * normal_draw(keys[10], (FFN_DIM,)),
        'w_up2': normal_draw(keys[11], (MODEL_DIM, FFN_DIM)) * MODEL_DIM ** -0.5,
        'b_up2': 0.5 * normal_draw(keys[12], (FFN_DIM,)),
        'w_down': normal_draw(keys[13], (FFN_DIM, MODEL_DIM)) * FFN_DIM ** -0.5,
        'b_down': 0.3 * normal_draw(keys[14], (MODEL_DIM,)),
    }


def bf16_value(vals):
    return vals + lax.stop_gradient(vals.astype(jnp.bfloat16).astype(jnp.float32) - vals)


def rope_apply(values, rot_angle):
    half_dims = ROPE_DIMS // 2
    cos_a = jnp.cos(rot_angle)
    sin_a = jnp.sin(rot_angle)
    first_half = values[..., :half_dims]
    second_half = values[..., half_dims:ROPE_DIMS]
    return jnp.concatenate([first_half * cos_a - second_half * sin_a, second_half * cos_a + first_half * sin_a, values[..., ROPE_DIMS:]], axis=-1)


def seq_attention(q_rot, kv_all, seg_q, seg_all):
    q_rows = min(SEQ_LEN, WINDOW // 2)
    key_span = WINDOW + q_rows
    n_blocks = SEQ_LEN // q_rows
    row_ids = jnp.arange(q_rows)[:, None]
    col_ids = jnp.arange(key_span)[None, :]
    in_window = (col_ids > row_ids) & (col_ids <= row_ids + WINDOW)

    def one_block(blk_index):
        row_start = blk_index * q_rows
        q_blk = bf16_value(lax.dynamic_slice_in_dim(q_rot, row_start, q_rows, axis=0))
        kv_blk = bf16_value(lax.dynamic_slice_in_dim(kv_all, row_start, key_span, axis=0))
        segq_blk = lax.dynamic_slice_in_dim(seg_q, row_start, q_rows, axis=0)
        segk_blk = lax.dynamic_slice_in_dim(seg_all, row_start, key_span, axis=0)
        key_pos = row_start - WINDOW + jnp.arange(key_span)
        allowed = in_window & (key_pos >= 0)[None, :] & (segq_blk[:, None] == segk_blk[None, :])
        scores = jnp.einsum('rhd,jd->hrj', q_blk, kv_blk[:, :HEAD_DIM]) * (HEAD_DIM ** -0.5)
        scores = jnp.where(allowed[None], scores, -1e30)
        scores = scores - lax.stop_gradient(jnp.max(scores, axis=-1, keepdims=True))
        exp_scores = jnp.exp(scores)
        prob_vals = bf16_value(exp_scores / jnp.sum(exp_scores, axis=-1, keepdims=True))
        return jnp.einsum('hrj,jd->rhd', prob_vals, kv_blk[:, HEAD_DIM:])

    blk_out = lax.map(jax.checkpoint(one_block), jnp.arange(n_blocks))
    return blk_out.reshape(SEQ_LEN, NUM_HEADS, HEAD_DIM)


def layer_forward(x_f, seg_id, seg_pos, weight_set):
    scale_v, wq_v, wk_v, wv_v, wo_v, bo_v, w1_v, b1_v, w2_v, b2_v, wd_v, bd_v = [bf16_value(weight_arr) for weight_arr in weight_set]
    inv_rms = lax.rsqrt(jnp.mean(x_f * x_f, axis=-1, keepdims=True) + 1e-6)
    normed = bf16_value(x_f * inv_rms * (1.0 + scale_v))
    q_lin = jnp.einsum('btd,de->bte', normed, wq_v).reshape(BATCH_ALL, SEQ_LEN, NUM_HEADS, HEAD_DIM)
    k_lin = jnp.einsum('btd,de->bte', normed, wk_v)
    v_lin = jnp.einsum('btd,de->bte', normed, wv_v)
    half_dims = ROPE_DIMS // 2
    inv_freq = 10000.0 ** (-jnp.arange(half_dims, dtype=jnp.float32) / half_dims)
    rot_angle = seg_pos.astype(jnp.float32)[..., None] * inv_freq
    q_rot = rope_apply(q_lin, rot_angle[:, :, None, :])
    kv_local = jnp.concatenate([rope_apply(k_lin, rot_angle), v_lin], axis=-1)
    kv_all = jnp.pad(kv_local, ((0, 0), (WINDOW, 0), (0, 0)))
    seg_all = jnp.pad(seg_id, ((0, 0), (WINDOW, 0)))

    def seq_item(seq_args):
        return seq_attention(seq_args[0], seq_args[1], seq_args[2], seq_args[3])

    attn_o = bf16_value(lax.map(seq_item, (q_rot, kv_all, seg_id, seg_all))).reshape(BATCH_ALL, SEQ_LEN, NUM_HEADS * HEAD_DIM)
    attn_out = jnp.einsum('bte,ed->btd', attn_o, wo_v) + bo_v
    h_one = jnp.einsum('btd,df->btf', normed, w1_v) + b1_v
    h_two = jnp.einsum('btd,df->btf', normed, w2_v) + b2_v
    act_vals = bf16_value(jax.nn.gelu(h_one, approximate=True) * h_two)
    mlp_out = jnp.einsum('btf,fd->btd', act_vals, wd_v) + bd_v
    return x_f + attn_out + mlp_out


def reference(x_in, grad_out, seg_id, seg_pos, norm_scale, w_q, w_k, w_v, w_o, b_o, w_up1, b_up1, w_up2, b_up2, w_down, b_down):
    weight_set = (norm_scale, w_q, w_k, w_v, w_o, b_o, w_up1, b_up1, w_up2, b_up2, w_down, b_down)

    def forward(x_f, weights_in):
        return layer_forward(x_f, seg_id, seg_pos, weights_in)

    out_f, pullback = jax.vjp(forward, x_in.astype(jnp.float32), weight_set)
    d_xf, d_set = pullback(grad_out.astype(jnp.float32))
    return (out_f.astype(jnp.bfloat16), d_xf.astype(jnp.bfloat16), d_set[0], d_set[1], d_set[2], d_set[3], d_set[4], d_set[5], d_set[6], d_set[7], d_set[8], d_set[9], d_set[10], d_set[11])
```

```python
import functools
import jax
import jax.numpy as jnp
from jax import lax
from jax.experimental import pallas as pl
from jax.experimental.pallas import tpu as pltpu
from jax.sharding import Mesh, PartitionSpec as P

ROPE_DIMS = 128
HEAD_DIM = 256
N_HEADS = 4
MASKED = -1.6e31
EXP_SCALE = 1.4426950408889634 / 16.0
CHIPS = ('z', 'y', 'x')
ALL_AXES = ('z', 'y', 'x', 'core')
F32 = jnp.float32
BF16 = jnp.bfloat16


def dot_nn(a, b):
    return lax.dot_general(a, b, (((1,), (0,)), ((), ())), preferred_element_type=F32)


def dot_nt(a, b):
    return lax.dot_general(a, b, (((1,), (1,)), ((), ())), preferred_element_type=F32)


def dot_tn(a, b):
    return lax.dot_general(a, b, (((0,), (0,)), ((), ())), preferred_element_type=F32)


def rotate(values, cos_b, sin_b):
    return values * cos_b + pltpu.roll(values, ROPE_DIMS // 2, axis=1) * sin_b


def attn_kernel(n_ref, g_ref, wqkv_ref, wo_ref, cos_ref, sin_ref, cosk_ref, sink_ref, segq_ref, segk_ref, o_ref, dqkv_ref,
                q_s, do_s, k_s, v_s, kt_s, vt_s, mask_s, s_s, p_s, dk_s, dv_s):
    step = pl.program_id(0)
    n_blocks = pl.num_programs(0)
    rows = n_ref.shape[0]
    qk = N_HEADS * HEAD_DIM
    base = pl.multiple_of(step * rows, rows)
    cos_b = cos_ref[...]
    sin_b = sin_ref[...]
    n_blk = n_ref[...]

    @pl.when(step == 0)
    def _():
        dk_s[...] = jnp.zeros_like(dk_s)
        dv_s[...] = jnp.zeros_like(dv_s)

    for h in range(N_HEADS):
        lin = dot_nn(n_blk, wqkv_ref[:, h * HEAD_DIM:(h + 1) * HEAD_DIM])
        q_s[h, :, :ROPE_DIMS] = rotate(lin[:, :ROPE_DIMS], cos_b, sin_b).astype(BF16)
        q_s[h, :, ROPE_DIMS:] = lin[:, ROPE_DIMS:].astype(BF16)
        do_s[h] = dot_nt(g_ref[...], wo_ref[h * HEAD_DIM:(h + 1) * HEAD_DIM, :]).astype(BF16)
    k_lin = dot_nn(n_blk, wqkv_ref[:, qk:qk + HEAD_DIM])
    k_blk = jnp.concatenate([rotate(k_lin[:, :ROPE_DIMS], cos_b, sin_b), k_lin[:, ROPE_DIMS:]], axis=1)
    v_blk = dot_nn(n_blk, wqkv_ref[:, qk + HEAD_DIM:])
    k_s[pl.ds(base, rows), :] = k_blk.astype(BF16)
    v_s[pl.ds(base, rows), :] = v_blk.astype(BF16)
    kt_s[:, pl.ds(base, rows)] = k_blk.T.astype(BF16)
    vt_s[:, pl.ds(base, rows)] = v_blk.T.astype(BF16)

    def block(blk):
        n_chunk = blk + 1
        seg_q = segq_ref[:, :1]
        for c in range(n_chunk):
            same = seg_q == segk_ref[:1, c * rows:(c + 1) * rows]
            if c == blk:
                r_id = lax.broadcasted_iota(jnp.int32, (rows, rows), 0)
                c_id = lax.broadcasted_iota(jnp.int32, (rows, rows), 1)
                same = same & (c_id <= r_id)
            mask_s[:, c * rows:(c + 1) * rows] = jnp.where(same, 1.0, 0.0)

        def head(h, carry):
            q = q_s[h]
            do = do_s[h]
            m_run = None
            for c in range(n_chunk):
                sl = slice(c * rows, (c + 1) * rows)
                s = jnp.where(mask_s[:, sl] > 0.5, dot_nn(q, kt_s[:, sl]), MASKED)
                s_s[:, sl] = s
                m_c = jnp.max(s, axis=1, keepdims=True)
                m_run = m_c if m_run is None else jnp.maximum(m_run, m_c)
            l_run = None
            for c in range(n_chunk):
                sl = slice(c * rows, (c + 1) * rows)
                e = jnp.exp2((s_s[:, sl] - m_run) * EXP_SCALE)
                s_s[:, sl] = e
                l_c = jnp.sum(e, axis=1, keepdims=True)
                l_run = l_c if l_run is None else l_run + l_c
            inv = 1.0 / l_run
            for c in range(n_chunk):
                sl = slice(c * rows, (c + 1) * rows)
                p = s_s[:, sl] * inv
                s_s[:, sl] = p
                p_s[:, sl] = p.astype(BF16)
            o = dot_nn(p_s[:, :n_chunk * rows], v_s[:n_chunk * rows, :])
            delta = jnp.sum(o * do.astype(F32), axis=1, keepdims=True)
            o_ref[:, pl.ds(pl.multiple_of(h * HEAD_DIM, HEAD_DIM), HEAD_DIM)] = o.astype(BF16)
            dq = None
            for c in range(n_chunk):
                sl = slice(c * rows, (c + 1) * rows)
                ds = (s_s[:, sl] * (dot_nn(do, vt_s[:, sl]) - delta)).astype(BF16)
                dq_c = dot_nn(ds, k_s[sl, :])
                dq = dq_c if dq is None else dq + dq_c
                dk_s[sl, :] += dot_tn(ds, q)
                dv_s[sl, :] += dot_tn(p_s[:, sl], do)
            dq = dq * 0.0625
            dq = jnp.concatenate([rotate(dq[:, :ROPE_DIMS], cos_b, -sin_b), dq[:, ROPE_DIMS:]], axis=1)
            dqkv_ref[pl.ds(base, rows), pl.ds(pl.multiple_of(h * HEAD_DIM, HEAD_DIM), HEAD_DIM)] = dq.astype(BF16)
            return carry

        lax.fori_loop(0, N_HEADS, head, 0)

    for blk in range(4):
        pl.when(step == blk)(functools.partial(block, blk))

    @pl.when(step == n_blocks - 1)
    def _():
        dk = dk_s[...] * 0.0625
        dk = jnp.concatenate([rotate(dk[:, :ROPE_DIMS], cosk_ref[...], -sink_ref[...]), dk[:, ROPE_DIMS:]], axis=1)
        dqkv_ref[:, qk:qk + HEAD_DIM] = dk.astype(BF16)
        dqkv_ref[:, qk + HEAD_DIM:] = dv_s[...].astype(BF16)


def attention(n_own, g_own, wqkv, wo, cos_b, sin_b, seg_own):
    t_len, d_model = n_own.shape
    rows = t_len // 4
    qk = N_HEADS * HEAD_DIM
    segq = jnp.broadcast_to(seg_own[:, None], (t_len, 128))
    segk = jnp.broadcast_to(seg_own[None, :], (8, t_len))
    row_spec = lambda width: pl.BlockSpec((rows, width), lambda i: (i, 0))
    full = lambda a: pl.BlockSpec(a.shape, lambda i: (0,) * a.ndim)
    return pl.pallas_call(
        attn_kernel,
        grid=(4,),
        in_specs=[row_spec(d_model), row_spec(d_model), full(wqkv), full(wo), row_spec(ROPE_DIMS), row_spec(ROPE_DIMS), full(cos_b), full(sin_b), row_spec(128), full(segk)],
        out_specs=[row_spec(qk), pl.BlockSpec((t_len, qk + 2 * HEAD_DIM), lambda i: (0, 0))],
        out_shape=[jax.ShapeDtypeStruct((t_len, qk), BF16), jax.ShapeDtypeStruct((t_len, qk + 2 * HEAD_DIM), BF16)],
        scratch_shapes=[
            pltpu.VMEM((N_HEADS, rows, HEAD_DIM), BF16), pltpu.VMEM((N_HEADS, rows, HEAD_DIM), BF16),
            pltpu.VMEM((t_len, HEAD_DIM), BF16), pltpu.VMEM((t_len, HEAD_DIM), BF16),
            pltpu.VMEM((HEAD_DIM, t_len), BF16), pltpu.VMEM((HEAD_DIM, t_len), BF16),
            pltpu.VMEM((rows, t_len), F32), pltpu.VMEM((rows, t_len), F32), pltpu.VMEM((rows, t_len), BF16),
            pltpu.VMEM((t_len, HEAD_DIM), F32), pltpu.VMEM((t_len, HEAD_DIM), F32)],
        compiler_params=pltpu.CompilerParams(vmem_limit_bytes=60 * 1024 * 1024, dimension_semantics=('arbitrary',)),
        cost_estimate=pl.CostEstimate(flops=45_000_000_000, bytes_accessed=40_000_000, transcendentals=10_000_000),
        name='attn',
    )(n_own, g_own, wqkv, wo, cos_b, sin_b, cos_b, sin_b, segq, segk)


def split_kernel(w1_ref, w2_ref, keep_ref, send_ref):
    core = lax.axis_index('core')
    width = keep_ref.shape[2] // 8
    for i, w_ref in enumerate((w1_ref, w2_ref)):
        even = jnp.concatenate([w_ref[:, 2 * j * width:(2 * j + 1) * width] for j in range(8)], axis=1)
        odd = jnp.concatenate([w_ref[:, (2 * j + 1) * width:(2 * j + 2) * width] for j in range(8)], axis=1)

        even = even.astype(BF16)
        odd = odd.astype(BF16)

        @pl.when(core == 0)
        def _():
            keep_ref[i] = even
            send_ref[i] = odd

        @pl.when(core == 1)
        def _():
            keep_ref[i] = odd
            send_ref[i] = even


def split_up(w1, w2):
    rows, cols = w1.shape
    out = jax.ShapeDtypeStruct((2, rows, cols // 2), BF16)
    return pl.pallas_call(split_kernel, out_shape=[out, out], name='split_up')(w1, w2)


def join_kernel(keep_ref, recv_ref, out_ref):
    core = lax.axis_index('core')
    width = keep_ref.shape[1] // 8

    def put(even, odd):
        out_ref[...] = jnp.concatenate([part[:, j * width:(j + 1) * width] for j in range(8) for part in (even, odd)], axis=1)

    pl.when(core == 0)(lambda: put(keep_ref[...], recv_ref[...]))
    pl.when(core == 1)(lambda: put(recv_ref[...], keep_ref[...]))


def join_up(keep, recv):
    rows, cols = keep.shape
    return pl.pallas_call(join_kernel, out_shape=jax.ShapeDtypeStruct((rows, 2 * cols), F32), name='join_up')(keep, recv)


def pack_kernel(wq_ref, wk_ref, wv_ref, wo_ref, scale_ref, bo_ref, bd_ref, b1_ref, b2_ref, out_ref, side_s):
    r_o, d_model = wo_ref.shape
    side_w = side_s.shape[1]
    side_s[...] = jnp.zeros_like(side_s)
    for row, ref in enumerate((scale_ref, bo_ref, bd_ref)):
        side_s[row:row + 1, :ref.shape[1]] = ref[...]
    for row, ref in ((3, b1_ref), (5, b2_ref)):
        rest = ref.shape[1] - side_w
        side_s[row:row + 1, :] = ref[:, :side_w]
        side_s[row + 1:row + 2, :rest] = ref[:, side_w:]
    out_ref[:r_o, :d_model] = wo_ref[...].astype(BF16)
    out_ref[:r_o, d_model:] = side_s[...].astype(BF16)
    qk = wq_ref.shape[1]
    out_ref[r_o:, :qk] = wq_ref[...].astype(BF16)
    out_ref[r_o:, qk:qk + HEAD_DIM] = wk_ref[...].astype(BF16)
    out_ref[r_o:, qk + HEAD_DIM:] = wv_ref[...].astype(BF16)


def pack(w_q, w_k, w_v, w_o, *vectors):
    rows = w_o.shape[0] + w_q.shape[0]
    width = w_q.shape[1] + 2 * HEAD_DIM
    return pl.pallas_call(
        pack_kernel,
        out_shape=jax.ShapeDtypeStruct((rows, width), BF16),
        scratch_shapes=[pltpu.VMEM((w_o.shape[0], width - w_o.shape[1]), F32)],
        name='pack',
    )(w_q, w_k, w_v, w_o, *[vector[None] for vector in vectors])


def solution(mesh):
    mesh4 = Mesh(mesh.devices.reshape(2, 2, 2, 2), ALL_AXES)
    tok_spec = P(('x', 'core'), ('z', 'y'), None)
    pos_spec = P(('x', 'core'), ('z', 'y'))
    vec_spec = P(ALL_AXES)
    mat_spec = P(ALL_AXES, None)
    param_specs = (vec_spec, mat_spec, mat_spec, mat_spec, mat_spec, vec_spec, mat_spec, vec_spec, mat_spec, vec_spec, mat_spec, vec_spec)

    def swap_core(values):
        return lax.ppermute(values, 'core', [(0, 1), (1, 0)])

    def exchange(values, cp_index):
        out = jnp.zeros_like(values)
        own = lax.dynamic_index_in_dim(values, cp_index, 0, keepdims=True)
        out = lax.dynamic_update_slice_in_dim(out, own, cp_index, 0)
        for flip in (3, 1, 2):
            sent = lax.dynamic_index_in_dim(values, cp_index ^ flip, 0, keepdims=True)
            got = lax.ppermute(sent, ('z', 'y'), [(i, i ^ flip) for i in range(4)])
            out = lax.dynamic_update_slice_in_dim(out, got, cp_index ^ flip, 0)
        return out

    def local_step(x_in, grad_out, seg_id, seg_pos, norm_scale, w_q, w_k, w_v, w_o, b_o, w_up1, b_up1, w_up2, b_up2, w_down, b_down):
        n_seq, piece, d_model = x_in.shape
        t_len = n_seq * piece
        core = lax.axis_index('core')
        cp_index = lax.axis_index('z') * 2 + lax.axis_index('y')
        first = core == 0
        r_in = w_q.shape[0]
        r_o = w_o.shape[0]
        f_blk = b_up1.shape[0]
        qk = N_HEADS * HEAD_DIM

        bundle = lax.all_gather(pack(w_q, w_k, w_v, w_o, norm_scale, b_o, b_down, b_up1, b_up2), ALL_AXES, axis=0)
        wqkv = bundle[:, r_o:].reshape(16 * r_in, -1)
        wo = bundle[:, :r_o, :d_model].reshape(16 * r_o, d_model)
        vec_all = bundle[:, :8, d_model:]
        side_w = vec_all.shape[2]
        scale_f, bo_f, bd_f = [vec_all[:, i, :r_in].reshape(1, d_model).astype(F32) for i in range(3)]
        b_ups = []
        for row in (3, 5):
            both = jnp.concatenate([vec_all[:, row], vec_all[:, row + 1, :f_blk - side_w]], axis=1).reshape(8, 2, f_blk)
            b_ups.append(jnp.where(first, both[:, 0], both[:, 1]).reshape(1, 8 * f_blk).astype(F32))
        b1_f, b2_f = b_ups

        keep, send = split_up(w_up1, w_up2)
        recv = swap_core(send)
        up = jnp.where(first, jnp.stack([keep, recv], axis=1), jnp.stack([recv, keep], axis=1))
        up = up.reshape(2, 2 * r_in, 8 * f_blk)
        w1 = lax.all_gather(up[0], CHIPS, axis=0, tiled=True)
        w2 = lax.all_gather(up[1], CHIPS, axis=0, tiled=True)
        wd = lax.all_gather(w_down.astype(BF16), CHIPS, axis=0, tiled=True)

        x_own = exchange(x_in, cp_index).reshape(t_len, d_model)
        seg_all = exchange(jnp.stack([seg_id, seg_pos], axis=1), cp_index)
        g_own = exchange(grad_out, cp_index).reshape(t_len, d_model)
        seg_own = seg_all[:, 0].reshape(t_len)
        pos_own = seg_all[:, 1].reshape(t_len)
        x_pair = jnp.stack([x_own, swap_core(x_own)])
        g_pair = jnp.concatenate([g_own, swap_core(g_own)])
        x_f = x_pair.astype(F32)
        inv_rms = lax.rsqrt(jnp.mean(x_f * x_f, axis=-1, keepdims=True) + 1e-6)
        n_pair = (x_f * inv_rms * (1.0 + scale_f)).astype(BF16)
        n_own = n_pair[0]
        n_pair = n_pair.reshape(2 * t_len, d_model)

        half = ROPE_DIMS // 2
        inv_freq = 10000.0 ** (-jnp.arange(half, dtype=F32) / half)
        angle = pos_own.astype(F32)[:, None] * inv_freq
        cos_a = jnp.cos(angle)
        sin_a = jnp.sin(angle)
        cos_b = jnp.concatenate([cos_a, cos_a], axis=1)
        sin_b = jnp.concatenate([-sin_a, sin_a], axis=1)

        o_own, dqkv = attention(n_own, g_own, wqkv, wo, cos_b, sin_b, seg_own)
        d_wqkv = dot_tn(n_own, dqkv)
        d_wo = dot_tn(o_own, g_own)
        g_wqkv = lax.psum_scatter(d_wqkv, ALL_AXES, scatter_dimension=0, tiled=True)
        g_wo = lax.psum_scatter(d_wo, ALL_AXES, scatter_dimension=0, tiled=True)

        h_one = dot_nn(n_pair, w1) + b1_f
        h_two = dot_nn(n_pair, w2) + b2_f
        act_f, act_back = jax.vjp(lambda a, b: jax.nn.gelu(a, approximate=True) * b, h_one, h_two)
        act = act_f.astype(BF16)
        d_h1, d_h2 = act_back(dot_nt(g_pair, wd))
        dh1 = d_h1.astype(BF16)
        dh2 = d_h2.astype(BF16)
        d_wd = dot_tn(act, g_pair)
        g_wd = lax.psum_scatter(d_wd, CHIPS, scatter_dimension=0, tiled=True)
        d_w1 = dot_tn(n_pair, dh1)
        half_w1 = lax.psum_scatter(d_w1, CHIPS, scatter_dimension=0, tiled=True)
        d_w2 = dot_tn(n_pair, dh2)
        half_w2 = lax.psum_scatter(d_w2, CHIPS, scatter_dimension=0, tiled=True)

        mlp_other = swap_core(dot_nn(act[t_len:], wd))
        x_sum = x_pair[0].astype(F32) + dot_nn(o_own, wo) + bo_f + dot_nn(act[:t_len], wd) + mlp_other + bd_f
        x_out = exchange(x_sum.astype(BF16).reshape(n_seq, piece, d_model), cp_index)

        dn_other = swap_core(dot_nt(dh1[t_len:], w1) + dot_nt(dh2[t_len:], w2))
        d_normed = dot_nt(dh1[:t_len], w1) + dot_nt(dh2[:t_len], w2) + dn_other + dot_nt(dqkv, wqkv)
        xo_f = x_own.astype(F32)
        inv_own = inv_rms[0]
        scaled = d_normed * (1.0 + scale_f)
        proj = jnp.mean(scaled * xo_f, axis=-1, keepdims=True)
        d_xf = inv_own * scaled - xo_f * (inv_own * inv_own * inv_own * proj)
        d_scale = jnp.sum(d_normed * xo_f * inv_own, axis=0)
        d_x = exchange((g_own.astype(F32) + d_xf).astype(BF16).reshape(n_seq, piece, d_model), cp_index)

        d_bias = jnp.sum(g_own.astype(F32), axis=0)
        db = jnp.stack([jnp.sum(d_h1, axis=0), jnp.sum(d_h2, axis=0)]).reshape(2, 8, f_blk)
        zero = jnp.zeros_like(db)
        db = jnp.where(first, jnp.stack([db, zero], axis=2), jnp.stack([zero, db], axis=2)).reshape(2, 16, f_blk)
        small = jnp.concatenate([d_scale.reshape(16, r_in), d_bias.reshape(16, r_in), db[0], db[1]], axis=1)
        small = lax.psum_scatter(small, ALL_AXES, scatter_dimension=0, tiled=True)[0]
        g_scale, g_bias, g_b1, g_b2 = small[:r_in], small[r_in:2 * r_in], small[2 * r_in:2 * r_in + f_blk], small[2 * r_in + f_blk:]

        ups = []
        for half_w in (half_w1, half_w2):
            mine = jnp.where(first, half_w[:r_in], half_w[r_in:])
            other = jnp.where(first, half_w[r_in:], half_w[:r_in])
            ups.append(join_up(mine, swap_core(other)))
        g_wq, g_wk, g_wv = g_wqkv[:, :qk], g_wqkv[:, qk:qk + HEAD_DIM], g_wqkv[:, qk + HEAD_DIM:]
        return (x_out, d_x, g_scale, g_wq, g_wk, g_wv, g_wo, g_bias, ups[0], g_b1, ups[1], g_b2, g_wd, g_bias)

    in_specs = (tok_spec, tok_spec, pos_spec, pos_spec) + param_specs
    out_specs = (tok_spec, tok_spec) + param_specs
    return jax.shard_map(local_step, mesh=mesh4, in_specs=in_specs, out_specs=out_specs, check_vma=False)
```

```python
import functools
import jax
import jax.numpy as jnp
from jax import lax
from jax.experimental import pallas as pl
from jax.experimental.pallas import tpu as pltpu
from jax.sharding import Mesh, PartitionSpec as P

ROPE_DIMS = 128
HEAD_DIM = 256
N_HEADS = 4
MASKED = -1.6e31
EXP_SCALE = 1.4426950408889634 / 16.0
CHIPS = ('z', 'y', 'x')
ALL_AXES = ('z', 'y', 'x', 'core')
F32 = jnp.float32
BF16 = jnp.bfloat16


def dot_nn(a, b):
    return lax.dot_general(a, b, (((1,), (0,)), ((), ())), preferred_element_type=F32)


def dot_nt(a, b):
    return lax.dot_general(a, b, (((1,), (1,)), ((), ())), preferred_element_type=F32)


def dot_tn(a, b):
    return lax.dot_general(a, b, (((0,), (0,)), ((), ())), preferred_element_type=F32)


def rotate(values, cos_b, sin_b):
    return values * cos_b + pltpu.roll(values, ROPE_DIMS // 2, axis=1) * sin_b


def attn_kernel(n_ref, g_ref, wqkv_ref, wo_ref, cos_ref, sin_ref, cosk_ref, sink_ref, segq_ref, segk_ref, o_ref, dqkv_ref,
                q_s, do_s, k_s, v_s, kt_s, vt_s, mask_s, s_s, p_s, dk_s, dv_s):
    step = pl.program_id(0)
    n_blocks = pl.num_programs(0)
    rows = n_ref.shape[0]
    qk = N_HEADS * HEAD_DIM
    base = pl.multiple_of(step * rows, rows)
    cos_b = cos_ref[...]
    sin_b = sin_ref[...]
    n_blk = n_ref[...]

    @pl.when(step == 0)
    def _():
        dk_s[...] = jnp.zeros_like(dk_s)
        dv_s[...] = jnp.zeros_like(dv_s)

    for h in range(N_HEADS):
        lin = dot_nn(n_blk, wqkv_ref[:, h * HEAD_DIM:(h + 1) * HEAD_DIM])
        q_s[h, :, :ROPE_DIMS] = rotate(lin[:, :ROPE_DIMS], cos_b, sin_b).astype(BF16)
        q_s[h, :, ROPE_DIMS:] = lin[:, ROPE_DIMS:].astype(BF16)
        do_s[h] = dot_nt(g_ref[...], wo_ref[h * HEAD_DIM:(h + 1) * HEAD_DIM, :]).astype(BF16)
    k_lin = dot_nn(n_blk, wqkv_ref[:, qk:qk + HEAD_DIM])
    k_blk = jnp.concatenate([rotate(k_lin[:, :ROPE_DIMS], cos_b, sin_b), k_lin[:, ROPE_DIMS:]], axis=1)
    v_blk = dot_nn(n_blk, wqkv_ref[:, qk + HEAD_DIM:])
    k_s[pl.ds(base, rows), :] = k_blk.astype(BF16)
    v_s[pl.ds(base, rows), :] = v_blk.astype(BF16)
    kt_s[:, pl.ds(base, rows)] = k_blk.T.astype(BF16)
    vt_s[:, pl.ds(base, rows)] = v_blk.T.astype(BF16)

    def block(blk):
        n_chunk = blk + 1
        seg_q = segq_ref[:, :1]
        for c in range(n_chunk):
            same = seg_q == segk_ref[:1, c * rows:(c + 1) * rows]
            if c == blk:
                r_id = lax.broadcasted_iota(jnp.int32, (rows, rows), 0)
                c_id = lax.broadcasted_iota(jnp.int32, (rows, rows), 1)
                same = same & (c_id <= r_id)
            mask_s[:, c * rows:(c + 1) * rows] = jnp.where(same, 1.0, 0.0)

        def head(h, carry):
            q = q_s[h]
            do = do_s[h]
            m_run = None
            for c in range(n_chunk):
                sl = slice(c * rows, (c + 1) * rows)
                s = jnp.where(mask_s[:, sl] > 0.5, dot_nn(q, kt_s[:, sl]), MASKED)
                s_s[:, sl] = s
                m_c = jnp.max(s, axis=1, keepdims=True)
                m_run = m_c if m_run is None else jnp.maximum(m_run, m_c)
            l_run = None
            for c in range(n_chunk):
                sl = slice(c * rows, (c + 1) * rows)
                e = jnp.exp2((s_s[:, sl] - m_run) * EXP_SCALE)
                s_s[:, sl] = e
                l_c = jnp.sum(e, axis=1, keepdims=True)
                l_run = l_c if l_run is None else l_run + l_c
            inv = 1.0 / l_run
            for c in range(n_chunk):
                sl = slice(c * rows, (c + 1) * rows)
                p = s_s[:, sl] * inv
                s_s[:, sl] = p
                p_s[:, sl] = p.astype(BF16)
            o = dot_nn(p_s[:, :n_chunk * rows], v_s[:n_chunk * rows, :])
            delta = jnp.sum(o * do.astype(F32), axis=1, keepdims=True)
            o_ref[:, pl.ds(pl.multiple_of(h * HEAD_DIM, HEAD_DIM), HEAD_DIM)] = o.astype(BF16)
            dq = None
            for c in range(n_chunk):
                sl = slice(c * rows, (c + 1) * rows)
                ds = (s_s[:, sl] * (dot_nn(do, vt_s[:, sl]) - delta)).astype(BF16)
                dq_c = dot_nn(ds, k_s[sl, :])
                dq = dq_c if dq is None else dq + dq_c
                dk_s[sl, :] += dot_tn(ds, q)
                dv_s[sl, :] += dot_tn(p_s[:, sl], do)
            dq = dq * 0.0625
            dq = jnp.concatenate([rotate(dq[:, :ROPE_DIMS], cos_b, -sin_b), dq[:, ROPE_DIMS:]], axis=1)
            dqkv_ref[pl.ds(base, rows), pl.ds(pl.multiple_of(h * HEAD_DIM, HEAD_DIM), HEAD_DIM)] = dq.astype(BF16)
            return carry

        lax.fori_loop(0, N_HEADS, head, 0)

    for blk in range(4):
        pl.when(step == blk)(functools.partial(block, blk))

    @pl.when(step == n_blocks - 1)
    def _():
        dk = dk_s[...] * 0.0625
        dk = jnp.concatenate([rotate(dk[:, :ROPE_DIMS], cosk_ref[...], -sink_ref[...]), dk[:, ROPE_DIMS:]], axis=1)
        dqkv_ref[:, qk:qk + HEAD_DIM] = dk.astype(BF16)
        dqkv_ref[:, qk + HEAD_DIM:] = dv_s[...].astype(BF16)


def attention(n_own, g_own, wqkv, wo, cos_b, sin_b, seg_own):
    t_len, d_model = n_own.shape
    rows = t_len // 4
    qk = N_HEADS * HEAD_DIM
    segq = jnp.broadcast_to(seg_own[:, None], (t_len, 128))
    segk = jnp.broadcast_to(seg_own[None, :], (8, t_len))
    row_spec = lambda width: pl.BlockSpec((rows, width), lambda i: (i, 0))
    full = lambda a: pl.BlockSpec(a.shape, lambda i: (0,) * a.ndim)
    return pl.pallas_call(
        attn_kernel,
        grid=(4,),
        in_specs=[row_spec(d_model), row_spec(d_model), full(wqkv), full(wo), row_spec(ROPE_DIMS), row_spec(ROPE_DIMS), full(cos_b), full(sin_b), row_spec(128), full(segk)],
        out_specs=[row_spec(qk), pl.BlockSpec((t_len, qk + 2 * HEAD_DIM), lambda i: (0, 0))],
        out_shape=[jax.ShapeDtypeStruct((t_len, qk), BF16), jax.ShapeDtypeStruct((t_len, qk + 2 * HEAD_DIM), BF16)],
        scratch_shapes=[
            pltpu.VMEM((N_HEADS, rows, HEAD_DIM), BF16), pltpu.VMEM((N_HEADS, rows, HEAD_DIM), BF16),
            pltpu.VMEM((t_len, HEAD_DIM), BF16), pltpu.VMEM((t_len, HEAD_DIM), BF16),
            pltpu.VMEM((HEAD_DIM, t_len), BF16), pltpu.VMEM((HEAD_DIM, t_len), BF16),
            pltpu.VMEM((rows, t_len), F32), pltpu.VMEM((rows, t_len), F32), pltpu.VMEM((rows, t_len), BF16),
            pltpu.VMEM((t_len, HEAD_DIM), F32), pltpu.VMEM((t_len, HEAD_DIM), F32)],
        compiler_params=pltpu.CompilerParams(vmem_limit_bytes=60 * 1024 * 1024, dimension_semantics=('arbitrary',)),
        cost_estimate=pl.CostEstimate(flops=45_000_000_000, bytes_accessed=40_000_000, transcendentals=10_000_000),
        name='attn',
    )(n_own, g_own, wqkv, wo, cos_b, sin_b, cos_b, sin_b, segq, segk)


def order_x_kernel(x_ref, a_ref, b_ref, c_ref, scale_ref, out_ref, n_ref):
    cp = lax.axis_index('z') * 2 + lax.axis_index('y')
    rows = a_ref.shape[1]
    for flip, ref in enumerate((x_ref.at[cp], a_ref.at[0], b_ref.at[0], c_ref.at[0])):
        base = pl.multiple_of((cp ^ flip) * rows, rows)
        for part in range(0, rows, 128):
            x_blk = ref[part:part + 128, :]
            x_f = x_blk.astype(F32)
            inv = lax.rsqrt(jnp.mean(x_f * x_f, axis=1, keepdims=True) + 1e-6)
            out_ref[pl.ds(base + part, 128), :] = x_blk
            n_ref[pl.ds(base + part, 128), :] = (x_f * inv * (1.0 + scale_ref[...])).astype(BF16)


def order_x(x_in, got, scale_f):
    n_seq, rows, d_model = x_in.shape
    out = jax.ShapeDtypeStruct((n_seq * rows, d_model), BF16)
    return pl.pallas_call(
        order_x_kernel, out_shape=[out, out], name='order_x',
        compiler_params=pltpu.CompilerParams(vmem_limit_bytes=40 * 1024 * 1024),
        cost_estimate=pl.CostEstimate(flops=3_000_000_000, bytes_accessed=15_000_000, transcendentals=2048),
    )(x_in, *got, scale_f)


def order_kernel(x_ref, a_ref, b_ref, c_ref, out_ref):
    cp = lax.axis_index('z') * 2 + lax.axis_index('y')
    rows = a_ref.shape[1]
    for flip, ref in enumerate((x_ref.at[cp], a_ref.at[0], b_ref.at[0], c_ref.at[0])):
        out_ref[pl.ds(pl.multiple_of((cp ^ flip) * rows, rows), rows), :] = ref[...]


def order(values, got):
    n_seq, rows, width = values.shape
    return pl.pallas_call(
        order_kernel, out_shape=jax.ShapeDtypeStruct((n_seq * rows, width), values.dtype), name='order',
        compiler_params=pltpu.CompilerParams(vmem_limit_bytes=40 * 1024 * 1024),
        cost_estimate=pl.CostEstimate(flops=2_000_000_000, bytes_accessed=10_000_000, transcendentals=0),
    )(values, *got)


N_PART = 3


def split_kernel(w1_ref, w2_ref, keep_ref, send_ref):
    core = lax.axis_index('core')
    d_model = keep_ref.shape[2] // 2
    sub = d_model // 8
    for part in range(N_PART):
        for i, w_ref in enumerate((w1_ref, w2_ref)):
            even, odd = [
                jnp.concatenate([w_ref[:, ((2 * j + k) * N_PART + part) * sub:((2 * j + k) * N_PART + part + 1) * sub] for j in range(8)], axis=1).astype(BF16)
                for k in range(2)]

            @pl.when(core == 0)
            def _():
                keep_ref[part, :, i * d_model:(i + 1) * d_model] = even
                send_ref[part, :, i * d_model:(i + 1) * d_model] = odd

            @pl.when(core == 1)
            def _():
                keep_ref[part, :, i * d_model:(i + 1) * d_model] = odd
                send_ref[part, :, i * d_model:(i + 1) * d_model] = even


def split_up(w1, w2):
    rows, cols = w1.shape
    out = jax.ShapeDtypeStruct((N_PART, rows, cols // N_PART), BF16)
    return pl.pallas_call(split_kernel, out_shape=[out, out], name='split_up')(w1, w2)


def stack_kernel(keep_ref, recv_ref, wd_ref, *out_refs):
    core = lax.axis_index('core')
    rows, cols = keep_ref.shape[1:]
    for part, out_ref in enumerate(out_refs):
        own = pl.multiple_of(core * rows, 8)
        out_ref[pl.ds(own, rows), :cols] = keep_ref[part]
        out_ref[pl.ds(pl.multiple_of(rows - own, 8), rows), :cols] = recv_ref[part]
        out_ref[:, cols:] = wd_ref[part * 2 * rows:(part + 1) * 2 * rows, :].astype(BF16)


def stack_up(keep, recv, w_down):
    _, rows, cols = keep.shape
    out = jax.ShapeDtypeStruct((2 * rows, cols + w_down.shape[1]), BF16)
    return pl.pallas_call(stack_kernel, out_shape=[out] * N_PART, name='stack_up')(keep, recv, w_down)


def join_kernel(*refs):
    own_refs, recv_refs, (w1_ref, w2_ref, wd_ref) = refs[:N_PART], refs[N_PART:2 * N_PART], refs[2 * N_PART:]
    core = lax.axis_index('core')
    rows = w1_ref.shape[0]
    d_model = wd_ref.shape[1]
    sub = d_model // 8

    def put(even_of, odd_of):
        for i, w_ref in enumerate((w1_ref, w2_ref)):
            pieces = []
            for j in range(8):
                for of in (even_of, odd_of):
                    for part in range(N_PART):
                        pieces.append(of(part)[:, i * d_model + j * sub:i * d_model + (j + 1) * sub])
            w_ref[...] = jnp.concatenate(pieces, axis=1)

    pl.when(core == 0)(lambda: put(lambda p: own_refs[p][:rows, :2 * d_model], lambda p: recv_refs[p][...]))
    pl.when(core == 1)(lambda: put(lambda p: recv_refs[p][...], lambda p: own_refs[p][rows:, :2 * d_model]))
    for part in range(N_PART):
        wd_ref[part * 2 * rows:(part + 1) * 2 * rows, :] = own_refs[part][:, 2 * d_model:]


def join_up(owns, recvs):
    rows, cols = recvs[0].shape
    d_model = cols // 2
    up = jax.ShapeDtypeStruct((rows, N_PART * cols), F32)
    return pl.pallas_call(
        join_kernel, out_shape=[up, up, jax.ShapeDtypeStruct((N_PART * 2 * rows, d_model), F32)], name='join_up',
    )(*owns, *recvs)


GELU_C = 0.7978845608028654
GELU_A = 0.044715


def hidden_kernel(n_own_ref, n_oth_ref, g_own_ref, g_oth_ref, w_ref, b1_ref, b2_ref, act_ref, dh_ref, dw_ref, db_ref,
                  h_s, da_s, n_s, g_s, acc_s, sem):
    step = pl.program_id(0)
    last = pl.num_programs(0) - 1
    rows, d_model = n_s.shape
    own = step < pl.num_programs(0) // 2
    n_s[...] = jnp.where(own, n_own_ref[...], n_oth_ref[...])
    g_s[...] = jnp.where(own, g_own_ref[...], g_oth_ref[...])

    @pl.when(step == 0)
    def _():
        acc_s[...] = jnp.zeros_like(acc_s)
        db_ref[...] = jnp.zeros_like(db_ref)

    n_sub = 2
    sub = rows // n_sub
    w12 = w_ref[:, :2 * d_model]
    for i in range(n_sub):
        sl = slice(i * sub, (i + 1) * sub)
        h_s[sl, :] = dot_nn(n_s[sl, :], w12)
        da_s[sl, :] = dot_nt(g_s[sl, :], w_ref[:, 2 * d_model:])
    b1 = b1_ref[...]
    b2 = b2_ref[...]
    for i in range(n_sub):
        sl = slice(i * sub, (i + 1) * sub)
        s1 = None
        s2 = None
        for r in range(i * sub, (i + 1) * sub, 64):
            rs = slice(r, r + 64)
            u = h_s[rs, :d_model] + b1
            v = h_s[rs, d_model:] + b2
            da = da_s[rs, :]
            u2 = u * u
            t = jnp.tanh(u * (GELU_C + (GELU_C * GELU_A) * u2))
            half = 0.5 + 0.5 * t
            gelu = u * half
            slope = half + (half * (1.0 - t)) * (u * (GELU_C + (3.0 * GELU_C * GELU_A) * u2))
            d1 = da * v * slope
            d2 = da * gelu
            act_ref[rs, :] = (gelu * v).astype(BF16)
            dh_ref[rs, :d_model] = d1.astype(BF16)
            dh_ref[rs, d_model:] = d2.astype(BF16)
            p1 = jnp.sum(d1.reshape(8, 8, d_model), axis=0)
            p2 = jnp.sum(d2.reshape(8, 8, d_model), axis=0)
            s1 = p1 if s1 is None else s1 + p1
            s2 = p2 if s2 is None else s2 + p2
        db_ref[:8, :] += s1
        db_ref[8:, :] += s2
        acc_s[:, :2 * d_model] += dot_tn(n_s[sl, :], dh_ref[sl, :])
        acc_s[:, 2 * d_model:] += dot_tn(act_ref[sl, :], g_s[sl, :])

    @pl.when(step == last)
    def _():
        copy = pltpu.make_async_copy(acc_s, dw_ref, sem)
        copy.start()
        copy.wait()


def hidden_part(n_own, n_oth, g_own, g_oth, w_part, b1, b2):
    t_len, d_model = n_own.shape
    rows = 512
    steps = 2 * t_len // rows
    half = steps // 2
    own_spec = pl.BlockSpec((rows, d_model), lambda i: (jnp.minimum(i, half - 1), 0))
    oth_spec = pl.BlockSpec((rows, d_model), lambda i: (jnp.maximum(i - half, 0), 0))
    full = lambda a: pl.BlockSpec(a.shape, lambda i: (0, 0), pipeline_mode=pl.Buffered(1))
    row = lambda width: pl.BlockSpec((rows, width), lambda i: (i, 0))
    return pl.pallas_call(
        hidden_kernel,
        grid=(steps,),
        in_specs=[own_spec, oth_spec, own_spec, oth_spec, full(w_part), full(b1), full(b2)],
        out_specs=[row(d_model), row(2 * d_model), pl.BlockSpec(memory_space=pl.ANY), pl.BlockSpec((16, d_model), lambda i: (0, 0))],
        out_shape=[jax.ShapeDtypeStruct((2 * t_len, d_model), BF16), jax.ShapeDtypeStruct((2 * t_len, 2 * d_model), BF16),
                   jax.ShapeDtypeStruct(w_part.shape, F32), jax.ShapeDtypeStruct((16, d_model), F32)],
        scratch_shapes=[pltpu.VMEM((rows, 2 * d_model), F32), pltpu.VMEM((rows, d_model), F32), pltpu.VMEM((rows, d_model), BF16),
                        pltpu.VMEM((rows, d_model), BF16), pltpu.VMEM(w_part.shape, F32), pltpu.SemaphoreType.DMA],
        compiler_params=pltpu.CompilerParams(vmem_limit_bytes=63 * 1024 * 1024, dimension_semantics=('arbitrary',)),
        cost_estimate=pl.CostEstimate(flops=65_000_000_000, bytes_accessed=70_000_000, transcendentals=4_700_000),
        name='hidden',
    )(n_own, n_oth, g_own, g_oth, w_part, b1, b2)


def attn_grad_kernel(n_ref, dqkv_ref, o_ref, g_ref, out_ref):
    step = pl.program_id(0)
    r_o, r_in = o_ref.shape[1] // 16, n_ref.shape[1] // 16
    d_wqkv = dot_tn(n_ref[...], dqkv_ref[...])
    width = dqkv_ref.shape[1]
    for dev in range(16):
        out_ref[dev, r_o:, :] = d_wqkv[dev * r_in:(dev + 1) * r_in]

    def low(cols, used):
        d_wo = dot_tn(o_ref[...], g_ref[:, cols:cols + used])
        for dev in range(16):
            out_ref[dev, :r_o, :used] = d_wo[dev * r_o:(dev + 1) * r_o]
            if used < width:
                out_ref[dev, :r_o, used:] = jnp.zeros((r_o, width - used), F32)

    d_model = g_ref.shape[1]
    for i in range(-(-d_model // width)):
        pl.when(step == i)(functools.partial(low, i * width, min(width, d_model - i * width)))


def attn_grad(n_own, dqkv, o_own, g_own):
    t_len, d_model = n_own.shape
    width = 512
    total = dqkv.shape[1]
    full = lambda a: pl.BlockSpec(a.shape, lambda i: (0, 0), pipeline_mode=pl.Buffered(1))
    rows = (d_model + o_own.shape[1]) // 16
    return pl.pallas_call(
        attn_grad_kernel,
        grid=(total // width,),
        in_specs=[full(n_own), pl.BlockSpec((t_len, width), lambda i: (0, i)), full(o_own), full(g_own)],
        out_specs=pl.BlockSpec((16, rows, width), lambda i: (0, 0, i)),
        out_shape=jax.ShapeDtypeStruct((16, rows, total), F32),
        compiler_params=pltpu.CompilerParams(vmem_limit_bytes=60 * 1024 * 1024, dimension_semantics=('arbitrary',)),
        cost_estimate=pl.CostEstimate(flops=12_000_000_000, bytes_accessed=33_000_000, transcendentals=0),
        name='attn_grad',
    )(n_own, dqkv, o_own, g_own)


def out_products(act_refs, dh_refs, w_refs):
    d_model = act_refs[0].shape[1]
    out = None
    d_n = None
    for act_ref, dh_ref, w_ref in zip(act_refs, dh_refs, w_refs):
        o_part = dot_nn(act_ref[...], w_ref[:, 2 * d_model:])
        n_part = dot_nt(dh_ref[...], w_ref[:, :2 * d_model])
        out = o_part if out is None else out + o_part
        d_n = n_part if d_n is None else d_n + n_part
    return out, d_n


def out_other_kernel(*refs):
    out, d_n = out_products(refs[:3], refs[3:6], refs[6:9])
    refs[9][...] = out
    refs[10][...] = d_n


def out_specs_of(rows, d_model, w_parts, first_block):
    tile = lambda width: pl.BlockSpec((rows, width), lambda i: (i + first_block, 0))
    full = pl.BlockSpec(w_parts[0].shape, lambda i: (0, 0), pipeline_mode=pl.Buffered(1))
    return [tile(d_model)] * 3 + [tile(2 * d_model)] * 3 + [full] * 3


def out_other(acts, dhs, w_parts):
    t_len, d_model = acts[0].shape[0] // 2, acts[0].shape[1]
    rows = 256
    tile = pl.BlockSpec((rows, d_model), lambda i: (i, 0))
    out = jax.ShapeDtypeStruct((t_len, d_model), F32)
    return pl.pallas_call(
        out_other_kernel,
        grid=(t_len // rows,),
        in_specs=out_specs_of(rows, d_model, w_parts, t_len // rows),
        out_specs=[tile, tile],
        out_shape=[out, out],
        compiler_params=pltpu.CompilerParams(vmem_limit_bytes=60 * 1024 * 1024, dimension_semantics=('arbitrary',)),
        cost_estimate=pl.CostEstimate(flops=49_000_000_000, bytes_accessed=86_000_000, transcendentals=0),
        name='out_other',
    )(*acts, *dhs, *w_parts)


def out_own_kernel(*refs):
    (o_ref, dqkv_ref, wo_ref, wqkv_ref, x_ref, g_ref, got_o_ref, got_n_ref, scale_ref, bias_ref, x_out_ref, d_x_ref, sums_ref) = refs[9:]
    d_model = x_ref.shape[1]

    @pl.when(pl.program_id(0) == 0)
    def _():
        sums_ref[...] = jnp.zeros_like(sums_ref)

    out, d_n = out_products(refs[:3], refs[3:6], refs[6:9])
    out = out + dot_nn(o_ref[...], wo_ref[...])
    d_n = d_n + dot_nt(dqkv_ref[...], wqkv_ref[...])
    x_f = x_ref[...].astype(F32)
    g_f = g_ref[...].astype(F32)
    x_out_ref[...] = (x_f + out + got_o_ref[...] + bias_ref[...]).astype(BF16)
    d_n = d_n + got_n_ref[...]
    inv = lax.rsqrt(jnp.mean(x_f * x_f, axis=1, keepdims=True) + 1e-6)
    scaled = d_n * (1.0 + scale_ref[...])
    xn = x_f * inv
    proj = jnp.mean(scaled * xn, axis=1, keepdims=True)
    d_x_ref[...] = (g_f + inv * (scaled - xn * proj)).astype(BF16)
    rows = x_f.shape[0]
    sums_ref[:8, :] += jnp.sum((d_n * xn).reshape(rows // 8, 8, d_model), axis=0)
    sums_ref[8:, :] += jnp.sum(g_f.reshape(rows // 8, 8, d_model), axis=0)


def out_own(acts, dhs, w_parts, o_own, dqkv, wo, wqkv, x_own, g_own, got_o, got_n, scale_f, bias_f):
    t_len, d_model = x_own.shape
    rows = 256
    tile = lambda width: pl.BlockSpec((rows, width), lambda i: (i, 0))
    full = lambda a: pl.BlockSpec(a.shape, lambda i: (0, 0), pipeline_mode=pl.Buffered(1))
    out = jax.ShapeDtypeStruct((t_len, d_model), BF16)
    return pl.pallas_call(
        out_own_kernel,
        grid=(t_len // rows,),
        in_specs=out_specs_of(rows, d_model, w_parts, 0) + [tile(o_own.shape[1]), tile(dqkv.shape[1]), full(wo), full(wqkv)]
                 + [tile(d_model)] * 4 + [full(scale_f), full(bias_f)],
        out_specs=[tile(d_model), tile(d_model), pl.BlockSpec((16, d_model), lambda i: (0, 0))],
        out_shape=[out, out, jax.ShapeDtypeStruct((16, d_model), F32)],
        compiler_params=pltpu.CompilerParams(vmem_limit_bytes=63 * 1024 * 1024, dimension_semantics=('arbitrary',)),
        cost_estimate=pl.CostEstimate(flops=61_000_000_000, bytes_accessed=125_000_000, transcendentals=0),
        name='out_own',
    )(*acts, *dhs, *w_parts, o_own, dqkv, wo, wqkv, x_own, g_own, got_o, got_n, scale_f, bias_f)


def pack_kernel(wq_ref, wk_ref, wv_ref, wo_ref, scale_ref, bo_ref, bd_ref, b1_ref, b2_ref, out_ref, side_s):
    r_o, d_model = wo_ref.shape
    side_w = side_s.shape[1]
    side_s[...] = jnp.zeros_like(side_s)
    for row, ref in enumerate((scale_ref, bo_ref, bd_ref)):
        side_s[row:row + 1, :ref.shape[1]] = ref[...]
    for row, ref in ((3, b1_ref), (5, b2_ref)):
        rest = ref.shape[1] - side_w
        side_s[row:row + 1, :] = ref[:, :side_w]
        side_s[row + 1:row + 2, :rest] = ref[:, side_w:]
    out_ref[:r_o, :d_model] = wo_ref[...].astype(BF16)
    out_ref[:r_o, d_model:] = side_s[...].astype(BF16)
    qk = wq_ref.shape[1]
    out_ref[r_o:, :qk] = wq_ref[...].astype(BF16)
    out_ref[r_o:, qk:qk + HEAD_DIM] = wk_ref[...].astype(BF16)
    out_ref[r_o:, qk + HEAD_DIM:] = wv_ref[...].astype(BF16)


def pack(w_q, w_k, w_v, w_o, *vectors):
    rows = w_o.shape[0] + w_q.shape[0]
    width = w_q.shape[1] + 2 * HEAD_DIM
    return pl.pallas_call(
        pack_kernel,
        out_shape=jax.ShapeDtypeStruct((rows, width), BF16),
        scratch_shapes=[pltpu.VMEM((w_o.shape[0], width - w_o.shape[1]), F32)],
        name='pack',
    )(w_q, w_k, w_v, w_o, *[vector[None] for vector in vectors])


def solution(mesh):
    mesh4 = Mesh(mesh.devices.reshape(2, 2, 2, 2), ALL_AXES)
    tok_spec = P(('x', 'core'), ('z', 'y'), None)
    pos_spec = P(('x', 'core'), ('z', 'y'))
    vec_spec = P(ALL_AXES)
    mat_spec = P(ALL_AXES, None)
    param_specs = (vec_spec, mat_spec, mat_spec, mat_spec, mat_spec, vec_spec, mat_spec, vec_spec, mat_spec, vec_spec, mat_spec, vec_spec)

    def swap_core(values):
        return lax.ppermute(values, 'core', [(0, 1), (1, 0)])

    def send_blocks(values, cp_index):
        got = []
        for flip in (1, 2, 3):
            sent = lax.dynamic_index_in_dim(values, cp_index ^ flip, 0, keepdims=True)
            got.append(lax.ppermute(sent, ('z', 'y'), [(i, i ^ flip) for i in range(4)]))
        return got

    def local_step(x_in, grad_out, seg_id, seg_pos, norm_scale, w_q, w_k, w_v, w_o, b_o, w_up1, b_up1, w_up2, b_up2, w_down, b_down):
        n_seq, piece, d_model = x_in.shape
        t_len = n_seq * piece
        core = lax.axis_index('core')
        cp_index = lax.axis_index('z') * 2 + lax.axis_index('y')
        first = core == 0
        r_in = w_q.shape[0]
        r_o = w_o.shape[0]
        f_blk = b_up1.shape[0]
        sub = f_blk // N_PART
        qk = N_HEADS * HEAD_DIM

        x_got = send_blocks(x_in, cp_index)
        seg_pack = jnp.stack([seg_id, seg_pos], axis=1)
        seg_got = send_blocks(seg_pack, cp_index)
        g_got = send_blocks(grad_out, cp_index)

        bundle = lax.all_gather(pack(w_q, w_k, w_v, w_o, norm_scale, b_o, b_down, b_up1, b_up2), ALL_AXES, axis=0)
        wqkv = bundle[:, r_o:].reshape(16 * r_in, -1)
        wo = bundle[:, :r_o, :d_model].reshape(16 * r_o, d_model)
        vec_all = bundle[:, :8, d_model:]
        side_w = vec_all.shape[2]
        scale_f, bo_f, bd_f = [vec_all[:, i, :r_in].reshape(1, d_model).astype(F32) for i in range(3)]
        b_ups = []
        for row in (3, 5):
            both = jnp.concatenate([vec_all[:, row], vec_all[:, row + 1, :f_blk - side_w]], axis=1).reshape(8, 2, N_PART, sub)
            mine = jnp.where(first, both[:, 0], both[:, 1]).astype(F32)
            b_ups.append([mine[:, part].reshape(1, d_model) for part in range(N_PART)])

        keep, send = split_up(w_up1, w_up2)
        shards = stack_up(keep, swap_core(send), w_down)
        w_parts = [lax.all_gather(shard, CHIPS, axis=0, tiled=True) for shard in shards]

        x_own, n_own = order_x(x_in, x_got, scale_f)
        n_oth = swap_core(n_own)
        g_own = order(grad_out, g_got)
        g_oth = swap_core(g_own)
        seg_all = jnp.zeros_like(seg_pack)
        for flip, got in enumerate([lax.dynamic_index_in_dim(seg_pack, cp_index, 0, keepdims=True)] + seg_got):
            seg_all = lax.dynamic_update_slice_in_dim(seg_all, got, cp_index ^ flip, 0)
        seg_own = seg_all[:, 0].reshape(t_len)
        pos_own = seg_all[:, 1].reshape(t_len)
        half = ROPE_DIMS // 2
        inv_freq = 10000.0 ** (-jnp.arange(half, dtype=F32) / half)
        angle = pos_own.astype(F32)[:, None] * inv_freq
        cos_a = jnp.cos(angle)
        sin_a = jnp.sin(angle)
        cos_b = jnp.concatenate([cos_a, cos_a], axis=1)
        sin_b = jnp.concatenate([-sin_a, sin_a], axis=1)

        o_own, dqkv = attention(n_own, g_own, wqkv, wo, cos_b, sin_b, seg_own)
        d_attn = attn_grad(n_own, dqkv, o_own, g_own).reshape(8, 2, r_o + r_in, -1)
        d_keep = jnp.where(first, d_attn[:, 0], d_attn[:, 1])
        d_send = jnp.where(first, d_attn[:, 1], d_attn[:, 0])
        d_pair = (d_keep + swap_core(d_send)).reshape(8 * (r_o + r_in), -1)
        g_attn = lax.psum_scatter(d_pair, CHIPS, scatter_dimension=0, tiled=True)

        acts, dhs, dbs, owns, recvs = [], [], [], [], []
        for part in range(N_PART):
            act, dh, d_w, db = hidden_part(n_own, n_oth, g_own, g_oth, w_parts[part], b_ups[0][part], b_ups[1][part])
            own = lax.psum_scatter(d_w, CHIPS, scatter_dimension=0, tiled=True)
            recvs.append(swap_core(jnp.where(first, own[r_in:, :2 * d_model], own[:r_in, :2 * d_model])))
            acts.append(act)
            dhs.append(dh)
            dbs.append(jnp.sum(db.reshape(2, 8, d_model), axis=1).reshape(2, 8, sub))
            owns.append(own)

        out_oth, dn_oth = out_other(acts, dhs, w_parts)
        got_o = swap_core(out_oth)
        got_n = swap_core(dn_oth)
        x_out, d_x, sums = out_own(acts, dhs, w_parts, o_own, dqkv, wo, wqkv, x_own, g_own, got_o, got_n, scale_f, bo_f + bd_f)
        x_blocks = x_out.reshape(n_seq, piece, d_model)
        x_out = order(x_blocks, send_blocks(x_blocks, cp_index)).reshape(n_seq, piece, d_model)
        d_blocks = d_x.reshape(n_seq, piece, d_model)
        d_x = order(d_blocks, send_blocks(d_blocks, cp_index)).reshape(n_seq, piece, d_model)

        sums = jnp.sum(sums.reshape(2, 8, d_model), axis=1).reshape(2, 16, r_in)
        db = jnp.stack(dbs, axis=2).reshape(2, 8, f_blk)
        zero = jnp.zeros_like(db)
        db = jnp.where(first, jnp.stack([db, zero], axis=2), jnp.stack([zero, db], axis=2)).reshape(2, 16, f_blk)
        small = jnp.concatenate([sums[0], sums[1], db[0], db[1]], axis=1)
        small = lax.psum_scatter(small, ALL_AXES, scatter_dimension=0, tiled=True)[0]
        g_scale, g_bias, g_b1, g_b2 = small[:r_in], small[r_in:2 * r_in], small[2 * r_in:2 * r_in + f_blk], small[2 * r_in + f_blk:]

        g_w1, g_w2, g_wd = join_up(owns, recvs)
        g_wo, g_wq, g_wk, g_wv = g_attn[:r_o, :d_model], g_attn[r_o:, :qk], g_attn[r_o:, qk:qk + HEAD_DIM], g_attn[r_o:, qk + HEAD_DIM:]
        return (x_out, d_x, g_scale, g_wq, g_wk, g_wv, g_wo, g_bias, g_w1, g_b1, g_w2, g_b2, g_wd, g_bias)

    in_specs = (tok_spec, tok_spec, pos_spec, pos_spec) + param_specs
    out_specs = (tok_spec, tok_spec) + param_specs
    return jax.shard_map(local_step, mesh=mesh4, in_specs=in_specs, out_specs=out_specs, check_vma=False)
```

```python
import functools
import jax
import jax.numpy as jnp
from jax import lax
from jax.experimental import pallas as pl
from jax.experimental.pallas import tpu as pltpu
from jax.sharding import Mesh, PartitionSpec as P


ROPE_DIMS = 128
HEAD_DIM = 256
N_HEADS = 4
MASKED = -1.6e31
EXP_SCALE = 1.4426950408889634 / 16.0
CHIPS = ('z', 'y', 'x')
ALL_AXES = ('z', 'y', 'x', 'core')
F32 = jnp.float32
BF16 = jnp.bfloat16


def dot_nn(a, b):
    return lax.dot_general(a, b, (((1,), (0,)), ((), ())), preferred_element_type=F32)


def dot_nt(a, b):
    return lax.dot_general(a, b, (((1,), (1,)), ((), ())), preferred_element_type=F32)


def dot_tn(a, b):
    return lax.dot_general(a, b, (((0,), (0,)), ((), ())), preferred_element_type=F32)


def rotate(values, cos_b, sin_b):
    return values * cos_b + pltpu.roll(values, ROPE_DIMS // 2, axis=1) * sin_b


def attn_kernel(ng_ref, wqkv_ref, wo_ref, cos_ref, sin_ref, cosk_ref, sink_ref, segq_ref, segk_ref, out_ref,
                q_s, do_s, k_s, v_s, kt_s, vt_s, mask_s, s_s, p_s, dk_s, dv_s):
    step = pl.program_id(0)
    n_blocks = pl.num_programs(0)
    rows = ng_ref.shape[0]
    d_model = ng_ref.shape[1] // 2
    qk = N_HEADS * HEAD_DIM
    base = pl.multiple_of(step * rows, rows)
    cos_b = cos_ref[...]
    sin_b = sin_ref[...]
    n_blk = ng_ref[:, :d_model]
    g_blk = ng_ref[:, d_model:]

    @pl.when(step == 0)
    def _():
        dk_s[...] = jnp.zeros_like(dk_s)
        dv_s[...] = jnp.zeros_like(dv_s)

    for h in range(N_HEADS):
        lin = dot_nn(n_blk, wqkv_ref[:, h * HEAD_DIM:(h + 1) * HEAD_DIM])
        q_s[h, :, :ROPE_DIMS] = rotate(lin[:, :ROPE_DIMS], cos_b, sin_b).astype(BF16)
        q_s[h, :, ROPE_DIMS:] = lin[:, ROPE_DIMS:].astype(BF16)
        do_s[h] = dot_nt(g_blk, wo_ref[h * HEAD_DIM:(h + 1) * HEAD_DIM, :]).astype(BF16)
    k_lin = dot_nn(n_blk, wqkv_ref[:, qk:qk + HEAD_DIM])
    k_blk = jnp.concatenate([rotate(k_lin[:, :ROPE_DIMS], cos_b, sin_b), k_lin[:, ROPE_DIMS:]], axis=1)
    v_blk = dot_nn(n_blk, wqkv_ref[:, qk + HEAD_DIM:])
    k_s[pl.ds(base, rows), :] = k_blk.astype(BF16)
    v_s[pl.ds(base, rows), :] = v_blk.astype(BF16)
    kt_s[:, pl.ds(base, rows)] = k_blk.T.astype(BF16)
    vt_s[:, pl.ds(base, rows)] = v_blk.T.astype(BF16)

    def block(blk):
        n_chunk = blk + 1
        seg_q = segq_ref[:, :1]
        for c in range(n_chunk):
            same = seg_q == segk_ref[:1, c * rows:(c + 1) * rows]
            if c == blk:
                r_id = lax.broadcasted_iota(jnp.int32, (rows, rows), 0)
                c_id = lax.broadcasted_iota(jnp.int32, (rows, rows), 1)
                same = same & (c_id <= r_id)
            mask_s[:, c * rows:(c + 1) * rows] = jnp.where(same, 1.0, 0.0)

        def head(h, carry):
            q = q_s[h]
            do = do_s[h]
            m_run = None
            for c in range(n_chunk):
                sl = slice(c * rows, (c + 1) * rows)
                s = jnp.where(mask_s[:, sl] > 0.5, dot_nn(q, kt_s[:, sl]), MASKED)
                s_s[:, sl] = s
                m_c = jnp.max(s, axis=1, keepdims=True)
                m_run = m_c if m_run is None else jnp.maximum(m_run, m_c)
            l_run = None
            for c in range(n_chunk):
                sl = slice(c * rows, (c + 1) * rows)
                e = jnp.exp2((s_s[:, sl] - m_run) * EXP_SCALE)
                s_s[:, sl] = e
                l_c = jnp.sum(e, axis=1, keepdims=True)
                l_run = l_c if l_run is None else l_run + l_c
            inv = 1.0 / l_run
            for c in range(n_chunk):
                sl = slice(c * rows, (c + 1) * rows)
                p = s_s[:, sl] * inv
                s_s[:, sl] = p
                p_s[:, sl] = p.astype(BF16)
            o = dot_nn(p_s[:, :n_chunk * rows], v_s[:n_chunk * rows, :])
            delta = jnp.sum(o * do.astype(F32), axis=1, keepdims=True)
            out_ref[pl.ds(base, rows), pl.ds(pl.multiple_of(qk + 2 * HEAD_DIM + h * HEAD_DIM, HEAD_DIM), HEAD_DIM)] = o.astype(BF16)
            dq = None
            for c in range(n_chunk):
                sl = slice(c * rows, (c + 1) * rows)
                ds = (s_s[:, sl] * (dot_nn(do, vt_s[:, sl]) - delta)).astype(BF16)
                dq_c = dot_nn(ds, k_s[sl, :])
                dq = dq_c if dq is None else dq + dq_c
                dk_s[sl, :] += dot_tn(ds, q)
                dv_s[sl, :] += dot_tn(p_s[:, sl], do)
            dq = dq * 0.0625
            dq = jnp.concatenate([rotate(dq[:, :ROPE_DIMS], cos_b, -sin_b), dq[:, ROPE_DIMS:]], axis=1)
            out_ref[pl.ds(base, rows), pl.ds(pl.multiple_of(h * HEAD_DIM, HEAD_DIM), HEAD_DIM)] = dq.astype(BF16)
            return carry

        lax.fori_loop(0, N_HEADS, head, 0)

    for blk in range(4):
        pl.when(step == blk)(functools.partial(block, blk))

    @pl.when(step == n_blocks - 1)
    def _():
        dk = dk_s[...] * 0.0625
        dk = jnp.concatenate([rotate(dk[:, :ROPE_DIMS], cosk_ref[...], -sink_ref[...]), dk[:, ROPE_DIMS:]], axis=1)
        out_ref[:, qk:qk + HEAD_DIM] = dk.astype(BF16)
        out_ref[:, qk + HEAD_DIM:qk + 2 * HEAD_DIM] = dv_s[...].astype(BF16)


def attention(ng_seq, wqkv, wo, cos_b, sin_b, seg_own):
    t_len, both = ng_seq.shape
    rows = t_len // 4
    qk = N_HEADS * HEAD_DIM
    segq = jnp.broadcast_to(seg_own[:, None], (t_len, 128))
    segk = jnp.broadcast_to(seg_own[None, :], (8, t_len))
    row_spec = lambda width: pl.BlockSpec((rows, width), lambda i: (i, 0))
    full = lambda a: pl.BlockSpec(a.shape, lambda i: (0,) * a.ndim, pipeline_mode=pl.Buffered(1))
    width = 2 * (qk + HEAD_DIM)
    return pl.pallas_call(
        attn_kernel,
        grid=(4,),
        in_specs=[row_spec(both), full(wqkv), full(wo), row_spec(ROPE_DIMS), row_spec(ROPE_DIMS), full(cos_b), full(sin_b), row_spec(128), full(segk)],
        out_specs=pl.BlockSpec((t_len, width), lambda i: (0, 0)),
        out_shape=jax.ShapeDtypeStruct((t_len, width), BF16),
        scratch_shapes=[
            pltpu.VMEM((N_HEADS, rows, HEAD_DIM), BF16), pltpu.VMEM((N_HEADS, rows, HEAD_DIM), BF16),
            pltpu.VMEM((t_len, HEAD_DIM), BF16), pltpu.VMEM((t_len, HEAD_DIM), BF16),
            pltpu.VMEM((HEAD_DIM, t_len), BF16), pltpu.VMEM((HEAD_DIM, t_len), BF16),
            pltpu.VMEM((rows, t_len), F32), pltpu.VMEM((rows, t_len), F32), pltpu.VMEM((rows, t_len), BF16),
            pltpu.VMEM((t_len, HEAD_DIM), F32), pltpu.VMEM((t_len, HEAD_DIM), F32)],
        compiler_params=pltpu.CompilerParams(vmem_limit_bytes=60 * 1024 * 1024, dimension_semantics=('arbitrary',)),
        cost_estimate=pl.CostEstimate(flops=45_000_000_000, bytes_accessed=40_000_000, transcendentals=10_000_000),
        name='attn',
    )(ng_seq, wqkv, wo, cos_b, sin_b, cos_b, sin_b, segq, segk)


def norm_kernel(x_ref, g_ref, scale_ref, out_ref):
    d_model = x_ref.shape[1]
    for part in range(0, x_ref.shape[0], 128):
        sl = slice(part, part + 128)
        x_f = x_ref[sl, :].astype(F32)
        inv = lax.rsqrt(jnp.mean(x_f * x_f, axis=1, keepdims=True) + 1e-6)
        out_ref[sl, :d_model] = (x_f * inv * (1.0 + scale_ref[...])).astype(BF16)
        out_ref[sl, d_model:] = g_ref[sl, :]


def norm_and_grad(x_loc, g_loc, scale_f):
    t_len, d_model = x_loc.shape
    rows = 512
    tile = pl.BlockSpec((rows, d_model), lambda i: (i, 0))
    return pl.pallas_call(
        norm_kernel, grid=(t_len // rows,), name='norm',
        in_specs=[tile, tile, pl.BlockSpec(scale_f.shape, lambda i: (0, 0))],
        out_specs=pl.BlockSpec((rows, 2 * d_model), lambda i: (i, 0)),
        out_shape=jax.ShapeDtypeStruct((t_len, 2 * d_model), BF16),
        cost_estimate=pl.CostEstimate(flops=4_000_000_000, bytes_accessed=19_000_000, transcendentals=2048),
    )(x_loc, g_loc, scale_f)


def order_kernel(x_ref, a_ref, b_ref, c_ref, out_ref):
    cp = lax.axis_index('z') * 2 + lax.axis_index('y')
    rows = a_ref.shape[1]
    for flip, ref in enumerate((x_ref.at[cp], a_ref.at[0], b_ref.at[0], c_ref.at[0])):
        out_ref[pl.ds(pl.multiple_of((cp ^ flip) * rows, rows), rows), :] = ref[...]


def order(values, got):
    n_seq, rows, width = values.shape
    return pl.pallas_call(
        order_kernel, out_shape=jax.ShapeDtypeStruct((n_seq * rows, width), values.dtype), name='order',
        compiler_params=pltpu.CompilerParams(vmem_limit_bytes=40 * 1024 * 1024),
        cost_estimate=pl.CostEstimate(flops=2_000_000_000, bytes_accessed=10_000_000, transcendentals=0),
    )(values, *got)


N_PART = 3
EXTRA_GATHER = 1


def split_kernel(w1_ref, w2_ref, keep_ref, send_ref):
    core = lax.axis_index('core')
    d_model = keep_ref.shape[2] // 2
    sub = d_model // 8
    for part in range(N_PART):
        for i, w_ref in enumerate((w1_ref, w2_ref)):
            even, odd = [
                jnp.concatenate([w_ref[:, ((2 * j + k) * N_PART + part) * sub:((2 * j + k) * N_PART + part + 1) * sub] for j in range(8)], axis=1).astype(BF16)
                for k in range(2)]

            @pl.when(core == 0)
            def _():
                keep_ref[part, :, i * d_model:(i + 1) * d_model] = even
                send_ref[part, :, i * d_model:(i + 1) * d_model] = odd

            @pl.when(core == 1)
            def _():
                keep_ref[part, :, i * d_model:(i + 1) * d_model] = odd
                send_ref[part, :, i * d_model:(i + 1) * d_model] = even


def split_up(w1, w2):
    rows, cols = w1.shape
    out = jax.ShapeDtypeStruct((N_PART, rows, cols // N_PART), BF16)
    return pl.pallas_call(split_kernel, out_shape=[out, out], name='split_up')(w1, w2)


def stack_kernel(keep_ref, recv_ref, wd_ref, extra_ref, *out_refs):
    core = lax.axis_index('core')
    rows, cols = keep_ref.shape[1:]
    d_model = wd_ref.shape[1]
    for part, out_ref in enumerate(out_refs):
        own = pl.multiple_of(core * rows, 8)
        out_ref[pl.ds(own, rows), :cols] = keep_ref[part]
        out_ref[pl.ds(pl.multiple_of(rows - own, 8), rows), :cols] = recv_ref[part]
        out_ref[:, cols:cols + d_model] = wd_ref[part * 2 * rows:(part + 1) * 2 * rows, :].astype(BF16)
        if part == EXTRA_GATHER:
            n_extra = extra_ref.shape[0]
            out_ref[:n_extra, cols + d_model:] = extra_ref[...]
            out_ref[n_extra:, cols + d_model:] = jnp.zeros((2 * rows - n_extra, extra_ref.shape[1]), BF16)


def stack_up(keep, recv, w_down, extra):
    _, rows, cols = keep.shape
    width = cols + w_down.shape[1]
    outs = [jax.ShapeDtypeStruct((2 * rows, width + (extra.shape[1] if part == EXTRA_GATHER else 0)), BF16) for part in range(N_PART)]
    return pl.pallas_call(stack_kernel, out_shape=outs, name='stack_up')(keep, recv, w_down, extra)


def unpack_kernel(own_ref, oth_ref, wqkv_ref, wo_ref):
    core = lax.axis_index('core')
    r_o, r_in = wo_ref.shape[0] // 16, wqkv_ref.shape[0] // 16
    d_model = wo_ref.shape[1]
    rows = own_ref.shape[0] // 8
    for chip in range(8):
        for flip, ref in enumerate((own_ref, oth_ref)):
            dev = 2 * chip + (core ^ flip)
            wo_ref[pl.ds(pl.multiple_of(dev * r_o, 8), r_o), :] = ref[chip * rows:chip * rows + r_o, :d_model]
            wqkv_ref[pl.ds(pl.multiple_of(dev * r_in, 8), r_in), :] = ref[chip * rows + r_o:chip * rows + r_o + r_in, :]


def unpack(own, oth, r_o, r_in, d_model):
    return pl.pallas_call(
        unpack_kernel, name='unpack',
        out_shape=[jax.ShapeDtypeStruct((16 * r_in, own.shape[1]), BF16), jax.ShapeDtypeStruct((16 * r_o, d_model), BF16)],
    )(own, oth)


def join_kernel(*refs):
    own_refs, recv_refs, (w1_ref, w2_ref, wd_ref) = refs[:N_PART], refs[N_PART:2 * N_PART], refs[2 * N_PART:]
    core = lax.axis_index('core')
    rows = w1_ref.shape[0]
    d_model = wd_ref.shape[1]
    sub = d_model // 8

    def put(even_of, odd_of):
        for i, w_ref in enumerate((w1_ref, w2_ref)):
            pieces = []
            for j in range(8):
                for of in (even_of, odd_of):
                    for part in range(N_PART):
                        pieces.append(of(part)[:, i * d_model + j * sub:i * d_model + (j + 1) * sub])
            w_ref[...] = jnp.concatenate(pieces, axis=1)

    pl.when(core == 0)(lambda: put(lambda p: own_refs[p][:rows, :2 * d_model], lambda p: recv_refs[p][...]))
    pl.when(core == 1)(lambda: put(lambda p: recv_refs[p][...], lambda p: own_refs[p][rows:, :2 * d_model]))
    for part in range(N_PART):
        wd_ref[part * 2 * rows:(part + 1) * 2 * rows, :] = own_refs[part][:, 2 * d_model:3 * d_model]


def join_up(owns, recvs):
    rows, cols = recvs[0].shape
    d_model = cols // 2
    up = jax.ShapeDtypeStruct((rows, N_PART * cols), F32)
    return pl.pallas_call(
        join_kernel, out_shape=[up, up, jax.ShapeDtypeStruct((N_PART * 2 * rows, d_model), F32)], name='join_up',
    )(*owns, *recvs)


GELU_C = 0.7978845608028654
GELU_A = 0.044715


def hidden_kernel(own_ref, oth_ref, w_ref, b1_ref, b2_ref, *refs):
    extra_refs = refs[:-10]
    act_ref, dh_ref, dw_ref, db_ref, h_s, da_s, ng_s, acc_s, side_s, sems = refs[-10:]
    step = pl.program_id(0)
    last = pl.num_programs(0) - 1
    rows, d_model = da_s.shape
    own = step < pl.num_programs(0) // 2
    ng_s[...] = jnp.where(own, own_ref[...], oth_ref[...])

    @pl.when(step == 0)
    def _():
        acc_s[...] = jnp.zeros_like(acc_s)
        db_ref[...] = jnp.zeros_like(db_ref)

    n_sub = 2
    sub = rows // n_sub
    w12 = w_ref[:, :2 * d_model]
    for i in range(n_sub):
        sl = slice(i * sub, (i + 1) * sub)
        h_s[sl, :] = dot_nn(ng_s[sl, :d_model], w12)
        da_s[sl, :] = dot_nt(ng_s[sl, d_model:], w_ref[:, 2 * d_model:])
    b1 = b1_ref[...]
    b2 = b2_ref[...]
    for i in range(n_sub):
        sl = slice(i * sub, (i + 1) * sub)
        s1 = None
        s2 = None
        for r in range(i * sub, (i + 1) * sub, 64):
            rs = slice(r, r + 64)
            u = h_s[rs, :d_model] + b1
            v = h_s[rs, d_model:] + b2
            da = da_s[rs, :]
            u2 = u * u
            t = jnp.tanh(u * (GELU_C + (GELU_C * GELU_A) * u2))
            half = 0.5 + 0.5 * t
            gelu = u * half
            slope = half + (half * (1.0 - t)) * (u * (GELU_C + (3.0 * GELU_C * GELU_A) * u2))
            d1 = da * v * slope
            d2 = da * gelu
            act_ref[rs, :] = (gelu * v).astype(BF16)
            dh_ref[rs, :d_model] = d1.astype(BF16)
            dh_ref[rs, d_model:] = d2.astype(BF16)
            p1 = jnp.sum(d1.reshape(8, 8, d_model), axis=0)
            p2 = jnp.sum(d2.reshape(8, 8, d_model), axis=0)
            s1 = p1 if s1 is None else s1 + p1
            s2 = p2 if s2 is None else s2 + p2
        db_ref[:8, :] += s1
        db_ref[8:, :] += s2
        acc_s[:, :2 * d_model] += dot_tn(ng_s[sl, :d_model], dh_ref[sl, :])
        acc_s[:, 2 * d_model:] += dot_tn(act_ref[sl, :], ng_s[sl, d_model:])

    if extra_refs:
        keep_ref, got_ref = extra_refs
        block = side_s.shape[1]
        n_extra = keep_ref.shape[1]
        slot = lax.rem(step, 2)

        def side_copy(at_slot, at_step):
            place = dw_ref.at[pl.ds(pl.multiple_of(at_step * block, 8), block), 3 * d_model:]
            return pltpu.make_async_copy(side_s.at[at_slot], place, sems.at[1 + at_slot])

        @pl.when(step >= 2)
        def _():
            side_copy(slot, step - 2).wait()

        side_s[slot, :n_extra, :] = keep_ref[0] + got_ref[0]
        side_s[slot, n_extra:, :] = jnp.zeros((block - n_extra, keep_ref.shape[2]), F32)
        side_copy(slot, step).start()

        @pl.when(step == last)
        def _():
            side_copy(1 - slot, step - 1).wait()
            side_copy(slot, step).wait()

    @pl.when(step == last)
    def _():
        copy = pltpu.make_async_copy(acc_s, dw_ref.at[:, :3 * d_model], sems.at[0])
        copy.start()
        copy.wait()


def hidden_part(ng_own, ng_oth, w_part, b1, b2, extra=()):
    t_len, both = ng_own.shape
    d_model = both // 2
    rows = 512
    steps = 2 * t_len // rows
    half = steps // 2
    own_spec = pl.BlockSpec((rows, both), lambda i: (jnp.minimum(i, half - 1), 0))
    oth_spec = pl.BlockSpec((rows, both), lambda i: (jnp.maximum(i - half, 0), 0))
    full = lambda a, width: pl.BlockSpec((a.shape[0], width), lambda i: (0, 0), pipeline_mode=pl.Buffered(1))
    row = lambda width: pl.BlockSpec((rows, width), lambda i: (i, 0))
    blk = [pl.BlockSpec((1,) + a.shape[1:], lambda i: (i, 0, 0)) for a in extra]
    side = (2, d_model // 8, extra[0].shape[2]) if extra else (2, 8, 128)
    return pl.pallas_call(
        hidden_kernel,
        grid=(steps,),
        in_specs=[own_spec, oth_spec, full(w_part, 3 * d_model), full(b1, d_model), full(b2, d_model)] + blk,
        out_specs=[row(d_model), row(2 * d_model), pl.BlockSpec(memory_space=pl.ANY), pl.BlockSpec((16, d_model), lambda i: (0, 0))],
        out_shape=[jax.ShapeDtypeStruct((2 * t_len, d_model), BF16), jax.ShapeDtypeStruct((2 * t_len, 2 * d_model), BF16),
                   jax.ShapeDtypeStruct((d_model, 3 * d_model + (extra[0].shape[2] if extra else 0)), F32), jax.ShapeDtypeStruct((16, d_model), F32)],
        scratch_shapes=[pltpu.VMEM((rows, 2 * d_model), F32), pltpu.VMEM((rows, d_model), F32), pltpu.VMEM((rows, both), BF16),
                        pltpu.VMEM((d_model, 3 * d_model), F32), pltpu.VMEM(side, F32), pltpu.SemaphoreType.DMA((3,))],
        compiler_params=pltpu.CompilerParams(vmem_limit_bytes=63 * 1024 * 1024, dimension_semantics=('arbitrary',)),
        cost_estimate=pl.CostEstimate(flops=65_000_000_000, bytes_accessed=70_000_000, transcendentals=4_700_000),
        name='hidden',
    )(ng_own, ng_oth, w_part, b1, b2, *extra)


def attn_grad_kernel(n_ref, dqkv_ref, o_lo_ref, o_hi_ref, g_ref, keep_ref, send_ref):
    step = pl.program_id(0)
    core = lax.axis_index('core')
    r_o, r_in = o_lo_ref.shape[1] // 8, n_ref.shape[1] // 16
    width = dqkv_ref.shape[1]
    d_model = g_ref.shape[1]

    def put(rows, cols, value_of):
        for dev in range(16):
            for ref, flip in ((keep_ref, 0), (send_ref, 1)):
                @pl.when((core ^ flip) == dev % 2)
                def _():
                    ref[dev // 2, rows, cols] = value_of(dev)

    d_wqkv = dot_tn(n_ref[...], dqkv_ref[...])
    put(slice(r_o, r_o + r_in), slice(0, width), lambda dev: d_wqkv[dev * r_in:(dev + 1) * r_in])

    def low(first_col, used):
        g_cols = g_ref[:, first_col:first_col + used]
        d_wo = [dot_tn(o_lo_ref[...], g_cols), dot_tn(o_hi_ref[...], g_cols)]
        put(slice(0, r_o), slice(0, used), lambda dev: d_wo[dev // 8][dev % 8 * r_o:(dev % 8 + 1) * r_o])
        if used < width:
            put(slice(0, r_o), slice(used, width), lambda dev: jnp.zeros((r_o, width - used), F32))

    for i in range(-(-d_model // width)):
        pl.when(step == i)(functools.partial(low, i * width, min(width, d_model - i * width)))


def attn_grad(ng_seq, od_seq, r_o, r_in):
    t_len, both = ng_seq.shape
    d_model = both // 2
    width = 512
    qk = N_HEADS * HEAD_DIM
    total = qk + 2 * HEAD_DIM
    out = jax.ShapeDtypeStruct((8, r_o + r_in, total), F32)
    out_spec = pl.BlockSpec((8, r_o + r_in, width), lambda i: (0, 0, i))
    one = pl.Buffered(1)
    return pl.pallas_call(
        attn_grad_kernel,
        grid=(total // width,),
        in_specs=[pl.BlockSpec((t_len, d_model), lambda i: (0, 0), pipeline_mode=one), pl.BlockSpec((t_len, width), lambda i: (0, i)),
                  pl.BlockSpec((t_len, width), lambda i: (0, total // width), pipeline_mode=one), pl.BlockSpec((t_len, width), lambda i: (0, total // width + 1), pipeline_mode=one),
                  pl.BlockSpec((t_len, d_model), lambda i: (0, 1), pipeline_mode=one)],
        out_specs=[out_spec, out_spec],
        out_shape=[out, out],
        compiler_params=pltpu.CompilerParams(vmem_limit_bytes=60 * 1024 * 1024, dimension_semantics=('arbitrary',)),
        cost_estimate=pl.CostEstimate(flops=12_000_000_000, bytes_accessed=33_000_000, transcendentals=0),
        name='attn_grad',
    )(ng_seq, od_seq, od_seq, od_seq, ng_seq)


def out_products(act_refs, dh_refs, w_refs):
    d_model = act_refs[0].shape[1]
    out = None
    d_n = None
    for act_ref, dh_ref, w_ref in zip(act_refs, dh_refs, w_refs):
        o_part = dot_nn(act_ref[...], w_ref[:, 2 * d_model:3 * d_model])
        n_part = dot_nt(dh_ref[...], w_ref[:, :2 * d_model])
        out = o_part if out is None else out + o_part
        d_n = n_part if d_n is None else d_n + n_part
    return out, d_n


def out_other_kernel(*refs):
    out, d_n = out_products(refs[:3], refs[3:6], refs[6:9])
    refs[9][...] = out
    refs[10][...] = d_n


def out_specs_of(rows, d_model, first_block):
    tile = lambda width: pl.BlockSpec((rows, width), lambda i: (i + first_block, 0))
    full = pl.BlockSpec((d_model, 3 * d_model), lambda i: (0, 0), pipeline_mode=pl.Buffered(1))
    return [tile(d_model)] * 3 + [tile(2 * d_model)] * 3 + [full] * 3


def out_other(acts, dhs, w_parts):
    t_len, d_model = acts[0].shape[0] // 2, acts[0].shape[1]
    rows = 256
    tile = pl.BlockSpec((rows, d_model), lambda i: (i, 0))
    out = jax.ShapeDtypeStruct((t_len, d_model), F32)
    return pl.pallas_call(
        out_other_kernel,
        grid=(t_len // rows,),
        in_specs=out_specs_of(rows, d_model, t_len // rows),
        out_specs=[tile, tile],
        out_shape=[out, out],
        compiler_params=pltpu.CompilerParams(vmem_limit_bytes=60 * 1024 * 1024, dimension_semantics=('arbitrary',)),
        cost_estimate=pl.CostEstimate(flops=49_000_000_000, bytes_accessed=86_000_000, transcendentals=0),
        name='out_other',
    )(*acts, *dhs, *w_parts)


def out_own_kernel(*refs):
    (od_ref, wo_ref, wqkv_ref, x_ref, g_ref, got_o_ref, got_n_ref, scale_ref, bias_ref, x_out_ref, d_x_ref, sums_ref) = refs[9:]
    d_model = x_ref.shape[1]

    @pl.when(pl.program_id(0) == 0)
    def _():
        sums_ref[...] = jnp.zeros_like(sums_ref)

    out, d_n = out_products(refs[:3], refs[3:6], refs[6:9])
    split = wqkv_ref.shape[1]
    out = out + dot_nn(od_ref[:, split:], wo_ref[...])
    d_n = d_n + dot_nt(od_ref[:, :split], wqkv_ref[...])
    x_f = x_ref[...].astype(F32)
    g_f = g_ref[...].astype(F32)
    x_out_ref[...] = (x_f + out + got_o_ref[...] + bias_ref[...]).astype(BF16)
    d_n = d_n + got_n_ref[...]
    inv = lax.rsqrt(jnp.mean(x_f * x_f, axis=1, keepdims=True) + 1e-6)
    scaled = d_n * (1.0 + scale_ref[...])
    xn = x_f * inv
    proj = jnp.mean(scaled * xn, axis=1, keepdims=True)
    d_x_ref[...] = (g_f + inv * (scaled - xn * proj)).astype(BF16)
    rows = x_f.shape[0]
    sums_ref[:8, :] += jnp.sum((d_n * xn).reshape(rows // 8, 8, d_model), axis=0)
    sums_ref[8:, :] += jnp.sum(g_f.reshape(rows // 8, 8, d_model), axis=0)


def out_own(acts, dhs, w_parts, od_loc, wo, wqkv, x_loc, ng_own, got_o, got_n, scale_f, bias_f):
    t_len, d_model = x_loc.shape
    rows = 256
    tile = lambda width: pl.BlockSpec((rows, width), lambda i: (i, 0))
    full = lambda a: pl.BlockSpec(a.shape, lambda i: (0, 0), pipeline_mode=pl.Buffered(1))
    out = jax.ShapeDtypeStruct((t_len, d_model), BF16)
    return pl.pallas_call(
        out_own_kernel,
        grid=(t_len // rows,),
        in_specs=out_specs_of(rows, d_model, 0) + [tile(od_loc.shape[1]), full(wo), full(wqkv), tile(d_model), pl.BlockSpec((rows, d_model), lambda i: (i, 1))]
                 + [tile(d_model)] * 2 + [full(scale_f), full(bias_f)],
        out_specs=[tile(d_model), tile(d_model), pl.BlockSpec((16, d_model), lambda i: (0, 0))],
        out_shape=[out, out, jax.ShapeDtypeStruct((16, d_model), F32)],
        compiler_params=pltpu.CompilerParams(vmem_limit_bytes=63 * 1024 * 1024, dimension_semantics=('arbitrary',)),
        cost_estimate=pl.CostEstimate(flops=61_000_000_000, bytes_accessed=125_000_000, transcendentals=0),
        name='out_own',
    )(*acts, *dhs, *w_parts, od_loc, wo, wqkv, x_loc, ng_own, got_o, got_n, scale_f, bias_f)


def pack_kernel(wq_ref, wk_ref, wv_ref, wo_ref, out_ref):
    r_o, d_model = wo_ref.shape
    qk = wq_ref.shape[1]
    out_ref[:r_o, :d_model] = wo_ref[...].astype(BF16)
    out_ref[:r_o, d_model:] = jnp.zeros((r_o, out_ref.shape[1] - d_model), BF16)
    out_ref[r_o:, :qk] = wq_ref[...].astype(BF16)
    out_ref[r_o:, qk:qk + HEAD_DIM] = wk_ref[...].astype(BF16)
    out_ref[r_o:, qk + HEAD_DIM:] = wv_ref[...].astype(BF16)


def pack(w_q, w_k, w_v, w_o):
    out = jax.ShapeDtypeStruct((w_o.shape[0] + w_q.shape[0], w_q.shape[1] + 2 * HEAD_DIM), BF16)
    return pl.pallas_call(pack_kernel, out_shape=out, name='pack')(w_q, w_k, w_v, w_o)


def vector_kernel(scale_ref, bo_ref, bd_ref, b1_ref, b2_ref, out_ref, side_s):
    side_s[...] = jnp.zeros_like(side_s)
    for row, ref in enumerate((scale_ref, bo_ref, bd_ref, b1_ref, b2_ref)):
        side_s[row:row + 1, :ref.shape[1]] = ref[...]
    out_ref[...] = side_s[...].astype(BF16)


def vectors(*parts):
    width = -(-max(part.shape[0] for part in parts) // 128) * 128
    return pl.pallas_call(
        vector_kernel, out_shape=jax.ShapeDtypeStruct((8, width), BF16), scratch_shapes=[pltpu.VMEM((8, width), F32)], name='vectors',
    )(*[part[None] for part in parts])


def solution(mesh):
    mesh4 = Mesh(mesh.devices.reshape(2, 2, 2, 2), ALL_AXES)
    tok_spec = P(('x', 'core'), ('z', 'y'), None)
    pos_spec = P(('x', 'core'), ('z', 'y'))
    vec_spec = P(ALL_AXES)
    mat_spec = P(ALL_AXES, None)
    param_specs = (vec_spec, mat_spec, mat_spec, mat_spec, mat_spec, vec_spec, mat_spec, vec_spec, mat_spec, vec_spec, mat_spec, vec_spec)

    def swap_core(values):
        return lax.ppermute(values, 'core', [(0, 1), (1, 0)])

    def send_blocks(values, cp_index):
        got = []
        for flip in (1, 2, 3):
            sent = lax.dynamic_index_in_dim(values, cp_index ^ flip, 0, keepdims=True)
            got.append(lax.ppermute(sent, ('z', 'y'), [(i, i ^ flip) for i in range(4)]))
        return got

    def local_step(x_in, grad_out, seg_id, seg_pos, norm_scale, w_q, w_k, w_v, w_o, b_o, w_up1, b_up1, w_up2, b_up2, w_down, b_down):
        n_seq, piece, d_model = x_in.shape
        t_len = n_seq * piece
        core = lax.axis_index('core')
        cp_index = lax.axis_index('z') * 2 + lax.axis_index('y')
        first = core == 0
        r_in = w_q.shape[0]
        r_o = w_o.shape[0]
        f_blk = b_up1.shape[0]
        sub = f_blk // N_PART
        qk = N_HEADS * HEAD_DIM

        def after(value, *deps):
            return lax.optimization_barrier((value,) + deps)[0]

        keep, send = split_up(w_up1, w_up2)
        shards = stack_up(keep, swap_core(send), w_down, pack(w_q, w_k, w_v, w_o))

        def gather(shard):
            return lax.all_gather(shard, CHIPS, axis=0, tiled=True)

        w_parts = [gather(shards[0])]

        vec_all = lax.all_gather(vectors(norm_scale, b_o, b_down, b_up1, b_up2), ALL_AXES, axis=0)
        scale_f, bo_f, bd_f = [vec_all[:, i, :r_in].reshape(1, d_model).astype(F32) for i in range(3)]
        b_ups = []
        for row in (3, 4):
            both = vec_all[:, row, :f_blk].reshape(8, 2, N_PART, sub)
            mine = jnp.where(first, both[:, 0], both[:, 1]).astype(F32)
            b_ups.append([mine[:, part].reshape(1, d_model) for part in range(N_PART)])

        x_loc = x_in.reshape(t_len, d_model)
        g_loc = grad_out.reshape(t_len, d_model)
        ng_own = norm_and_grad(x_loc, g_loc, scale_f)
        ng_oth = swap_core(ng_own)
        w_parts.append(gather(shards[1]))
        w_parts.append(gather(shards[2]))

        seg_pack = jnp.stack([seg_id, seg_pos], axis=1)
        seg_got = send_blocks(seg_pack, cp_index)
        seg_all = jnp.zeros_like(seg_pack)
        for flip, got in enumerate([lax.dynamic_index_in_dim(seg_pack, cp_index, 0, keepdims=True)] + seg_got):
            seg_all = lax.dynamic_update_slice_in_dim(seg_all, got, cp_index ^ flip, 0)
        seg_own = seg_all[:, 0].reshape(t_len)
        pos_own = seg_all[:, 1].reshape(t_len)
        half = ROPE_DIMS // 2
        inv_freq = 10000.0 ** (-jnp.arange(half, dtype=F32) / half)
        angle = pos_own.astype(F32)[:, None] * inv_freq
        cos_a = jnp.cos(angle)
        sin_a = jnp.sin(angle)
        cos_b = jnp.concatenate([cos_a, cos_a], axis=1)
        sin_b = jnp.concatenate([-sin_a, sin_a], axis=1)
        ng_blocks = ng_own.reshape(n_seq, piece, 2 * d_model)
        ng_seq = order(ng_blocks, send_blocks(after(ng_blocks, w_parts[0]), cp_index))

        acts, dhs, dbs, owns, recvs = [], [], [], [], []

        def third(part, ng_in, extra=()):
            act, dh, d_w, db = hidden_part(ng_in, ng_oth, w_parts[part], b_ups[0][part], b_ups[1][part], extra)
            own = lax.psum_scatter(d_w, CHIPS, scatter_dimension=0, tiled=True)
            recvs.append(swap_core(jnp.where(first, own[r_in:, :2 * d_model], own[:r_in, :2 * d_model])))
            acts.append(act)
            dhs.append(dh)
            dbs.append(jnp.sum(db.reshape(2, 8, d_model), axis=1).reshape(2, 8, sub))
            owns.append(own)

        third(0, ng_own)
        third(1, after(ng_own, dbs[0]))
        extra_own = w_parts[1][:, 3 * d_model:]
        wqkv, wo = unpack(extra_own, swap_core(extra_own), r_o, r_in, d_model)
        od_seq = attention(after(ng_seq, dbs[1]), wqkv, wo, cos_b, sin_b, seg_own)
        d_keep, d_send = attn_grad(ng_seq, od_seq, r_o, r_in)
        third(2, ng_own, (d_keep, swap_core(d_send)))
        od_blocks = od_seq.reshape(n_seq, piece, -1)
        od_loc = order(od_blocks, send_blocks(od_blocks, cp_index))

        out_oth, dn_oth = out_other(acts, dhs, w_parts)
        x_out, d_x, sums = out_own(acts, dhs, w_parts, od_loc, wo, wqkv, x_loc, ng_own, swap_core(out_oth), swap_core(dn_oth), scale_f, bo_f + bd_f)
        x_out = x_out.reshape(n_seq, piece, d_model)
        d_x = d_x.reshape(n_seq, piece, d_model)

        sums = jnp.sum(sums.reshape(2, 8, d_model), axis=1).reshape(2, 16, r_in)
        db = jnp.stack(dbs, axis=2).reshape(2, 8, f_blk)
        zero = jnp.zeros_like(db)
        db = jnp.where(first, jnp.stack([db, zero], axis=2), jnp.stack([zero, db], axis=2)).reshape(2, 16, f_blk)
        small = jnp.concatenate([sums[0], sums[1], db[0], db[1]], axis=1)
        small = lax.psum(small, ALL_AXES)
        small = lax.dynamic_index_in_dim(small, lax.axis_index(ALL_AXES), 0, keepdims=False)
        g_scale, g_bias, g_b1, g_b2 = small[:r_in], small[r_in:2 * r_in], small[2 * r_in:2 * r_in + f_blk], small[2 * r_in + f_blk:]

        g_w1, g_w2, g_wd = join_up(owns, recvs)
        g_attn = owns[2][:r_o + r_in, 3 * d_model:]
        g_wo, g_wq, g_wk, g_wv = g_attn[:r_o, :d_model], g_attn[r_o:, :qk], g_attn[r_o:, qk:qk + HEAD_DIM], g_attn[r_o:, qk + HEAD_DIM:]
        return (x_out, d_x, g_scale, g_wq, g_wk, g_wv, g_wo, g_bias, g_w1, g_b1, g_w2, g_b2, g_wd, g_bias)

    in_specs = (tok_spec, tok_spec, pos_spec, pos_spec) + param_specs
    out_specs = (tok_spec, tok_spec) + param_specs
    return jax.shard_map(local_step, mesh=mesh4, in_specs=in_specs, out_specs=out_specs, check_vma=False)
```

```python
import functools
import jax
import jax.numpy as jnp
from jax import lax
from jax.experimental import pallas as pl
from jax.experimental.pallas import tpu as pltpu
from jax.sharding import Mesh, PartitionSpec as P


ROPE_DIMS = 128
HEAD_DIM = 256
N_HEADS = 4
MASKED = -1.6e31
EXP_SCALE = 1.4426950408889634 / 16.0
CHIPS = ('z', 'y', 'x')
ALL_AXES = ('z', 'y', 'x', 'core')
F32 = jnp.float32
BF16 = jnp.bfloat16


def dot_nn(a, b):
    return lax.dot_general(a, b, (((1,), (0,)), ((), ())), preferred_element_type=F32)


def dot_nt(a, b):
    return lax.dot_general(a, b, (((1,), (1,)), ((), ())), preferred_element_type=F32)


def dot_tn(a, b):
    return lax.dot_general(a, b, (((0,), (0,)), ((), ())), preferred_element_type=F32)


def rotate(values, cos_b, sin_b):
    return values * cos_b + pltpu.roll(values, ROPE_DIMS // 2, axis=1) * sin_b


def attn_kernel(cp_ref, own_ref, n1_ref, n2_ref, n3_ref, g1_ref, g2_ref, g3_ref, wqkv_ref, wo_ref, cos_ref, sin_ref, cosk_ref, sink_ref, segq_ref, segk_ref, out_ref,
                n_s, g_s, q_s, do_s, k_s, v_s, kt_s, vt_s, mask_s, s_s, p_s, dk_s, dv_s):
    step = pl.program_id(0)
    n_blocks = pl.num_programs(0)
    rows, d_model = n_s.shape
    qk = N_HEADS * HEAD_DIM
    base = pl.multiple_of(step * rows, rows)
    cos_b = cos_ref[...]
    sin_b = sin_ref[...]
    flip = step ^ cp_ref[0]

    @pl.when(flip == 0)
    def _():
        n_s[...] = own_ref[0, :, :d_model]
        g_s[...] = own_ref[0, :, d_model:]

    for i, (n_ref, g_ref) in enumerate(((n1_ref, g1_ref), (n2_ref, g2_ref), (n3_ref, g3_ref))):
        @pl.when(flip == i + 1)
        def _():
            n_s[...] = n_ref[0]
            g_s[...] = g_ref[0]

    n_blk = n_s[...]
    g_blk = g_s[...]

    @pl.when(step == 0)
    def _():
        dk_s[...] = jnp.zeros_like(dk_s)
        dv_s[...] = jnp.zeros_like(dv_s)

    for h in range(N_HEADS):
        lin = dot_nn(n_blk, wqkv_ref[:, h * HEAD_DIM:(h + 1) * HEAD_DIM])
        q_s[h, :, :ROPE_DIMS] = rotate(lin[:, :ROPE_DIMS], cos_b, sin_b).astype(BF16)
        q_s[h, :, ROPE_DIMS:] = lin[:, ROPE_DIMS:].astype(BF16)
        do_s[h] = dot_nt(g_blk, wo_ref[h * HEAD_DIM:(h + 1) * HEAD_DIM, :]).astype(BF16)
    k_lin = dot_nn(n_blk, wqkv_ref[:, qk:qk + HEAD_DIM])
    k_blk = jnp.concatenate([rotate(k_lin[:, :ROPE_DIMS], cos_b, sin_b), k_lin[:, ROPE_DIMS:]], axis=1)
    v_blk = dot_nn(n_blk, wqkv_ref[:, qk + HEAD_DIM:])
    k_s[pl.ds(base, rows), :] = k_blk.astype(BF16)
    v_s[pl.ds(base, rows), :] = v_blk.astype(BF16)
    kt_s[:, pl.ds(base, rows)] = k_blk.T.astype(BF16)
    vt_s[:, pl.ds(base, rows)] = v_blk.T.astype(BF16)

    def block(blk):
        n_chunk = blk + 1
        seg_q = segq_ref[:, :1]
        for c in range(n_chunk):
            same = seg_q == segk_ref[:1, c * rows:(c + 1) * rows]
            if c == blk:
                r_id = lax.broadcasted_iota(jnp.int32, (rows, rows), 0)
                c_id = lax.broadcasted_iota(jnp.int32, (rows, rows), 1)
                same = same & (c_id <= r_id)
            mask_s[:, c * rows:(c + 1) * rows] = jnp.where(same, 1.0, 0.0)

        def head(h, carry):
            q = q_s[h]
            do = do_s[h]
            m_run = None
            for c in range(n_chunk):
                sl = slice(c * rows, (c + 1) * rows)
                s = jnp.where(mask_s[:, sl] > 0.5, dot_nn(q, kt_s[:, sl]), MASKED)
                s_s[:, sl] = s
                m_c = jnp.max(s, axis=1, keepdims=True)
                m_run = m_c if m_run is None else jnp.maximum(m_run, m_c)
            l_run = None
            for c in range(n_chunk):
                sl = slice(c * rows, (c + 1) * rows)
                e = jnp.exp2((s_s[:, sl] - m_run) * EXP_SCALE)
                s_s[:, sl] = e
                l_c = jnp.sum(e, axis=1, keepdims=True)
                l_run = l_c if l_run is None else l_run + l_c
            inv = 1.0 / l_run
            for c in range(n_chunk):
                sl = slice(c * rows, (c + 1) * rows)
                p = s_s[:, sl] * inv
                s_s[:, sl] = p
                p_s[:, sl] = p.astype(BF16)
            o = dot_nn(p_s[:, :n_chunk * rows], v_s[:n_chunk * rows, :])
            delta = jnp.sum(o * do.astype(F32), axis=1, keepdims=True)
            out_ref[pl.ds(base, rows), pl.ds(pl.multiple_of(qk + 2 * HEAD_DIM + h * HEAD_DIM, HEAD_DIM), HEAD_DIM)] = o.astype(BF16)
            dq = None
            for c in range(n_chunk):
                sl = slice(c * rows, (c + 1) * rows)
                ds = (s_s[:, sl] * (dot_nn(do, vt_s[:, sl]) - delta)).astype(BF16)
                dq_c = dot_nn(ds, k_s[sl, :])
                dq = dq_c if dq is None else dq + dq_c
                dk_s[sl, :] += dot_tn(ds, q)
                dv_s[sl, :] += dot_tn(p_s[:, sl], do)
            dq = dq * 0.0625
            dq = jnp.concatenate([rotate(dq[:, :ROPE_DIMS], cos_b, -sin_b), dq[:, ROPE_DIMS:]], axis=1)
            out_ref[pl.ds(base, rows), pl.ds(pl.multiple_of(h * HEAD_DIM, HEAD_DIM), HEAD_DIM)] = dq.astype(BF16)
            return carry

        lax.fori_loop(0, N_HEADS, head, 0)

    for blk in range(4):
        pl.when(step == blk)(functools.partial(block, blk))

    @pl.when(step == n_blocks - 1)
    def _():
        dk = dk_s[...] * 0.0625
        dk = jnp.concatenate([rotate(dk[:, :ROPE_DIMS], cosk_ref[...], -sink_ref[...]), dk[:, ROPE_DIMS:]], axis=1)
        out_ref[:, qk:qk + HEAD_DIM] = dk.astype(BF16)
        out_ref[:, qk + HEAD_DIM:qk + 2 * HEAD_DIM] = dv_s[...].astype(BF16)


def attention(cp_index, ng_blocks, n_got, g_got, wqkv, wo, cos_b, sin_b, seg_own):
    _, rows, both = ng_blocks.shape
    t_len = 4 * rows
    qk = N_HEADS * HEAD_DIM
    segq = jnp.broadcast_to(seg_own[:, None], (t_len, 128))
    segk = jnp.broadcast_to(seg_own[None, :], (8, t_len))
    row_spec = lambda width: pl.BlockSpec((rows, width), lambda i, cp: (i, 0))
    full = lambda a: pl.BlockSpec(a.shape, lambda i, cp: (0,) * a.ndim, pipeline_mode=pl.Buffered(1))
    own_spec = pl.BlockSpec((1, rows, both), lambda i, cp: (cp[0], 0, 0), pipeline_mode=pl.Buffered(1))
    width = 2 * (qk + HEAD_DIM)
    return pl.pallas_call(
        attn_kernel,
        grid_spec=pltpu.PrefetchScalarGridSpec(
            num_scalar_prefetch=1,
            grid=(4,),
            in_specs=[own_spec] + [full(a) for a in n_got + g_got] + [full(wqkv), full(wo), row_spec(ROPE_DIMS), row_spec(ROPE_DIMS), full(cos_b), full(sin_b), row_spec(128), full(segk)],
            out_specs=pl.BlockSpec((t_len, width), lambda i, cp: (0, 0)),
            scratch_shapes=[
                pltpu.VMEM((rows, both // 2), BF16), pltpu.VMEM((rows, both // 2), BF16),
                pltpu.VMEM((N_HEADS, rows, HEAD_DIM), BF16), pltpu.VMEM((N_HEADS, rows, HEAD_DIM), BF16),
                pltpu.VMEM((t_len, HEAD_DIM), BF16), pltpu.VMEM((t_len, HEAD_DIM), BF16),
                pltpu.VMEM((HEAD_DIM, t_len), BF16), pltpu.VMEM((HEAD_DIM, t_len), BF16),
                pltpu.VMEM((rows, t_len), F32), pltpu.VMEM((rows, t_len), F32), pltpu.VMEM((rows, t_len), BF16),
                pltpu.VMEM((t_len, HEAD_DIM), F32), pltpu.VMEM((t_len, HEAD_DIM), F32)]),
        out_shape=jax.ShapeDtypeStruct((t_len, width), BF16),
        compiler_params=pltpu.CompilerParams(vmem_limit_bytes=62 * 1024 * 1024, dimension_semantics=('arbitrary',)),
        cost_estimate=pl.CostEstimate(flops=45_000_000_000, bytes_accessed=40_000_000, transcendentals=10_000_000),
        name='attn',
    )(cp_index[None], ng_blocks, *n_got, *g_got, wqkv, wo, cos_b, sin_b, cos_b, sin_b, segq, segk)


def norm_kernel(x_ref, g_ref, scale_ref, out_ref):
    d_model = x_ref.shape[1]
    for part in range(0, x_ref.shape[0], 128):
        sl = slice(part, part + 128)
        x_f = x_ref[sl, :].astype(F32)
        inv = lax.rsqrt(jnp.mean(x_f * x_f, axis=1, keepdims=True) + 1e-6)
        out_ref[sl, :d_model] = (x_f * inv * (1.0 + scale_ref[...])).astype(BF16)
        out_ref[sl, d_model:] = g_ref[sl, :]


def norm_and_grad(x_loc, g_loc, scale_f):
    t_len, d_model = x_loc.shape
    rows = 512
    tile = pl.BlockSpec((rows, d_model), lambda i: (i, 0))
    return pl.pallas_call(
        norm_kernel, grid=(t_len // rows,), name='norm',
        in_specs=[tile, tile, pl.BlockSpec(scale_f.shape, lambda i: (0, 0))],
        out_specs=pl.BlockSpec((rows, 2 * d_model), lambda i: (i, 0)),
        out_shape=jax.ShapeDtypeStruct((t_len, 2 * d_model), BF16),
        cost_estimate=pl.CostEstimate(flops=4_000_000_000, bytes_accessed=19_000_000, transcendentals=2048),
    )(x_loc, g_loc, scale_f)


N_PART = 3


def split_kernel(w1_ref, w2_ref, keep_ref, send_ref):
    core = lax.axis_index('core')
    d_model = keep_ref.shape[2] // 2
    sub = d_model // 8
    for part in range(N_PART):
        for i, w_ref in enumerate((w1_ref, w2_ref)):
            even, odd = [
                jnp.concatenate([w_ref[:, ((2 * j + k) * N_PART + part) * sub:((2 * j + k) * N_PART + part + 1) * sub] for j in range(8)], axis=1).astype(BF16)
                for k in range(2)]

            @pl.when(core == 0)
            def _():
                keep_ref[part, :, i * d_model:(i + 1) * d_model] = even
                send_ref[part, :, i * d_model:(i + 1) * d_model] = odd

            @pl.when(core == 1)
            def _():
                keep_ref[part, :, i * d_model:(i + 1) * d_model] = odd
                send_ref[part, :, i * d_model:(i + 1) * d_model] = even


def split_up(w1, w2):
    rows, cols = w1.shape
    out = jax.ShapeDtypeStruct((N_PART, rows, cols // N_PART), BF16)
    return pl.pallas_call(split_kernel, out_shape=[out, out], name='split_up')(w1, w2)


def stack_kernel(keep_ref, recv_ref, wd_ref, extra_ref, first_ref, rest_ref):
    core = lax.axis_index('core')
    rows, cols = keep_ref.shape[1:]
    d_model = wd_ref.shape[1]
    own = pl.multiple_of(core * rows, 8)
    oth = pl.multiple_of(rows - own, 8)
    for part in range(N_PART):
        out_ref, base = (first_ref, 0) if part == 0 else (rest_ref, (part - 1) * (cols + d_model))
        out_ref[pl.ds(own, rows), base:base + cols] = keep_ref[part]
        out_ref[pl.ds(oth, rows), base:base + cols] = recv_ref[part]
        out_ref[:, base + cols:base + cols + d_model] = wd_ref[part * 2 * rows:(part + 1) * 2 * rows, :].astype(BF16)
    n_extra = extra_ref.shape[0]
    first_ref[:n_extra, cols + d_model:] = extra_ref[...]
    first_ref[n_extra:, cols + d_model:] = jnp.zeros((2 * rows - n_extra, extra_ref.shape[1]), BF16)


def stack_up(keep, recv, w_down, extra):
    _, rows, cols = keep.shape
    width = cols + w_down.shape[1]
    outs = [jax.ShapeDtypeStruct((2 * rows, width + extra.shape[1]), BF16), jax.ShapeDtypeStruct((2 * rows, (N_PART - 1) * width), BF16)]
    return pl.pallas_call(stack_kernel, out_shape=outs, name='stack_up')(keep, recv, w_down, extra)


def unpack_kernel(own_ref, oth_ref, wqkv_ref, wo_ref):
    core = lax.axis_index('core')
    r_o, r_in = wo_ref.shape[0] // 16, wqkv_ref.shape[0] // 16
    d_model = wo_ref.shape[1]
    rows = own_ref.shape[0] // 8
    for chip in range(8):
        for flip, ref in enumerate((own_ref, oth_ref)):
            dev = 2 * chip + (core ^ flip)
            wo_ref[pl.ds(pl.multiple_of(dev * r_o, 8), r_o), :] = ref[chip * rows:chip * rows + r_o, :d_model]
            wqkv_ref[pl.ds(pl.multiple_of(dev * r_in, 8), r_in), :] = ref[chip * rows + r_o:chip * rows + r_o + r_in, :]


def unpack(own, oth, r_o, r_in, d_model):
    return pl.pallas_call(
        unpack_kernel, name='unpack',
        out_shape=[jax.ShapeDtypeStruct((16 * r_in, own.shape[1]), BF16), jax.ShapeDtypeStruct((16 * r_o, d_model), BF16)],
    )(own, oth)


def join_kernel(*refs):
    own_refs, recv_refs, (w1_ref, w2_ref, wd_ref) = refs[:N_PART], refs[N_PART:2 * N_PART], refs[2 * N_PART:]
    core = lax.axis_index('core')
    rows = w1_ref.shape[0]
    d_model = wd_ref.shape[1]
    sub = d_model // 8

    def put(even_of, odd_of):
        for i, w_ref in enumerate((w1_ref, w2_ref)):
            pieces = []
            for j in range(8):
                for of in (even_of, odd_of):
                    for part in range(N_PART):
                        pieces.append(of(part)[:, i * d_model + j * sub:i * d_model + (j + 1) * sub])
            w_ref[...] = jnp.concatenate(pieces, axis=1)

    pl.when(core == 0)(lambda: put(lambda p: own_refs[p][:rows, :2 * d_model], lambda p: recv_refs[p][...]))
    pl.when(core == 1)(lambda: put(lambda p: recv_refs[p][...], lambda p: own_refs[p][rows:, :2 * d_model]))
    for part in range(N_PART):
        wd_ref[part * 2 * rows:(part + 1) * 2 * rows, :] = own_refs[part][:, 2 * d_model:3 * d_model]


def join_up(owns, recvs):
    rows, cols = recvs[0].shape
    d_model = cols // 2
    up = jax.ShapeDtypeStruct((rows, N_PART * cols), F32)
    return pl.pallas_call(
        join_kernel, out_shape=[up, up, jax.ShapeDtypeStruct((N_PART * 2 * rows, d_model), F32)], name='join_up',
    )(*owns, *recvs)


GELU_C = 0.7978845608028654
GELU_A = 0.044715


def hidden_kernel(own_ref, oth_ref, w_ref, b1_ref, b2_ref, *refs):
    extra_refs = refs[:-10]
    act_ref, dh_ref, dw_ref, db_ref, h_s, da_s, ng_s, acc_s, side_s, sems = refs[-10:]
    step = pl.program_id(0)
    last = pl.num_programs(0) - 1
    rows, d_model = da_s.shape
    own = step < pl.num_programs(0) // 2
    ng_s[...] = jnp.where(own, own_ref[...], oth_ref[...])

    @pl.when(step == 0)
    def _():
        acc_s[...] = jnp.zeros_like(acc_s)
        db_ref[...] = jnp.zeros_like(db_ref)

    n_sub = 2
    sub = rows // n_sub
    w12 = w_ref[:, :2 * d_model]
    for i in range(n_sub):
        sl = slice(i * sub, (i + 1) * sub)
        h_s[sl, :] = dot_nn(ng_s[sl, :d_model], w12)
        da_s[sl, :] = dot_nt(ng_s[sl, d_model:], w_ref[:, 2 * d_model:])
    b1 = b1_ref[...]
    b2 = b2_ref[...]
    for i in range(n_sub):
        sl = slice(i * sub, (i + 1) * sub)
        s1 = None
        s2 = None
        for r in range(i * sub, (i + 1) * sub, 64):
            rs = slice(r, r + 64)
            u = h_s[rs, :d_model] + b1
            v = h_s[rs, d_model:] + b2
            da = da_s[rs, :]
            u2 = u * u
            t = jnp.tanh(u * (GELU_C + (GELU_C * GELU_A) * u2))
            half = 0.5 + 0.5 * t
            gelu = u * half
            slope = half + (half * (1.0 - t)) * (u * (GELU_C + (3.0 * GELU_C * GELU_A) * u2))
            d1 = da * v * slope
            d2 = da * gelu
            act_ref[rs, :] = (gelu * v).astype(BF16)
            dh_ref[rs, :d_model] = d1.astype(BF16)
            dh_ref[rs, d_model:] = d2.astype(BF16)
            p1 = jnp.sum(d1.reshape(8, 8, d_model), axis=0)
            p2 = jnp.sum(d2.reshape(8, 8, d_model), axis=0)
            s1 = p1 if s1 is None else s1 + p1
            s2 = p2 if s2 is None else s2 + p2
        db_ref[:8, :] += s1
        db_ref[8:, :] += s2
        acc_s[:, :2 * d_model] += dot_tn(ng_s[sl, :d_model], dh_ref[sl, :])
        acc_s[:, 2 * d_model:] += dot_tn(act_ref[sl, :], ng_s[sl, d_model:])

    if extra_refs:
        keep_ref, got_ref = extra_refs
        block = side_s.shape[1]
        n_extra = keep_ref.shape[1]
        slot = lax.rem(step, 2)

        def side_copy(at_slot, at_step):
            place = dw_ref.at[pl.ds(pl.multiple_of(at_step * block, 8), block), 3 * d_model:]
            return pltpu.make_async_copy(side_s.at[at_slot], place, sems.at[1 + at_slot])

        @pl.when(step >= 2)
        def _():
            side_copy(slot, step - 2).wait()

        side_s[slot, :n_extra, :] = keep_ref[0] + got_ref[0]
        side_s[slot, n_extra:, :] = jnp.zeros((block - n_extra, keep_ref.shape[2]), F32)
        side_copy(slot, step).start()

        @pl.when(step == last)
        def _():
            side_copy(1 - slot, step - 1).wait()
            side_copy(slot, step).wait()

    @pl.when(step == last)
    def _():
        copy = pltpu.make_async_copy(acc_s, dw_ref.at[:, :3 * d_model], sems.at[0])
        copy.start()
        copy.wait()


def hidden_part(ng_own, ng_oth, weight, b1, b2, extra=()):
    w_part, w_col = weight
    t_len, both = ng_own.shape
    d_model = both // 2
    rows = 512
    steps = 2 * t_len // rows
    half = steps // 2
    own_spec = pl.BlockSpec((rows, both), lambda i: (jnp.minimum(i, half - 1), 0))
    oth_spec = pl.BlockSpec((rows, both), lambda i: (jnp.maximum(i - half, 0), 0))
    full = lambda a, width, col=0: pl.BlockSpec((a.shape[0], width), lambda i: (0, col), pipeline_mode=pl.Buffered(1))
    row = lambda width: pl.BlockSpec((rows, width), lambda i: (i, 0))
    blk = [pl.BlockSpec((1,) + a.shape[1:], lambda i: (i, 0, 0)) for a in extra]
    side = (2, d_model // 8, extra[0].shape[2]) if extra else (2, 8, 128)
    return pl.pallas_call(
        hidden_kernel,
        grid=(steps,),
        in_specs=[own_spec, oth_spec, full(w_part, 3 * d_model, w_col), full(b1, d_model), full(b2, d_model)] + blk,
        out_specs=[row(d_model), row(2 * d_model), pl.BlockSpec(memory_space=pl.ANY), pl.BlockSpec((16, d_model), lambda i: (0, 0))],
        out_shape=[jax.ShapeDtypeStruct((2 * t_len, d_model), BF16), jax.ShapeDtypeStruct((2 * t_len, 2 * d_model), BF16),
                   jax.ShapeDtypeStruct((d_model, 3 * d_model + (extra[0].shape[2] if extra else 0)), F32), jax.ShapeDtypeStruct((16, d_model), F32)],
        scratch_shapes=[pltpu.VMEM((rows, 2 * d_model), F32), pltpu.VMEM((rows, d_model), F32), pltpu.VMEM((rows, both), BF16),
                        pltpu.VMEM((d_model, 3 * d_model), F32), pltpu.VMEM(side, F32), pltpu.SemaphoreType.DMA((3,))],
        compiler_params=pltpu.CompilerParams(vmem_limit_bytes=63 * 1024 * 1024, dimension_semantics=('arbitrary',)),
        cost_estimate=pl.CostEstimate(flops=65_000_000_000, bytes_accessed=70_000_000, transcendentals=4_700_000),
        name='hidden',
    )(ng_own, ng_oth, w_part, b1, b2, *extra)


def attn_grad_kernel(cp_ref, own_ref, n1_ref, n2_ref, n3_ref, g1_ref, g2_ref, g3_ref, dqkv_ref, o_lo_ref, o_hi_ref, keep_ref, send_ref):
    step = pl.program_id(0)
    core = lax.axis_index('core')
    d_model = own_ref.shape[2] // 2
    r_o, r_in = o_lo_ref.shape[1] // 8, d_model // 16
    width = dqkv_ref.shape[1]
    rows = own_ref.shape[1]
    place = [pl.ds(pl.multiple_of((cp_ref[0] ^ flip) * rows, rows), rows) for flip in range(4)]

    def put(at, cols, value_of):
        for dev in range(16):
            for ref, flip in ((keep_ref, 0), (send_ref, 1)):
                @pl.when((core ^ flip) == dev % 2)
                def _():
                    ref[dev // 2, at, cols] = value_of(dev)

    d_wqkv = dot_tn(own_ref[0, :, :d_model], dqkv_ref[place[0], :])
    for flip, n_ref in ((1, n1_ref), (2, n2_ref), (3, n3_ref)):
        d_wqkv = d_wqkv + dot_tn(n_ref[0], dqkv_ref[place[flip], :])
    put(slice(r_o, r_o + r_in), slice(0, width), lambda dev: d_wqkv[dev * r_in:(dev + 1) * r_in])

    def low(first_col, used):
        d_wo = []
        for o_ref in (o_lo_ref, o_hi_ref):
            total = dot_tn(o_ref[place[0], :], own_ref[0, :, d_model + first_col:d_model + first_col + used])
            for flip, g_ref in ((1, g1_ref), (2, g2_ref), (3, g3_ref)):
                total = total + dot_tn(o_ref[place[flip], :], g_ref[0, :, first_col:first_col + used])
            d_wo.append(total)
        put(slice(0, r_o), slice(0, used), lambda dev: d_wo[dev // 8][dev % 8 * r_o:(dev % 8 + 1) * r_o])
        if used < width:
            put(slice(0, r_o), slice(used, width), lambda dev: jnp.zeros((r_o, width - used), F32))

    for i in range(-(-d_model // width)):
        pl.when(step == i)(functools.partial(low, i * width, min(width, d_model - i * width)))


def attn_grad(cp_index, ng_blocks, n_got, g_got, od_seq, r_o, r_in):
    _, rows, both = ng_blocks.shape
    t_len = od_seq.shape[0]
    width = 512
    total = (N_HEADS + 2) * HEAD_DIM
    out = jax.ShapeDtypeStruct((8, r_o + r_in, total), F32)
    out_spec = pl.BlockSpec((8, r_o + r_in, width), lambda i, cp: (0, 0, i))
    one = pl.Buffered(1)
    full = lambda a: pl.BlockSpec(a.shape, lambda i, cp: (0, 0, 0), pipeline_mode=one)
    return pl.pallas_call(
        attn_grad_kernel,
        grid_spec=pltpu.PrefetchScalarGridSpec(
            num_scalar_prefetch=1,
            grid=(total // width,),
            in_specs=[pl.BlockSpec((1, rows, both), lambda i, cp: (cp[0], 0, 0), pipeline_mode=one)] + [full(a) for a in n_got + g_got]
                     + [pl.BlockSpec((t_len, width), lambda i, cp: (0, i)),
                        pl.BlockSpec((t_len, width), lambda i, cp: (0, total // width), pipeline_mode=one),
                        pl.BlockSpec((t_len, width), lambda i, cp: (0, total // width + 1), pipeline_mode=one)],
            out_specs=[out_spec, out_spec]),
        out_shape=[out, out],
        compiler_params=pltpu.CompilerParams(vmem_limit_bytes=60 * 1024 * 1024, dimension_semantics=('arbitrary',)),
        cost_estimate=pl.CostEstimate(flops=12_000_000_000, bytes_accessed=33_000_000, transcendentals=0),
        name='attn_grad',
    )(cp_index[None], ng_blocks, *n_got, *g_got, od_seq, od_seq, od_seq)


def fwd_product(act_refs, w_refs):
    out = dot_nn(act_refs[0][...], w_refs[0][...])
    for act_ref, w_ref in zip(act_refs[1:], w_refs[1:]):
        out = out + dot_nn(act_ref[...], w_ref[...])
    return out


def bwd_product(dh_refs, w_refs):
    out = dot_nt(dh_refs[0][...], w_refs[0][:, :dh_refs[0].shape[1]])
    for dh_ref, w_ref in zip(dh_refs[1:], w_refs[1:]):
        out = out + dot_nt(dh_ref[...], w_ref[:, :dh_ref.shape[1]])
    return out


def other_kernel(product, *refs):
    refs[-1][...] = product(refs[:N_PART], refs[N_PART:2 * N_PART])


OUT_ROWS = 256


def out_specs_of(width, weights, w_width, w_off, first_block):
    tile = pl.BlockSpec((OUT_ROWS, width), lambda i, *_: (i + first_block, 0))
    specs = [tile] * N_PART
    for array, col in weights:
        specs.append(pl.BlockSpec((array.shape[0], w_width), lambda i, *_, at=w_off(col): (0, at), pipeline_mode=pl.Buffered(1)))
    return specs


def out_other(parts, weights, product, w_width, w_off):
    t_len, width = parts[0].shape[0] // 2, parts[0].shape[1]
    d_model = weights[0][0].shape[0]
    return pl.pallas_call(
        functools.partial(other_kernel, product),
        grid=(t_len // OUT_ROWS,),
        in_specs=out_specs_of(width, weights, w_width, w_off, t_len // OUT_ROWS),
        out_specs=pl.BlockSpec((OUT_ROWS, d_model), lambda i: (i, 0)),
        out_shape=jax.ShapeDtypeStruct((t_len, d_model), F32),
        compiler_params=pltpu.CompilerParams(vmem_limit_bytes=60 * 1024 * 1024, dimension_semantics=('arbitrary',)),
        cost_estimate=pl.CostEstimate(flops=2 * t_len * d_model * width * N_PART, bytes_accessed=50_000_000, transcendentals=0),
    )(*parts, *[array for array, _ in weights])


def fwd_own_kernel(cp_ref, *refs):
    o_refs = refs[2 * N_PART:2 * N_PART + 8]
    wo_ref, x_ref, got_ref, bias_ref, out_ref, o_s = refs[2 * N_PART + 8:]
    flip = (pl.program_id(0) // 2) ^ cp_ref[0]
    half = o_s.shape[1] // 2
    for i in range(4):
        @pl.when(flip == i)
        def _():
            o_s[:, :half] = o_refs[2 * i][0]
            o_s[:, half:] = o_refs[2 * i + 1][0]
    out = fwd_product(refs[:N_PART], refs[N_PART:2 * N_PART]) + dot_nn(o_s[...], wo_ref[...])
    out_ref[...] = (x_ref[...].astype(F32) + out + got_ref[...] + bias_ref[...]).astype(BF16)


def bwd_own_kernel(cp_ref, *refs):
    d_refs = refs[2 * N_PART:2 * N_PART + 4]
    wqkv_ref, x_ref, g_ref, got_ref, scale_ref, d_x_ref, sums_ref, d_s = refs[2 * N_PART + 4:]
    flip = (pl.program_id(0) // 2) ^ cp_ref[0]
    for i in range(4):
        @pl.when(flip == i)
        def _():
            d_s[...] = d_refs[i][0]

    @pl.when(pl.program_id(0) == 0)
    def _():
        sums_ref[...] = jnp.zeros_like(sums_ref)

    d_n = bwd_product(refs[:N_PART], refs[N_PART:2 * N_PART]) + dot_nt(d_s[...], wqkv_ref[...]) + got_ref[...]
    x_f = x_ref[...].astype(F32)
    g_f = g_ref[...].astype(F32)
    inv = lax.rsqrt(jnp.mean(x_f * x_f, axis=1, keepdims=True) + 1e-6)
    scaled = d_n * (1.0 + scale_ref[...])
    xn = x_f * inv
    proj = jnp.mean(scaled * xn, axis=1, keepdims=True)
    d_x_ref[...] = (g_f + inv * (scaled - xn * proj)).astype(BF16)
    rows, d_model = x_f.shape
    sums_ref[:8, :] += jnp.sum((d_n * xn).reshape(rows // 8, 8, d_model), axis=0)
    sums_ref[8:, :] += jnp.sum(g_f.reshape(rows // 8, 8, d_model), axis=0)


def own_call(kernel, cp_index, parts, weights, w_width, w_off, od_blocks, od_got, od_cols, od_width, rest, rest_specs, out_specs, out_shape, scratch):
    t_len, width = parts[0].shape[0] // 2, parts[0].shape[1]
    specs = out_specs_of(width, weights, w_width, w_off, 0)
    args = list(parts) + [array for array, _ in weights]
    for i, source in enumerate([od_blocks] + od_got):
        for col in od_cols:
            if i == 0:
                specs.append(pl.BlockSpec((1, OUT_ROWS, od_width), lambda j, cp, col=col: (cp[0], j % 2, col)))
            else:
                specs.append(pl.BlockSpec((1, OUT_ROWS, od_width), lambda j, cp, col=col: (0, j % 2, col)))
            args.append(source)
    return pl.pallas_call(
        kernel,
        grid_spec=pltpu.PrefetchScalarGridSpec(
            num_scalar_prefetch=1, grid=(t_len // OUT_ROWS,), in_specs=specs + rest_specs, out_specs=out_specs, scratch_shapes=scratch),
        out_shape=out_shape,
        compiler_params=pltpu.CompilerParams(vmem_limit_bytes=62 * 1024 * 1024, dimension_semantics=('arbitrary',)),
        cost_estimate=pl.CostEstimate(flops=2 * t_len * weights[0][0].shape[0] * (width * N_PART + 1024), bytes_accessed=80_000_000, transcendentals=0),
    )(cp_index[None], *args, *rest)


def pack_kernel(wq_ref, wk_ref, wv_ref, wo_ref, out_ref):
    r_o, d_model = wo_ref.shape
    qk = wq_ref.shape[1]
    out_ref[:r_o, :d_model] = wo_ref[...].astype(BF16)
    out_ref[:r_o, d_model:] = jnp.zeros((r_o, out_ref.shape[1] - d_model), BF16)
    out_ref[r_o:, :qk] = wq_ref[...].astype(BF16)
    out_ref[r_o:, qk:qk + HEAD_DIM] = wk_ref[...].astype(BF16)
    out_ref[r_o:, qk + HEAD_DIM:] = wv_ref[...].astype(BF16)


def pack(w_q, w_k, w_v, w_o):
    out = jax.ShapeDtypeStruct((w_o.shape[0] + w_q.shape[0], w_q.shape[1] + 2 * HEAD_DIM), BF16)
    return pl.pallas_call(pack_kernel, out_shape=out, name='pack')(w_q, w_k, w_v, w_o)


def vector_kernel(scale_ref, bo_ref, bd_ref, b1_ref, b2_ref, out_ref, side_s):
    side_s[...] = jnp.zeros_like(side_s)
    for row, ref in enumerate((scale_ref, bo_ref, bd_ref, b1_ref, b2_ref)):
        side_s[row:row + 1, :ref.shape[1]] = ref[...]
    out_ref[...] = side_s[...].astype(BF16)


def vectors(*parts):
    width = -(-max(part.shape[0] for part in parts) // 128) * 128
    return pl.pallas_call(
        vector_kernel, out_shape=jax.ShapeDtypeStruct((8, width), BF16), scratch_shapes=[pltpu.VMEM((8, width), F32)], name='vectors',
    )(*[part[None] for part in parts])


def solution(mesh):
    mesh4 = Mesh(mesh.devices.reshape(2, 2, 2, 2), ALL_AXES)
    tok_spec = P(('x', 'core'), ('z', 'y'), None)
    pos_spec = P(('x', 'core'), ('z', 'y'))
    vec_spec = P(ALL_AXES)
    mat_spec = P(ALL_AXES, None)
    param_specs = (vec_spec, mat_spec, mat_spec, mat_spec, mat_spec, vec_spec, mat_spec, vec_spec, mat_spec, vec_spec, mat_spec, vec_spec)

    def swap_core(values):
        return lax.ppermute(values, 'core', [(0, 1), (1, 0)])

    def send_blocks(values, cp_index, width=None):
        got = []
        for flip in (1, 2, 3):
            sent = lax.dynamic_index_in_dim(values, cp_index ^ flip, 0, keepdims=True)[..., :width]
            got.append(lax.ppermute(sent, ('z', 'y'), [(i, i ^ flip) for i in range(4)]))
        return got

    def local_step(x_in, grad_out, seg_id, seg_pos, norm_scale, w_q, w_k, w_v, w_o, b_o, w_up1, b_up1, w_up2, b_up2, w_down, b_down):
        n_seq, piece, d_model = x_in.shape
        t_len = n_seq * piece
        core = lax.axis_index('core')
        cp_index = lax.axis_index('z') * 2 + lax.axis_index('y')
        first = core == 0
        r_in = w_q.shape[0]
        r_o = w_o.shape[0]
        f_blk = b_up1.shape[0]
        sub = f_blk // N_PART
        qk = N_HEADS * HEAD_DIM

        def after(value, *deps):
            return lax.optimization_barrier((value,) + deps)[0]

        seg_pack = jnp.stack([seg_id, seg_pos], axis=1)
        seg_got = send_blocks(seg_pack, cp_index)
        g_got = send_blocks(grad_out, cp_index)

        keep, send = split_up(w_up1, w_up2)
        shards = stack_up(keep, swap_core(send), w_down, pack(w_q, w_k, w_v, w_o))

        def gather(shard):
            return lax.all_gather(shard, CHIPS, axis=0, tiled=True)

        whole = [gather(shards[0]), gather(shards[1])]
        weights = [(whole[0], 0), (whole[1], 0), (whole[1], 1)]

        vec_all = lax.all_gather(vectors(norm_scale, b_o, b_down, b_up1, b_up2), ALL_AXES, axis=0)
        scale_f, bo_f, bd_f = [vec_all[:, i, :r_in].reshape(1, d_model).astype(F32) for i in range(3)]
        b_ups = []
        for row in (3, 4):
            both = vec_all[:, row, :f_blk].reshape(8, 2, N_PART, sub)
            mine = jnp.where(first, both[:, 0], both[:, 1]).astype(F32)
            b_ups.append([mine[:, part].reshape(1, d_model) for part in range(N_PART)])

        x_loc = x_in.reshape(t_len, d_model)
        ng_own = norm_and_grad(x_loc, grad_out.reshape(t_len, d_model), scale_f)
        ng_oth = swap_core(ng_own)
        ng_blocks = ng_own.reshape(n_seq, piece, 2 * d_model)
        n_got = send_blocks(ng_blocks, cp_index, d_model)

        seg_all = jnp.zeros_like(seg_pack)
        for flip, got in enumerate([lax.dynamic_index_in_dim(seg_pack, cp_index, 0, keepdims=True)] + seg_got):
            seg_all = lax.dynamic_update_slice_in_dim(seg_all, got, cp_index ^ flip, 0)
        seg_own = seg_all[:, 0].reshape(t_len)
        pos_own = seg_all[:, 1].reshape(t_len)
        half = ROPE_DIMS // 2
        inv_freq = 10000.0 ** (-jnp.arange(half, dtype=F32) / half)
        angle = pos_own.astype(F32)[:, None] * inv_freq
        cos_a = jnp.cos(angle)
        sin_a = jnp.sin(angle)
        cos_b = jnp.concatenate([cos_a, cos_a], axis=1)
        sin_b = jnp.concatenate([-sin_a, sin_a], axis=1)

        acts, dhs, dbs, owns, recvs = [], [], [], [], []

        def third(part, ng_in, extra=()):
            act, dh, d_w, db = hidden_part(ng_in, ng_oth, weights[part], b_ups[0][part], b_ups[1][part], extra)
            own = lax.psum_scatter(d_w, CHIPS, scatter_dimension=0, tiled=True)
            recvs.append(swap_core(jnp.where(first, own[r_in:, :2 * d_model], own[:r_in, :2 * d_model])))
            acts.append(act)
            dhs.append(dh)
            dbs.append(jnp.sum(db.reshape(2, 8, d_model), axis=1).reshape(2, 8, sub))
            owns.append(own)

        third(0, ng_own)
        extra_own = whole[0][:, 3 * d_model:]
        wqkv, wo = unpack(extra_own, swap_core(extra_own), r_o, r_in, d_model)
        od_seq = attention(cp_index, after(ng_blocks, dbs[0]), n_got, g_got, wqkv, wo, cos_b, sin_b, seg_own)
        d_keep, d_send = attn_grad(cp_index, ng_blocks, n_got, g_got, od_seq, r_o, r_in)
        od_blocks = od_seq.reshape(n_seq, piece, -1)
        od_got = send_blocks(od_blocks, cp_index)
        third(1, ng_own, (d_keep, swap_core(d_send)))
        third(2, after(ng_own, dbs[1]))

        wd_off = lambda col: 3 * col + 2
        w12_off = lambda col: col
        tile = lambda width, col=0: pl.BlockSpec((OUT_ROWS, width), lambda i, *_: (i, col))
        full = lambda a: pl.BlockSpec(a.shape, lambda i, *_: (0, 0), pipeline_mode=pl.Buffered(1))
        out_oth = out_other(acts, weights, fwd_product, d_model, wd_off)
        dn_oth = out_other(after(tuple(dhs), out_oth), weights, bwd_product, 3 * d_model, w12_off)
        bias_f = bo_f + bd_f
        x_out = own_call(fwd_own_kernel, cp_index, after(tuple(acts), dn_oth), weights, d_model, wd_off, od_blocks, od_got, (3, 4), 512,
                         [wo, x_loc, swap_core(out_oth), bias_f], [full(wo), tile(d_model), tile(d_model), full(bias_f)],
                         tile(d_model), jax.ShapeDtypeStruct((t_len, d_model), BF16), [pltpu.VMEM((OUT_ROWS, qk), BF16)])
        d_x, sums = own_call(bwd_own_kernel, cp_index, after(tuple(dhs), x_out), weights, 3 * d_model, w12_off, od_blocks, od_got, (0,), qk + 2 * HEAD_DIM,
                             [wqkv, x_loc, ng_own, swap_core(dn_oth), scale_f],
                             [full(wqkv), tile(d_model), tile(d_model, 1), tile(d_model), full(scale_f)],
                             [tile(d_model), pl.BlockSpec((16, d_model), lambda i, *_: (0, 0))],
                             [jax.ShapeDtypeStruct((t_len, d_model), BF16), jax.ShapeDtypeStruct((16, d_model), F32)],
                             [pltpu.VMEM((OUT_ROWS, qk + 2 * HEAD_DIM), BF16)])
        x_out = x_out.reshape(n_seq, piece, d_model)
        d_x = d_x.reshape(n_seq, piece, d_model)

        sums = jnp.sum(sums.reshape(2, 8, d_model), axis=1).reshape(2, 16, r_in)
        db = jnp.stack(dbs, axis=2).reshape(2, 8, f_blk)
        zero = jnp.zeros_like(db)
        db = jnp.where(first, jnp.stack([db, zero], axis=2), jnp.stack([zero, db], axis=2)).reshape(2, 16, f_blk)
        small = jnp.concatenate([sums[0], sums[1], db[0], db[1]], axis=1)
        small = lax.psum(small, ALL_AXES)
        small = lax.dynamic_index_in_dim(small, lax.axis_index(ALL_AXES), 0, keepdims=False)
        g_scale, g_bias, g_b1, g_b2 = small[:r_in], small[r_in:2 * r_in], small[2 * r_in:2 * r_in + f_blk], small[2 * r_in + f_blk:]

        g_w1, g_w2, g_wd = join_up(owns, recvs)
        g_attn = owns[1][:r_o + r_in, 3 * d_model:]
        g_wo, g_wq, g_wk, g_wv = g_attn[:r_o, :d_model], g_attn[r_o:, :qk], g_attn[r_o:, qk:qk + HEAD_DIM], g_attn[r_o:, qk + HEAD_DIM:]
        return (x_out, d_x, g_scale, g_wq, g_wk, g_wv, g_wo, g_bias, g_w1, g_b1, g_w2, g_b2, g_wd, g_bias)

    in_specs = (tok_spec, tok_spec, pos_spec, pos_spec) + param_specs
    out_specs = (tok_spec, tok_spec) + param_specs
    return jax.shard_map(local_step, mesh=mesh4, in_specs=in_specs, out_specs=out_specs, check_vma=False)
```

```python
import functools
import jax
import jax.numpy as jnp
from jax import lax
from jax.experimental import pallas as pl
from jax.experimental.pallas import tpu as pltpu
from jax.sharding import Mesh, PartitionSpec as P


ROPE_DIMS = 128
HEAD_DIM = 256
N_HEADS = 4
MASKED = -1.6e31
EXP_SCALE = 1.4426950408889634 / 16.0
CHIPS = ('z', 'y', 'x')
ALL_AXES = ('z', 'y', 'x', 'core')
F32 = jnp.float32
BF16 = jnp.bfloat16


def dot_nn(a, b):
    return lax.dot_general(a, b, (((1,), (0,)), ((), ())), preferred_element_type=F32)


def dot_nt(a, b):
    return lax.dot_general(a, b, (((1,), (1,)), ((), ())), preferred_element_type=F32)


def dot_tn(a, b):
    return lax.dot_general(a, b, (((0,), (0,)), ((), ())), preferred_element_type=F32)


def rotate(values, cos_b, sin_b):
    return values * cos_b + pltpu.roll(values, ROPE_DIMS // 2, axis=1) * sin_b


def attn_kernel(cp_ref, own_ref, n1_ref, n2_ref, n3_ref, g1_ref, g2_ref, g3_ref, wqkv_ref, wo_ref, cos_ref, sin_ref, cosk_ref, sink_ref, segq_ref, segk_ref, out_ref,
                n_buf, g_buf, sems, q_s, do_s, k_s, v_s, kt_s, vt_s, mask_s, s_s, p_s, dk_s, dv_s):
    step = pl.program_id(0)
    n_blocks = pl.num_programs(0)
    rows, d_model = n_buf.shape[1:]
    qk = N_HEADS * HEAD_DIM
    base = pl.multiple_of(step * rows, rows)
    cos_b = cos_ref[...]
    sin_b = sin_ref[...]
    slot = lax.rem(step, 2)

    def fetch(at_step):
        flip = at_step ^ cp_ref[0]
        to = lax.rem(at_step, 2)
        own = own_ref.at[cp_ref[0]]
        sources = ((own.at[:, :d_model], own.at[:, d_model:]), (n1_ref.at[0], g1_ref.at[0]), (n2_ref.at[0], g2_ref.at[0]), (n3_ref.at[0], g3_ref.at[0]))
        for i, (n_src, g_src) in enumerate(sources):
            @pl.when(flip == i)
            def _():
                pltpu.make_async_copy(n_src, n_buf.at[to], sems.at[0, to]).start()
                pltpu.make_async_copy(g_src, g_buf.at[to], sems.at[1, to]).start()

    pl.when(step == 0)(lambda: fetch(step))
    pl.when(step + 1 < n_blocks)(lambda: fetch(step + 1))
    pltpu.make_async_copy(n1_ref.at[0], n_buf.at[slot], sems.at[0, slot]).wait()
    pltpu.make_async_copy(g1_ref.at[0], g_buf.at[slot], sems.at[1, slot]).wait()
    n_blk = n_buf[slot]
    g_blk = g_buf[slot]

    @pl.when(step == 0)
    def _():
        dk_s[...] = jnp.zeros_like(dk_s)
        dv_s[...] = jnp.zeros_like(dv_s)

    for h in range(N_HEADS):
        lin = dot_nn(n_blk, wqkv_ref[:, h * HEAD_DIM:(h + 1) * HEAD_DIM])
        q_s[h, :, :ROPE_DIMS] = rotate(lin[:, :ROPE_DIMS], cos_b, sin_b).astype(BF16)
        q_s[h, :, ROPE_DIMS:] = lin[:, ROPE_DIMS:].astype(BF16)
        do_s[h] = dot_nt(g_blk, wo_ref[h * HEAD_DIM:(h + 1) * HEAD_DIM, :]).astype(BF16)
    k_lin = dot_nn(n_blk, wqkv_ref[:, qk:qk + HEAD_DIM])
    k_blk = jnp.concatenate([rotate(k_lin[:, :ROPE_DIMS], cos_b, sin_b), k_lin[:, ROPE_DIMS:]], axis=1)
    v_blk = dot_nn(n_blk, wqkv_ref[:, qk + HEAD_DIM:])
    k_s[pl.ds(base, rows), :] = k_blk.astype(BF16)
    v_s[pl.ds(base, rows), :] = v_blk.astype(BF16)
    kt_s[:, pl.ds(base, rows)] = k_blk.T.astype(BF16)
    vt_s[:, pl.ds(base, rows)] = v_blk.T.astype(BF16)

    def block(blk):
        n_chunk = blk + 1
        seg_q = segq_ref[:, :1]
        for c in range(n_chunk):
            same = seg_q == segk_ref[:1, c * rows:(c + 1) * rows]
            if c == blk:
                r_id = lax.broadcasted_iota(jnp.int32, (rows, rows), 0)
                c_id = lax.broadcasted_iota(jnp.int32, (rows, rows), 1)
                same = same & (c_id <= r_id)
            mask_s[:, c * rows:(c + 1) * rows] = jnp.where(same, 1.0, 0.0)

        def head(h, carry):
            q = q_s[h]
            do = do_s[h]
            m_run = None
            for c in range(n_chunk):
                sl = slice(c * rows, (c + 1) * rows)
                s = jnp.where(mask_s[:, sl] > 0.5, dot_nn(q, kt_s[:, sl]), MASKED)
                s_s[:, sl] = s
                m_c = jnp.max(s, axis=1, keepdims=True)
                m_run = m_c if m_run is None else jnp.maximum(m_run, m_c)
            l_run = None
            for c in range(n_chunk):
                sl = slice(c * rows, (c + 1) * rows)
                e = jnp.exp2((s_s[:, sl] - m_run) * EXP_SCALE)
                s_s[:, sl] = e
                l_c = jnp.sum(e, axis=1, keepdims=True)
                l_run = l_c if l_run is None else l_run + l_c
            inv = 1.0 / l_run
            for c in range(n_chunk):
                sl = slice(c * rows, (c + 1) * rows)
                p = s_s[:, sl] * inv
                s_s[:, sl] = p
                p_s[:, sl] = p.astype(BF16)
            o = dot_nn(p_s[:, :n_chunk * rows], v_s[:n_chunk * rows, :])
            delta = jnp.sum(o * do.astype(F32), axis=1, keepdims=True)
            out_ref[pl.ds(base, rows), pl.ds(pl.multiple_of(qk + 2 * HEAD_DIM + h * HEAD_DIM, HEAD_DIM), HEAD_DIM)] = o.astype(BF16)
            dq = None
            for c in range(n_chunk):
                sl = slice(c * rows, (c + 1) * rows)
                ds = (s_s[:, sl] * (dot_nn(do, vt_s[:, sl]) - delta)).astype(BF16)
                dq_c = dot_nn(ds, k_s[sl, :])
                dq = dq_c if dq is None else dq + dq_c
                dk_s[sl, :] += dot_tn(ds, q)
                dv_s[sl, :] += dot_tn(p_s[:, sl], do)
            dq = dq * 0.0625
            dq = jnp.concatenate([rotate(dq[:, :ROPE_DIMS], cos_b, -sin_b), dq[:, ROPE_DIMS:]], axis=1)
            out_ref[pl.ds(base, rows), pl.ds(pl.multiple_of(h * HEAD_DIM, HEAD_DIM), HEAD_DIM)] = dq.astype(BF16)
            return carry

        lax.fori_loop(0, N_HEADS, head, 0)

    for blk in range(4):
        pl.when(step == blk)(functools.partial(block, blk))

    @pl.when(step == n_blocks - 1)
    def _():
        dk = dk_s[...] * 0.0625
        dk = jnp.concatenate([rotate(dk[:, :ROPE_DIMS], cosk_ref[...], -sink_ref[...]), dk[:, ROPE_DIMS:]], axis=1)
        out_ref[:, qk:qk + HEAD_DIM] = dk.astype(BF16)
        out_ref[:, qk + HEAD_DIM:qk + 2 * HEAD_DIM] = dv_s[...].astype(BF16)


def attention(cp_index, ng_blocks, n_got, g_got, wqkv, wo, cos_b, sin_b, seg_own):
    _, rows, both = ng_blocks.shape
    t_len = 4 * rows
    qk = N_HEADS * HEAD_DIM
    segq = jnp.broadcast_to(seg_own[:, None], (t_len, 128))
    segk = jnp.broadcast_to(seg_own[None, :], (8, t_len))
    row_spec = lambda width: pl.BlockSpec((rows, width), lambda i, cp: (i, 0))
    full = lambda a: pl.BlockSpec(a.shape, lambda i, cp: (0,) * a.ndim, pipeline_mode=pl.Buffered(1))
    anywhere = pl.BlockSpec(memory_space=pl.ANY)
    width = 2 * (qk + HEAD_DIM)
    return pl.pallas_call(
        attn_kernel,
        grid_spec=pltpu.PrefetchScalarGridSpec(
            num_scalar_prefetch=1,
            grid=(4,),
            in_specs=[anywhere] * 7 + [full(wqkv), full(wo), row_spec(ROPE_DIMS), row_spec(ROPE_DIMS), full(cos_b), full(sin_b), row_spec(128), full(segk)],
            out_specs=pl.BlockSpec((t_len, width), lambda i, cp: (0, 0)),
            scratch_shapes=[
                pltpu.VMEM((2, rows, both // 2), BF16), pltpu.VMEM((2, rows, both // 2), BF16), pltpu.SemaphoreType.DMA((2, 2)),
                pltpu.VMEM((N_HEADS, rows, HEAD_DIM), BF16), pltpu.VMEM((N_HEADS, rows, HEAD_DIM), BF16),
                pltpu.VMEM((t_len, HEAD_DIM), BF16), pltpu.VMEM((t_len, HEAD_DIM), BF16),
                pltpu.VMEM((HEAD_DIM, t_len), BF16), pltpu.VMEM((HEAD_DIM, t_len), BF16),
                pltpu.VMEM((rows, t_len), F32), pltpu.VMEM((rows, t_len), F32), pltpu.VMEM((rows, t_len), BF16),
                pltpu.VMEM((t_len, HEAD_DIM), F32), pltpu.VMEM((t_len, HEAD_DIM), F32)]),
        out_shape=jax.ShapeDtypeStruct((t_len, width), BF16),
        compiler_params=pltpu.CompilerParams(vmem_limit_bytes=62 * 1024 * 1024, dimension_semantics=('arbitrary',)),
        cost_estimate=pl.CostEstimate(flops=45_000_000_000, bytes_accessed=40_000_000, transcendentals=10_000_000),
        name='attn',
    )(cp_index[None], ng_blocks, *n_got, *g_got, wqkv, wo, cos_b, sin_b, cos_b, sin_b, segq, segk)


def norm_kernel(x_ref, g_ref, scale_ref, out_ref):
    d_model = x_ref.shape[1]
    for part in range(0, x_ref.shape[0], 128):
        sl = slice(part, part + 128)
        x_f = x_ref[sl, :].astype(F32)
        inv = lax.rsqrt(jnp.mean(x_f * x_f, axis=1, keepdims=True) + 1e-6)
        out_ref[sl, :d_model] = (x_f * inv * (1.0 + scale_ref[...])).astype(BF16)
        out_ref[sl, d_model:] = g_ref[sl, :]


def norm_and_grad(x_loc, g_loc, scale_f):
    t_len, d_model = x_loc.shape
    rows = 512
    tile = pl.BlockSpec((rows, d_model), lambda i: (i, 0))
    return pl.pallas_call(
        norm_kernel, grid=(t_len // rows,), name='norm',
        in_specs=[tile, tile, pl.BlockSpec(scale_f.shape, lambda i: (0, 0))],
        out_specs=pl.BlockSpec((rows, 2 * d_model), lambda i: (i, 0)),
        out_shape=jax.ShapeDtypeStruct((t_len, 2 * d_model), BF16),
        cost_estimate=pl.CostEstimate(flops=4_000_000_000, bytes_accessed=19_000_000, transcendentals=2048),
    )(x_loc, g_loc, scale_f)


N_PART = 3


def split_kernel(w1_ref, w2_ref, keep_ref, send_ref):
    core = lax.axis_index('core')
    d_model = keep_ref.shape[2] // 2
    sub = d_model // 8
    for part in range(N_PART):
        for i, w_ref in enumerate((w1_ref, w2_ref)):
            even, odd = [
                jnp.concatenate([w_ref[:, ((2 * j + k) * N_PART + part) * sub:((2 * j + k) * N_PART + part + 1) * sub] for j in range(8)], axis=1).astype(BF16)
                for k in range(2)]

            @pl.when(core == 0)
            def _():
                keep_ref[part, :, i * d_model:(i + 1) * d_model] = even
                send_ref[part, :, i * d_model:(i + 1) * d_model] = odd

            @pl.when(core == 1)
            def _():
                keep_ref[part, :, i * d_model:(i + 1) * d_model] = odd
                send_ref[part, :, i * d_model:(i + 1) * d_model] = even


def split_up(w1, w2):
    rows, cols = w1.shape
    out = jax.ShapeDtypeStruct((N_PART, rows, cols // N_PART), BF16)
    return pl.pallas_call(split_kernel, out_shape=[out, out], name='split_up')(w1, w2)


def stack_kernel(keep_ref, recv_ref, wd_ref, extra_ref, first_ref, rest_ref):
    core = lax.axis_index('core')
    rows, cols = keep_ref.shape[1:]
    d_model = wd_ref.shape[1]
    own = pl.multiple_of(core * rows, 8)
    oth = pl.multiple_of(rows - own, 8)
    for part in range(N_PART):
        out_ref, base = (first_ref, 0) if part == 0 else (rest_ref, (part - 1) * (cols + d_model))
        out_ref[pl.ds(own, rows), base:base + cols] = keep_ref[part]
        out_ref[pl.ds(oth, rows), base:base + cols] = recv_ref[part]
        out_ref[:, base + cols:base + cols + d_model] = wd_ref[part * 2 * rows:(part + 1) * 2 * rows, :].astype(BF16)
    n_extra = extra_ref.shape[0]
    first_ref[:n_extra, cols + d_model:] = extra_ref[...]
    first_ref[n_extra:, cols + d_model:] = jnp.zeros((2 * rows - n_extra, extra_ref.shape[1]), BF16)


def stack_up(keep, recv, w_down, extra):
    _, rows, cols = keep.shape
    width = cols + w_down.shape[1]
    outs = [jax.ShapeDtypeStruct((2 * rows, width + extra.shape[1]), BF16), jax.ShapeDtypeStruct((2 * rows, (N_PART - 1) * width), BF16)]
    return pl.pallas_call(stack_kernel, out_shape=outs, name='stack_up')(keep, recv, w_down, extra)


def unpack_kernel(own_ref, oth_ref, wqkv_ref, wo_ref):
    core = lax.axis_index('core')
    r_o, r_in = wo_ref.shape[0] // 16, wqkv_ref.shape[0] // 16
    d_model = wo_ref.shape[1]
    rows = own_ref.shape[0] // 8
    for chip in range(8):
        for flip, ref in enumerate((own_ref, oth_ref)):
            dev = 2 * chip + (core ^ flip)
            wo_ref[pl.ds(pl.multiple_of(dev * r_o, 8), r_o), :] = ref[chip * rows:chip * rows + r_o, :d_model]
            wqkv_ref[pl.ds(pl.multiple_of(dev * r_in, 8), r_in), :] = ref[chip * rows + r_o:chip * rows + r_o + r_in, :]


def unpack(own, oth, r_o, r_in, d_model):
    return pl.pallas_call(
        unpack_kernel, name='unpack',
        out_shape=[jax.ShapeDtypeStruct((16 * r_in, own.shape[1]), BF16), jax.ShapeDtypeStruct((16 * r_o, d_model), BF16)],
    )(own, oth)


def join_kernel(*refs):
    own_refs, recv_refs, (w1_ref, w2_ref, wd_ref) = refs[:N_PART], refs[N_PART:2 * N_PART], refs[2 * N_PART:]
    core = lax.axis_index('core')
    rows = w1_ref.shape[0]
    d_model = wd_ref.shape[1]
    sub = d_model // 8

    def put(even_of, odd_of):
        for i, w_ref in enumerate((w1_ref, w2_ref)):
            pieces = []
            for j in range(8):
                for of in (even_of, odd_of):
                    for part in range(N_PART):
                        pieces.append(of(part)[:, i * d_model + j * sub:i * d_model + (j + 1) * sub])
            w_ref[...] = jnp.concatenate(pieces, axis=1)

    pl.when(core == 0)(lambda: put(lambda p: own_refs[p][:rows, :2 * d_model], lambda p: recv_refs[p][...]))
    pl.when(core == 1)(lambda: put(lambda p: recv_refs[p][...], lambda p: own_refs[p][rows:, :2 * d_model]))
    for part in range(N_PART):
        wd_ref[part * 2 * rows:(part + 1) * 2 * rows, :] = own_refs[part][:, 2 * d_model:3 * d_model]


def join_up(owns, recvs):
    rows, cols = recvs[0].shape
    d_model = cols // 2
    up = jax.ShapeDtypeStruct((rows, N_PART * cols), F32)
    return pl.pallas_call(
        join_kernel, out_shape=[up, up, jax.ShapeDtypeStruct((N_PART * 2 * rows, d_model), F32)], name='join_up',
    )(*owns, *recvs)


GELU_C = 0.7978845608028654
GELU_A = 0.044715


def hidden_kernel(mode, own_ref, oth_ref, w_ref, b1_ref, b2_ref, *refs):
    extra_refs = refs[:2] if mode == 'extra' else ()
    act_ref, dh_ref, *dw_refs, db_ref, h_s, da_s, ng_s, acc_s, side_s, sems = refs[len(extra_refs):]
    dw_ref = dw_refs[0]
    step = pl.program_id(0)
    last = pl.num_programs(0) - 1
    rows, d_model = da_s.shape
    own = step < pl.num_programs(0) // 2
    ng_s[...] = jnp.where(own, own_ref[...], oth_ref[...])

    @pl.when(step == 0)
    def _():
        acc_s[...] = jnp.zeros_like(acc_s)
        db_ref[...] = jnp.zeros_like(db_ref)

    n_sub = 2
    sub = rows // n_sub
    w12 = w_ref[:, :2 * d_model]
    for i in range(n_sub):
        sl = slice(i * sub, (i + 1) * sub)
        h_s[sl, :] = dot_nn(ng_s[sl, :d_model], w12)
        da_s[sl, :] = dot_nt(ng_s[sl, d_model:], w_ref[:, 2 * d_model:])
    b1 = b1_ref[...]
    b2 = b2_ref[...]
    for i in range(n_sub):
        sl = slice(i * sub, (i + 1) * sub)
        s1 = None
        s2 = None
        for r in range(i * sub, (i + 1) * sub, 64):
            rs = slice(r, r + 64)
            u = h_s[rs, :d_model] + b1
            v = h_s[rs, d_model:] + b2
            da = da_s[rs, :]
            u2 = u * u
            t = jnp.tanh(u * (GELU_C + (GELU_C * GELU_A) * u2))
            half = 0.5 + 0.5 * t
            gelu = u * half
            slope = half + (half * (1.0 - t)) * (u * (GELU_C + (3.0 * GELU_C * GELU_A) * u2))
            d1 = da * v * slope
            d2 = da * gelu
            act_ref[rs, :] = (gelu * v).astype(BF16)
            dh_ref[rs, :d_model] = d1.astype(BF16)
            dh_ref[rs, d_model:] = d2.astype(BF16)
            p1 = jnp.sum(d1.reshape(8, 8, d_model), axis=0)
            p2 = jnp.sum(d2.reshape(8, 8, d_model), axis=0)
            s1 = p1 if s1 is None else s1 + p1
            s2 = p2 if s2 is None else s2 + p2
        db_ref[:8, :] += s1
        db_ref[8:, :] += s2
        acc_s[:, :2 * d_model] += dot_tn(ng_s[sl, :d_model], dh_ref[sl, :])
        acc_s[:, 2 * d_model:] += dot_tn(act_ref[sl, :], ng_s[sl, d_model:])

    if extra_refs:
        keep_ref, got_ref = extra_refs
        block = side_s.shape[1]
        n_extra = keep_ref.shape[1]
        slot = lax.rem(step, 2)

        def side_copy(at_slot, at_step):
            place = dw_ref.at[pl.ds(pl.multiple_of(at_step * block, 8), block), 3 * d_model:]
            return pltpu.make_async_copy(side_s.at[at_slot], place, sems.at[1 + at_slot])

        @pl.when(step >= 2)
        def _():
            side_copy(slot, step - 2).wait()

        side_s[slot, :n_extra, :] = keep_ref[0] + got_ref[0]
        side_s[slot, n_extra:, :] = jnp.zeros((block - n_extra, keep_ref.shape[2]), F32)
        side_copy(slot, step).start()

        @pl.when(step == last)
        def _():
            side_copy(1 - slot, step - 1).wait()
            side_copy(slot, step).wait()

    @pl.when(step == last)
    def _():
        if mode != 'halves':
            copy = pltpu.make_async_copy(acc_s, dw_ref.at[:, :3 * d_model], sems.at[0])
            copy.start()
            copy.wait()
            return
        x_index = lax.axis_index('x')
        block = d_model // 8

        def each(act):
            for chip in range(8):
                for ref, flip in zip(dw_refs, (0, 1)):
                    @pl.when((x_index ^ flip) == chip % 2)
                    def _():
                        act(pltpu.make_async_copy(acc_s.at[chip * block:(chip + 1) * block, :], ref.at[chip // 2], sems.at[0]))

        each(lambda copy: copy.start())
        each(lambda copy: copy.wait())


def hidden_part(ng_own, ng_oth, weight, b1, b2, extra=(), halves=False):
    w_part, w_col = weight
    t_len, both = ng_own.shape
    d_model = both // 2
    rows = 512
    steps = 2 * t_len // rows
    half = steps // 2
    own_spec = pl.BlockSpec((rows, both), lambda i: (jnp.minimum(i, half - 1), 0))
    oth_spec = pl.BlockSpec((rows, both), lambda i: (jnp.maximum(i - half, 0), 0))
    full = lambda a, width, col=0: pl.BlockSpec((a.shape[0], width), lambda i: (0, col), pipeline_mode=pl.Buffered(1))
    row = lambda width: pl.BlockSpec((rows, width), lambda i: (i, 0))
    blk = [pl.BlockSpec((1,) + a.shape[1:], lambda i: (i, 0, 0)) for a in extra]
    side = (2, d_model // 8, extra[0].shape[2]) if extra else (2, 8, 128)
    mode = 'halves' if halves else 'extra' if extra else 'plain'
    if halves:
        grads = [jax.ShapeDtypeStruct((4, d_model // 8, 3 * d_model), F32)] * 2
    else:
        grads = [jax.ShapeDtypeStruct((d_model, 3 * d_model + (extra[0].shape[2] if extra else 0)), F32)]
    return pl.pallas_call(
        functools.partial(hidden_kernel, mode),
        grid=(steps,),
        in_specs=[own_spec, oth_spec, full(w_part, 3 * d_model, w_col), full(b1, d_model), full(b2, d_model)] + blk,
        out_specs=[row(d_model), row(2 * d_model)] + [pl.BlockSpec(memory_space=pl.ANY)] * len(grads) + [pl.BlockSpec((16, d_model), lambda i: (0, 0))],
        out_shape=[jax.ShapeDtypeStruct((2 * t_len, d_model), BF16), jax.ShapeDtypeStruct((2 * t_len, 2 * d_model), BF16),
                   *grads, jax.ShapeDtypeStruct((16, d_model), F32)],
        scratch_shapes=[pltpu.VMEM((rows, 2 * d_model), F32), pltpu.VMEM((rows, d_model), F32), pltpu.VMEM((rows, both), BF16),
                        pltpu.VMEM((d_model, 3 * d_model), F32), pltpu.VMEM(side, F32), pltpu.SemaphoreType.DMA((3,))],
        compiler_params=pltpu.CompilerParams(vmem_limit_bytes=63 * 1024 * 1024, dimension_semantics=('arbitrary',)),
        cost_estimate=pl.CostEstimate(flops=65_000_000_000, bytes_accessed=70_000_000, transcendentals=4_700_000),
        name='hidden',
    )(ng_own, ng_oth, w_part, b1, b2, *extra)


A_SHARE = 14


def fold_first_kernel(keep_ref, got_ref, keep_a, send_a, keep_b, send_b):
    z_at, y_at = pl.program_id(0) // 2, lax.rem(pl.program_id(0), 2)
    cols = keep_a.shape[2]
    a = keep_ref[0, :, :cols] + got_ref[0, :, :cols]
    b = keep_ref[0, :, cols:] + got_ref[0, :, cols:]
    z_own = z_at == lax.axis_index('z')
    y_own = y_at == lax.axis_index('y')
    for ref, hit, at, value in ((keep_a, z_own, y_at, a), (send_a, jnp.logical_not(z_own), y_at, a), (keep_b, y_own, z_at, b), (send_b, jnp.logical_not(y_own), z_at, b)):
        @pl.when(hit)
        def _():
            ref[at] = value


def fold_first(keep, got):
    _, rows, width = keep.shape
    cols = A_SHARE * 128
    block = pl.BlockSpec((1, rows, width), lambda i: (i, 0, 0))
    shapes = [(2, rows, cols)] * 2 + [(2, rows, width - cols)] * 2
    return pl.pallas_call(
        fold_first_kernel, grid=(4,), in_specs=[block, block], name='fold_first',
        out_specs=[pl.BlockSpec(shape, lambda i: (0, 0, 0)) for shape in shapes],
        out_shape=[jax.ShapeDtypeStruct(shape, F32) for shape in shapes],
        compiler_params=pltpu.CompilerParams(vmem_limit_bytes=48 * 1024 * 1024, dimension_semantics=('arbitrary',)),
        cost_estimate=pl.CostEstimate(flops=6_000_000_000, bytes_accessed=24_000_000, transcendentals=0),
    )(keep, got)


def fold_second_kernel(a_ref, got_a_ref, b_ref, got_b_ref, keep_a, send_a, keep_b, send_b):
    for ref, got_ref, keep, send, own in ((a_ref, got_a_ref, keep_a, send_a, lax.axis_index('y')), (b_ref, got_b_ref, keep_b, send_b, lax.axis_index('z'))):
        keep[...] = ref[own] + got_ref[own]
        send[...] = ref[1 - own] + got_ref[1 - own]


def fold_second(*parts):
    shapes = [part.shape[1:] for part in parts]
    return pl.pallas_call(
        fold_second_kernel, out_shape=[jax.ShapeDtypeStruct(shape, F32) for shape in shapes], name='fold_second',
        compiler_params=pltpu.CompilerParams(vmem_limit_bytes=48 * 1024 * 1024),
        cost_estimate=pl.CostEstimate(flops=3_000_000_000, bytes_accessed=12_000_000, transcendentals=0),
    )(*parts)


def fold_third_kernel(a_ref, got_a_ref, b_ref, got_b_ref, out_ref):
    cols = a_ref.shape[1]
    out_ref[:, :cols] = a_ref[...] + got_a_ref[...]
    out_ref[:, cols:] = b_ref[...] + got_b_ref[...]


def fold_third(a, got_a, b, got_b):
    return pl.pallas_call(
        fold_third_kernel, out_shape=jax.ShapeDtypeStruct((a.shape[0], a.shape[1] + b.shape[1]), F32), name='fold_third',
        cost_estimate=pl.CostEstimate(flops=2_000_000_000, bytes_accessed=6_000_000, transcendentals=0),
    )(a, got_a, b, got_b)


def attn_grad_kernel(cp_ref, own_ref, n1_ref, n2_ref, n3_ref, g1_ref, g2_ref, g3_ref, dqkv_ref, o_lo_ref, o_hi_ref, keep_ref, send_ref):
    step = pl.program_id(0)
    core = lax.axis_index('core')
    d_model = own_ref.shape[2] // 2
    r_o, r_in = o_lo_ref.shape[1] // 8, d_model // 16
    width = dqkv_ref.shape[1]
    rows = own_ref.shape[1]
    place = [pl.ds(pl.multiple_of((cp_ref[0] ^ flip) * rows, rows), rows) for flip in range(4)]

    def put(at, cols, value_of):
        for dev in range(16):
            for ref, flip in ((keep_ref, 0), (send_ref, 1)):
                @pl.when((core ^ flip) == dev % 2)
                def _():
                    ref[dev // 2, at, cols] = value_of(dev)

    d_wqkv = dot_tn(own_ref[0, :, :d_model], dqkv_ref[place[0], :])
    for flip, n_ref in ((1, n1_ref), (2, n2_ref), (3, n3_ref)):
        d_wqkv = d_wqkv + dot_tn(n_ref[0], dqkv_ref[place[flip], :])
    put(slice(r_o, r_o + r_in), slice(0, width), lambda dev: d_wqkv[dev * r_in:(dev + 1) * r_in])

    def low(first_col, used):
        d_wo = []
        for o_ref in (o_lo_ref, o_hi_ref):
            total = dot_tn(o_ref[place[0], :], own_ref[0, :, d_model + first_col:d_model + first_col + used])
            for flip, g_ref in ((1, g1_ref), (2, g2_ref), (3, g3_ref)):
                total = total + dot_tn(o_ref[place[flip], :], g_ref[0, :, first_col:first_col + used])
            d_wo.append(total)
        put(slice(0, r_o), slice(0, used), lambda dev: d_wo[dev // 8][dev % 8 * r_o:(dev % 8 + 1) * r_o])
        if used < width:
            put(slice(0, r_o), slice(used, width), lambda dev: jnp.zeros((r_o, width - used), F32))

    for i in range(-(-d_model // width)):
        pl.when(step == i)(functools.partial(low, i * width, min(width, d_model - i * width)))


def attn_grad(cp_index, ng_blocks, n_got, g_got, od_seq, r_o, r_in):
    _, rows, both = ng_blocks.shape
    t_len = od_seq.shape[0]
    width = 512
    total = (N_HEADS + 2) * HEAD_DIM
    out = jax.ShapeDtypeStruct((8, r_o + r_in, total), F32)
    out_spec = pl.BlockSpec((8, r_o + r_in, width), lambda i, cp: (0, 0, i))
    one = pl.Buffered(1)
    full = lambda a: pl.BlockSpec(a.shape, lambda i, cp: (0, 0, 0), pipeline_mode=one)
    return pl.pallas_call(
        attn_grad_kernel,
        grid_spec=pltpu.PrefetchScalarGridSpec(
            num_scalar_prefetch=1,
            grid=(total // width,),
            in_specs=[pl.BlockSpec((1, rows, both), lambda i, cp: (cp[0], 0, 0), pipeline_mode=one)] + [full(a) for a in n_got + g_got]
                     + [pl.BlockSpec((t_len, width), lambda i, cp: (0, i)),
                        pl.BlockSpec((t_len, width), lambda i, cp: (0, total // width), pipeline_mode=one),
                        pl.BlockSpec((t_len, width), lambda i, cp: (0, total // width + 1), pipeline_mode=one)],
            out_specs=[out_spec, out_spec]),
        out_shape=[out, out],
        compiler_params=pltpu.CompilerParams(vmem_limit_bytes=60 * 1024 * 1024, dimension_semantics=('arbitrary',)),
        cost_estimate=pl.CostEstimate(flops=12_000_000_000, bytes_accessed=33_000_000, transcendentals=0),
        name='attn_grad',
    )(cp_index[None], ng_blocks, *n_got, *g_got, od_seq, od_seq, od_seq)


def fwd_product(act_refs, w_refs):
    out = dot_nn(act_refs[0][...], w_refs[0][...])
    for act_ref, w_ref in zip(act_refs[1:], w_refs[1:]):
        out = out + dot_nn(act_ref[...], w_ref[...])
    return out


def bwd_product(dh_refs, w_refs):
    out = dot_nt(dh_refs[0][...], w_refs[0][:, :dh_refs[0].shape[1]])
    for dh_ref, w_ref in zip(dh_refs[1:], w_refs[1:]):
        out = out + dot_nt(dh_ref[...], w_ref[:, :dh_ref.shape[1]])
    return out


def other_kernel(product, *refs):
    refs[-1][...] = product(refs[:N_PART], refs[N_PART:2 * N_PART])


OUT_ROWS = 256


def out_specs_of(width, weights, w_width, w_off, first_block):
    tile = pl.BlockSpec((OUT_ROWS, width), lambda i, *_: (i + first_block, 0))
    specs = [tile] * N_PART
    for array, col in weights:
        specs.append(pl.BlockSpec((array.shape[0], w_width), lambda i, *_, at=w_off(col): (0, at), pipeline_mode=pl.Buffered(1)))
    return specs


def out_other(parts, weights, product, w_width, w_off):
    t_len, width = parts[0].shape[0] // 2, parts[0].shape[1]
    d_model = weights[0][0].shape[0]
    return pl.pallas_call(
        functools.partial(other_kernel, product),
        grid=(t_len // OUT_ROWS,),
        in_specs=out_specs_of(width, weights, w_width, w_off, t_len // OUT_ROWS),
        out_specs=pl.BlockSpec((OUT_ROWS, d_model), lambda i: (i, 0)),
        out_shape=jax.ShapeDtypeStruct((t_len, d_model), F32),
        compiler_params=pltpu.CompilerParams(vmem_limit_bytes=60 * 1024 * 1024, dimension_semantics=('arbitrary',)),
        cost_estimate=pl.CostEstimate(flops=2 * t_len * d_model * width * N_PART, bytes_accessed=50_000_000, transcendentals=0),
    )(*parts, *[array for array, _ in weights])


def fwd_own_kernel(cp_ref, *refs):
    o_refs = refs[2 * N_PART:2 * N_PART + 8]
    wo_ref, x_ref, got_ref, bias_ref, out_ref, o_s = refs[2 * N_PART + 8:]
    flip = (pl.program_id(0) // 2) ^ cp_ref[0]
    half = o_s.shape[1] // 2
    for i in range(4):
        @pl.when(flip == i)
        def _():
            o_s[:, :half] = o_refs[2 * i][0]
            o_s[:, half:] = o_refs[2 * i + 1][0]
    out = fwd_product(refs[:N_PART], refs[N_PART:2 * N_PART]) + dot_nn(o_s[...], wo_ref[...])
    out_ref[...] = (x_ref[...].astype(F32) + out + got_ref[...] + bias_ref[...]).astype(BF16)


def bwd_own_kernel(cp_ref, *refs):
    d_refs = refs[2 * N_PART:2 * N_PART + 4]
    wqkv_ref, x_ref, g_ref, got_ref, scale_ref, d_x_ref, sums_ref, d_s = refs[2 * N_PART + 4:]
    flip = (pl.program_id(0) // 2) ^ cp_ref[0]
    for i in range(4):
        @pl.when(flip == i)
        def _():
            d_s[...] = d_refs[i][0]

    @pl.when(pl.program_id(0) == 0)
    def _():
        sums_ref[...] = jnp.zeros_like(sums_ref)

    d_n = bwd_product(refs[:N_PART], refs[N_PART:2 * N_PART]) + dot_nt(d_s[...], wqkv_ref[...]) + got_ref[...]
    x_f = x_ref[...].astype(F32)
    g_f = g_ref[...].astype(F32)
    inv = lax.rsqrt(jnp.mean(x_f * x_f, axis=1, keepdims=True) + 1e-6)
    scaled = d_n * (1.0 + scale_ref[...])
    xn = x_f * inv
    proj = jnp.mean(scaled * xn, axis=1, keepdims=True)
    d_x_ref[...] = (g_f + inv * (scaled - xn * proj)).astype(BF16)
    rows, d_model = x_f.shape
    sums_ref[:8, :] += jnp.sum((d_n * xn).reshape(rows // 8, 8, d_model), axis=0)
    sums_ref[8:, :] += jnp.sum(g_f.reshape(rows // 8, 8, d_model), axis=0)


def own_call(kernel, cp_index, parts, weights, w_width, w_off, od_blocks, od_got, od_cols, od_width, rest, rest_specs, out_specs, out_shape, scratch):
    t_len, width = parts[0].shape[0] // 2, parts[0].shape[1]
    specs = out_specs_of(width, weights, w_width, w_off, 0)
    args = list(parts) + [array for array, _ in weights]
    for i, source in enumerate([od_blocks] + od_got):
        for col in od_cols:
            if i == 0:
                specs.append(pl.BlockSpec((1, OUT_ROWS, od_width), lambda j, cp, col=col: (cp[0], jnp.clip(j - 2 * cp[0], 0, 1), col)))
            else:
                specs.append(pl.BlockSpec((1, OUT_ROWS, od_width), lambda j, cp, col=col, i=i: (0, jnp.clip(j - 2 * (cp[0] ^ i), 0, 1), col)))
            args.append(source)
    return pl.pallas_call(
        kernel,
        grid_spec=pltpu.PrefetchScalarGridSpec(
            num_scalar_prefetch=1, grid=(t_len // OUT_ROWS,), in_specs=specs + rest_specs, out_specs=out_specs, scratch_shapes=scratch),
        out_shape=out_shape,
        compiler_params=pltpu.CompilerParams(vmem_limit_bytes=62 * 1024 * 1024, dimension_semantics=('arbitrary',)),
        cost_estimate=pl.CostEstimate(flops=2 * t_len * weights[0][0].shape[0] * (width * N_PART + 1024), bytes_accessed=80_000_000, transcendentals=0),
    )(cp_index[None], *args, *rest)


def pack_kernel(wq_ref, wk_ref, wv_ref, wo_ref, out_ref):
    r_o, d_model = wo_ref.shape
    qk = wq_ref.shape[1]
    out_ref[:r_o, :d_model] = wo_ref[...].astype(BF16)
    out_ref[:r_o, d_model:] = jnp.zeros((r_o, out_ref.shape[1] - d_model), BF16)
    out_ref[r_o:, :qk] = wq_ref[...].astype(BF16)
    out_ref[r_o:, qk:qk + HEAD_DIM] = wk_ref[...].astype(BF16)
    out_ref[r_o:, qk + HEAD_DIM:] = wv_ref[...].astype(BF16)


def pack(w_q, w_k, w_v, w_o):
    out = jax.ShapeDtypeStruct((w_o.shape[0] + w_q.shape[0], w_q.shape[1] + 2 * HEAD_DIM), BF16)
    return pl.pallas_call(pack_kernel, out_shape=out, name='pack')(w_q, w_k, w_v, w_o)


def vector_kernel(scale_ref, bo_ref, bd_ref, b1_ref, b2_ref, out_ref, side_s):
    side_s[...] = jnp.zeros_like(side_s)
    for row, ref in enumerate((scale_ref, bo_ref, bd_ref, b1_ref, b2_ref)):
        side_s[row:row + 1, :ref.shape[1]] = ref[...]
    out_ref[...] = side_s[...].astype(BF16)


def vectors(*parts):
    width = -(-max(part.shape[0] for part in parts) // 128) * 128
    return pl.pallas_call(
        vector_kernel, out_shape=jax.ShapeDtypeStruct((8, width), BF16), scratch_shapes=[pltpu.VMEM((8, width), F32)], name='vectors',
    )(*[part[None] for part in parts])


def solution(mesh):
    mesh4 = Mesh(mesh.devices.reshape(2, 2, 2, 2), ALL_AXES)
    tok_spec = P(('x', 'core'), ('z', 'y'), None)
    pos_spec = P(('x', 'core'), ('z', 'y'))
    vec_spec = P(ALL_AXES)
    mat_spec = P(ALL_AXES, None)
    param_specs = (vec_spec, mat_spec, mat_spec, mat_spec, mat_spec, vec_spec, mat_spec, vec_spec, mat_spec, vec_spec, mat_spec, vec_spec)

    def swap_core(values):
        return lax.ppermute(values, 'core', [(0, 1), (1, 0)])

    def scatter_by_hand(keep, send):
        def shift(values, axis):
            return lax.ppermute(values, axis, [(0, 1), (1, 0)])

        keep_a, send_a, keep_b, send_b = fold_first(keep, shift(send, 'x'))
        keep_a, send_a, keep_b, send_b = fold_second(keep_a, shift(send_a, 'z'), keep_b, shift(send_b, 'y'))
        return fold_third(keep_a, shift(send_a, 'y'), keep_b, shift(send_b, 'z'))

    def after(value, *deps):
        return lax.optimization_barrier((value,) + deps)[0]

    def send_blocks(values, cp_index, width=None):
        got = []
        for flip in (1, 2, 3):
            sent = lax.dynamic_index_in_dim(values, cp_index ^ flip, 0, keepdims=True)[..., :width]
            got.append(lax.ppermute(sent, ('z', 'y'), [(i, i ^ flip) for i in range(4)]))
        return got

    def local_step(x_in, grad_out, seg_id, seg_pos, norm_scale, w_q, w_k, w_v, w_o, b_o, w_up1, b_up1, w_up2, b_up2, w_down, b_down):
        n_seq, piece, d_model = x_in.shape
        t_len = n_seq * piece
        core = lax.axis_index('core')
        cp_index = lax.axis_index('z') * 2 + lax.axis_index('y')
        first = core == 0
        r_in = w_q.shape[0]
        r_o = w_o.shape[0]
        f_blk = b_up1.shape[0]
        sub = f_blk // N_PART
        qk = N_HEADS * HEAD_DIM

        seg_pack = jnp.stack([seg_id, seg_pos], axis=1)
        seg_got = send_blocks(seg_pack, cp_index)
        g_got = send_blocks(grad_out, cp_index)

        keep, send = split_up(w_up1, w_up2)
        shards = stack_up(keep, swap_core(send), w_down, pack(w_q, w_k, w_v, w_o))

        def gather(shard):
            return lax.all_gather(shard, CHIPS, axis=0, tiled=True)

        whole = [gather(shards[0]), gather(shards[1])]
        weights = [(whole[0], 0), (whole[1], 0), (whole[1], 1)]

        vec_all = lax.all_gather(vectors(norm_scale, b_o, b_down, b_up1, b_up2), ALL_AXES, axis=0)
        scale_f, bo_f, bd_f = [vec_all[:, i, :r_in].reshape(1, d_model).astype(F32) for i in range(3)]
        b_ups = []
        for row in (3, 4):
            both = vec_all[:, row, :f_blk].reshape(8, 2, N_PART, sub)
            mine = jnp.where(first, both[:, 0], both[:, 1]).astype(F32)
            b_ups.append([mine[:, part].reshape(1, d_model) for part in range(N_PART)])

        x_loc = x_in.reshape(t_len, d_model)
        ng_own = norm_and_grad(x_loc, grad_out.reshape(t_len, d_model), scale_f)
        ng_oth = swap_core(ng_own)
        ng_blocks = ng_own.reshape(n_seq, piece, 2 * d_model)
        n_got = send_blocks(ng_blocks, cp_index, d_model)

        seg_all = jnp.zeros_like(seg_pack)
        for flip, got in enumerate([lax.dynamic_index_in_dim(seg_pack, cp_index, 0, keepdims=True)] + seg_got):
            seg_all = lax.dynamic_update_slice_in_dim(seg_all, got, cp_index ^ flip, 0)
        seg_own = seg_all[:, 0].reshape(t_len)
        pos_own = seg_all[:, 1].reshape(t_len)
        half = ROPE_DIMS // 2
        inv_freq = 10000.0 ** (-jnp.arange(half, dtype=F32) / half)
        angle = pos_own.astype(F32)[:, None] * inv_freq
        cos_a = jnp.cos(angle)
        sin_a = jnp.sin(angle)
        cos_b = jnp.concatenate([cos_a, cos_a], axis=1)
        sin_b = jnp.concatenate([-sin_a, sin_a], axis=1)

        acts, dhs, dbs, owns, recvs = [], [], [], [], []

        def third(part, ng_in, extra=()):
            act, dh, *d_w, db = hidden_part(ng_in, ng_oth, weights[part], b_ups[0][part], b_ups[1][part], extra, halves=part == 0)
            if part == 0:
                own = scatter_by_hand(*d_w)
            else:
                own = lax.psum_scatter(d_w[0], CHIPS, scatter_dimension=0, tiled=True)
            recvs.append(swap_core(jnp.where(first, own[r_in:, :2 * d_model], own[:r_in, :2 * d_model])))
            acts.append(act)
            dhs.append(dh)
            dbs.append(jnp.sum(db.reshape(2, 8, d_model), axis=1).reshape(2, 8, sub))
            owns.append(own)

        third(0, ng_own)
        extra_own = whole[0][:, 3 * d_model:]
        wqkv, wo = unpack(extra_own, swap_core(extra_own), r_o, r_in, d_model)
        od_seq = attention(cp_index, ng_blocks, n_got, g_got, wqkv, wo, cos_b, sin_b, seg_own)
        third(1, ng_own)
        d_keep, d_send = attn_grad(cp_index, ng_blocks, n_got, g_got, od_seq, r_o, r_in)
        od_blocks = od_seq.reshape(n_seq, piece, -1)
        od_got = send_blocks(od_blocks, cp_index)
        third(2, ng_own, (d_keep, swap_core(d_send)))

        wd_off = lambda col: 3 * col + 2
        w12_off = lambda col: col
        tile = lambda width, col=0: pl.BlockSpec((OUT_ROWS, width), lambda i, *_: (i, col))
        full = lambda a: pl.BlockSpec(a.shape, lambda i, *_: (0, 0), pipeline_mode=pl.Buffered(1))
        out_oth = out_other(acts, weights, fwd_product, d_model, wd_off)
        dn_oth = out_other(after(tuple(dhs), out_oth), weights, bwd_product, 3 * d_model, w12_off)
        bias_f = bo_f + bd_f
        x_out = own_call(fwd_own_kernel, cp_index, after(tuple(acts), dn_oth), weights, d_model, wd_off, od_blocks, od_got, (3, 4), 512,
                         [wo, x_loc, swap_core(out_oth), bias_f], [full(wo), tile(d_model), tile(d_model), full(bias_f)],
                         tile(d_model), jax.ShapeDtypeStruct((t_len, d_model), BF16), [pltpu.VMEM((OUT_ROWS, qk), BF16)])
        d_x, sums = own_call(bwd_own_kernel, cp_index, after(tuple(dhs), x_out), weights, 3 * d_model, w12_off, od_blocks, od_got, (0,), qk + 2 * HEAD_DIM,
                             [wqkv, x_loc, ng_own, swap_core(dn_oth), scale_f],
                             [full(wqkv), tile(d_model), tile(d_model, 1), tile(d_model), full(scale_f)],
                             [tile(d_model), pl.BlockSpec((16, d_model), lambda i, *_: (0, 0))],
                             [jax.ShapeDtypeStruct((t_len, d_model), BF16), jax.ShapeDtypeStruct((16, d_model), F32)],
                             [pltpu.VMEM((OUT_ROWS, qk + 2 * HEAD_DIM), BF16)])
        x_out = x_out.reshape(n_seq, piece, d_model)
        d_x = d_x.reshape(n_seq, piece, d_model)

        sums = jnp.sum(sums.reshape(2, 8, d_model), axis=1).reshape(2, 16, r_in)
        db = jnp.stack(dbs, axis=2).reshape(2, 8, f_blk)
        zero = jnp.zeros_like(db)
        db = jnp.where(first, jnp.stack([db, zero], axis=2), jnp.stack([zero, db], axis=2)).reshape(2, 16, f_blk)
        small = jnp.concatenate([sums[0], sums[1], db[0], db[1]], axis=1)
        small = lax.psum(small, ALL_AXES)
        small = lax.dynamic_index_in_dim(small, lax.axis_index(ALL_AXES), 0, keepdims=False)
        g_scale, g_bias, g_b1, g_b2 = small[:r_in], small[r_in:2 * r_in], small[2 * r_in:2 * r_in + f_blk], small[2 * r_in + f_blk:]

        g_w1, g_w2, g_wd = join_up(owns, recvs)
        g_attn = owns[2][:r_o + r_in, 3 * d_model:]
        g_wo, g_wq, g_wk, g_wv = g_attn[:r_o, :d_model], g_attn[r_o:, :qk], g_attn[r_o:, qk:qk + HEAD_DIM], g_attn[r_o:, qk + HEAD_DIM:]
        return (x_out, d_x, g_scale, g_wq, g_wk, g_wv, g_wo, g_bias, g_w1, g_b1, g_w2, g_b2, g_wd, g_bias)

    in_specs = (tok_spec, tok_spec, pos_spec, pos_spec) + param_specs
    out_specs = (tok_spec, tok_spec) + param_specs
    return jax.shard_map(local_step, mesh=mesh4, in_specs=in_specs, out_specs=out_specs, check_vma=False)
```

```python
import functools
import jax
import jax.numpy as jnp
from jax import lax
from jax.experimental import pallas as pl
from jax.experimental.pallas import tpu as pltpu
from jax.sharding import Mesh, PartitionSpec as P


ROPE_DIMS = 128
HEAD_DIM = 256
N_HEADS = 4
MASKED = -1.6e31
EXP_SCALE = 1.4426950408889634 / 16.0
CHIPS = ('z', 'y', 'x')
ALL_AXES = ('z', 'y', 'x', 'core')
F32 = jnp.float32
BF16 = jnp.bfloat16


def dot_nn(a, b):
    return lax.dot_general(a, b, (((1,), (0,)), ((), ())), preferred_element_type=F32)


def dot_nt(a, b):
    return lax.dot_general(a, b, (((1,), (1,)), ((), ())), preferred_element_type=F32)


def dot_tn(a, b):
    return lax.dot_general(a, b, (((0,), (0,)), ((), ())), preferred_element_type=F32)


def rotate(values, cos_b, sin_b):
    return values * cos_b + pltpu.roll(values, ROPE_DIMS // 2, axis=1) * sin_b


def attn_kernel(cp_ref, own_ref, n1_ref, n2_ref, n3_ref, g1_ref, g2_ref, g3_ref, wqkv_ref, wo_ref, cos_ref, sin_ref, cosk_ref, sink_ref, segq_ref, segk_ref, out_ref,
                n_buf, g_buf, sems, q_s, do_s, k_s, v_s, kt_s, vt_s, mask_s, s_s, p_s, dk_s, dv_s):
    step = pl.program_id(0)
    n_blocks = pl.num_programs(0)
    rows, d_model = n_buf.shape[1:]
    qk = N_HEADS * HEAD_DIM
    base = pl.multiple_of(step * rows, rows)
    cos_b = cos_ref[...]
    sin_b = sin_ref[...]
    slot = lax.rem(step, 2)

    def fetch(at_step):
        flip = at_step ^ cp_ref[0]
        to = lax.rem(at_step, 2)
        own = own_ref.at[cp_ref[0]]
        sources = ((own.at[:, :d_model], own.at[:, d_model:]), (n1_ref.at[0], g1_ref.at[0]), (n2_ref.at[0], g2_ref.at[0]), (n3_ref.at[0], g3_ref.at[0]))
        for i, (n_src, g_src) in enumerate(sources):
            @pl.when(flip == i)
            def _():
                pltpu.make_async_copy(n_src, n_buf.at[to], sems.at[0, to]).start()
                pltpu.make_async_copy(g_src, g_buf.at[to], sems.at[1, to]).start()

    pl.when(step == 0)(lambda: fetch(step))
    pl.when(step + 1 < n_blocks)(lambda: fetch(step + 1))
    pltpu.make_async_copy(n1_ref.at[0], n_buf.at[slot], sems.at[0, slot]).wait()
    pltpu.make_async_copy(g1_ref.at[0], g_buf.at[slot], sems.at[1, slot]).wait()
    n_blk = n_buf[slot]
    g_blk = g_buf[slot]

    @pl.when(step == 0)
    def _():
        dk_s[...] = jnp.zeros_like(dk_s)
        dv_s[...] = jnp.zeros_like(dv_s)

    for h in range(N_HEADS):
        lin = dot_nn(n_blk, wqkv_ref[:, h * HEAD_DIM:(h + 1) * HEAD_DIM])
        q_s[h, :, :ROPE_DIMS] = rotate(lin[:, :ROPE_DIMS], cos_b, sin_b).astype(BF16)
        q_s[h, :, ROPE_DIMS:] = lin[:, ROPE_DIMS:].astype(BF16)
        do_s[h] = dot_nt(g_blk, wo_ref[h * HEAD_DIM:(h + 1) * HEAD_DIM, :]).astype(BF16)
    k_lin = dot_nn(n_blk, wqkv_ref[:, qk:qk + HEAD_DIM])
    k_blk = jnp.concatenate([rotate(k_lin[:, :ROPE_DIMS], cos_b, sin_b), k_lin[:, ROPE_DIMS:]], axis=1)
    v_blk = dot_nn(n_blk, wqkv_ref[:, qk + HEAD_DIM:])
    k_s[pl.ds(base, rows), :] = k_blk.astype(BF16)
    v_s[pl.ds(base, rows), :] = v_blk.astype(BF16)
    kt_s[:, pl.ds(base, rows)] = k_blk.T.astype(BF16)
    vt_s[:, pl.ds(base, rows)] = v_blk.T.astype(BF16)

    def block(blk):
        n_chunk = blk + 1
        seg_q = segq_ref[:, :1]
        for c in range(n_chunk):
            same = seg_q == segk_ref[:1, c * rows:(c + 1) * rows]
            if c == blk:
                r_id = lax.broadcasted_iota(jnp.int32, (rows, rows), 0)
                c_id = lax.broadcasted_iota(jnp.int32, (rows, rows), 1)
                same = same & (c_id <= r_id)
            mask_s[:, c * rows:(c + 1) * rows] = jnp.where(same, 1.0, 0.0)

        def head(h, carry):
            q = q_s[h]
            do = do_s[h]
            m_run = None
            for c in range(n_chunk):
                sl = slice(c * rows, (c + 1) * rows)
                s = jnp.where(mask_s[:, sl] > 0.5, dot_nn(q, kt_s[:, sl]), MASKED)
                s_s[:, sl] = s
                m_c = jnp.max(s, axis=1, keepdims=True)
                m_run = m_c if m_run is None else jnp.maximum(m_run, m_c)
            l_run = None
            for c in range(n_chunk):
                sl = slice(c * rows, (c + 1) * rows)
                e = jnp.exp2((s_s[:, sl] - m_run) * EXP_SCALE)
                s_s[:, sl] = e
                l_c = jnp.sum(e, axis=1, keepdims=True)
                l_run = l_c if l_run is None else l_run + l_c
            inv = 1.0 / l_run
            for c in range(n_chunk):
                sl = slice(c * rows, (c + 1) * rows)
                p = s_s[:, sl] * inv
                s_s[:, sl] = p
                p_s[:, sl] = p.astype(BF16)
            o = dot_nn(p_s[:, :n_chunk * rows], v_s[:n_chunk * rows, :])
            delta = jnp.sum(o * do.astype(F32), axis=1, keepdims=True)
            out_ref[pl.ds(base, rows), pl.ds(pl.multiple_of(qk + 2 * HEAD_DIM + h * HEAD_DIM, HEAD_DIM), HEAD_DIM)] = o.astype(BF16)
            dq = None
            for c in range(n_chunk):
                sl = slice(c * rows, (c + 1) * rows)
                ds = (s_s[:, sl] * (dot_nn(do, vt_s[:, sl]) - delta)).astype(BF16)
                dq_c = dot_nn(ds, k_s[sl, :])
                dq = dq_c if dq is None else dq + dq_c
                dk_s[sl, :] += dot_tn(ds, q)
                dv_s[sl, :] += dot_tn(p_s[:, sl], do)
            dq = dq * 0.0625
            dq = jnp.concatenate([rotate(dq[:, :ROPE_DIMS], cos_b, -sin_b), dq[:, ROPE_DIMS:]], axis=1)
            out_ref[pl.ds(base, rows), pl.ds(pl.multiple_of(h * HEAD_DIM, HEAD_DIM), HEAD_DIM)] = dq.astype(BF16)
            return carry

        lax.fori_loop(0, N_HEADS, head, 0)

    for blk in range(4):
        pl.when(step == blk)(functools.partial(block, blk))

    @pl.when(step == n_blocks - 1)
    def _():
        dk = dk_s[...] * 0.0625
        dk = jnp.concatenate([rotate(dk[:, :ROPE_DIMS], cosk_ref[...], -sink_ref[...]), dk[:, ROPE_DIMS:]], axis=1)
        out_ref[:, qk:qk + HEAD_DIM] = dk.astype(BF16)
        out_ref[:, qk + HEAD_DIM:qk + 2 * HEAD_DIM] = dv_s[...].astype(BF16)


def attention(cp_index, ng_blocks, n_got, g_got, wqkv, wo, cos_b, sin_b, seg_own):
    _, rows, both = ng_blocks.shape
    t_len = 4 * rows
    qk = N_HEADS * HEAD_DIM
    segq = jnp.broadcast_to(seg_own[:, None], (t_len, 128))
    segk = jnp.broadcast_to(seg_own[None, :], (8, t_len))
    row_spec = lambda width: pl.BlockSpec((rows, width), lambda i, cp: (i, 0))
    full = lambda a: pl.BlockSpec(a.shape, lambda i, cp: (0,) * a.ndim, pipeline_mode=pl.Buffered(1))
    anywhere = pl.BlockSpec(memory_space=pl.ANY)
    width = 2 * (qk + HEAD_DIM)
    return pl.pallas_call(
        attn_kernel,
        grid_spec=pltpu.PrefetchScalarGridSpec(
            num_scalar_prefetch=1,
            grid=(4,),
            in_specs=[anywhere] * 7 + [full(wqkv), full(wo), row_spec(ROPE_DIMS), row_spec(ROPE_DIMS), full(cos_b), full(sin_b), row_spec(128), full(segk)],
            out_specs=pl.BlockSpec((t_len, width), lambda i, cp: (0, 0)),
            scratch_shapes=[
                pltpu.VMEM((2, rows, both // 2), BF16), pltpu.VMEM((2, rows, both // 2), BF16), pltpu.SemaphoreType.DMA((2, 2)),
                pltpu.VMEM((N_HEADS, rows, HEAD_DIM), BF16), pltpu.VMEM((N_HEADS, rows, HEAD_DIM), BF16),
                pltpu.VMEM((t_len, HEAD_DIM), BF16), pltpu.VMEM((t_len, HEAD_DIM), BF16),
                pltpu.VMEM((HEAD_DIM, t_len), BF16), pltpu.VMEM((HEAD_DIM, t_len), BF16),
                pltpu.VMEM((rows, t_len), F32), pltpu.VMEM((rows, t_len), F32), pltpu.VMEM((rows, t_len), BF16),
                pltpu.VMEM((t_len, HEAD_DIM), F32), pltpu.VMEM((t_len, HEAD_DIM), F32)]),
        out_shape=jax.ShapeDtypeStruct((t_len, width), BF16),
        compiler_params=pltpu.CompilerParams(vmem_limit_bytes=62 * 1024 * 1024, dimension_semantics=('arbitrary',)),
        cost_estimate=pl.CostEstimate(flops=45_000_000_000, bytes_accessed=40_000_000, transcendentals=10_000_000),
        name='attn',
    )(cp_index[None], ng_blocks, *n_got, *g_got, wqkv, wo, cos_b, sin_b, cos_b, sin_b, segq, segk)


def norm_kernel(x_ref, g_ref, scale_ref, out_ref):
    d_model = x_ref.shape[1]
    for part in range(0, x_ref.shape[0], 128):
        sl = slice(part, part + 128)
        x_f = x_ref[sl, :].astype(F32)
        inv = lax.rsqrt(jnp.mean(x_f * x_f, axis=1, keepdims=True) + 1e-6)
        out_ref[sl, :d_model] = (x_f * inv * (1.0 + scale_ref[...])).astype(BF16)
        out_ref[sl, d_model:] = g_ref[sl, :]


def norm_and_grad(x_loc, g_loc, scale_f):
    t_len, d_model = x_loc.shape
    rows = 512
    tile = pl.BlockSpec((rows, d_model), lambda i: (i, 0))
    return pl.pallas_call(
        norm_kernel, grid=(t_len // rows,), name='norm',
        in_specs=[tile, tile, pl.BlockSpec(scale_f.shape, lambda i: (0, 0))],
        out_specs=pl.BlockSpec((rows, 2 * d_model), lambda i: (i, 0)),
        out_shape=jax.ShapeDtypeStruct((t_len, 2 * d_model), BF16),
        cost_estimate=pl.CostEstimate(flops=4_000_000_000, bytes_accessed=19_000_000, transcendentals=2048),
    )(x_loc, g_loc, scale_f)


N_PART = 3


def split_kernel(w1_ref, w2_ref, keep_ref, send_ref):
    core = lax.axis_index('core')
    d_model = keep_ref.shape[2] // 2
    sub = d_model // 8
    for part in range(N_PART):
        for i, w_ref in enumerate((w1_ref, w2_ref)):
            even, odd = [
                jnp.concatenate([w_ref[:, ((2 * j + k) * N_PART + part) * sub:((2 * j + k) * N_PART + part + 1) * sub] for j in range(8)], axis=1).astype(BF16)
                for k in range(2)]

            @pl.when(core == 0)
            def _():
                keep_ref[part, :, i * d_model:(i + 1) * d_model] = even
                send_ref[part, :, i * d_model:(i + 1) * d_model] = odd

            @pl.when(core == 1)
            def _():
                keep_ref[part, :, i * d_model:(i + 1) * d_model] = odd
                send_ref[part, :, i * d_model:(i + 1) * d_model] = even


def split_up(w1, w2):
    rows, cols = w1.shape
    out = jax.ShapeDtypeStruct((N_PART, rows, cols // N_PART), BF16)
    return pl.pallas_call(split_kernel, out_shape=[out, out], name='split_up')(w1, w2)


def stack_kernel(keep_ref, recv_ref, wd_ref, extra_ref, first_ref, rest_ref):
    core = lax.axis_index('core')
    rows, cols = keep_ref.shape[1:]
    d_model = wd_ref.shape[1]
    own = pl.multiple_of(core * rows, 8)
    oth = pl.multiple_of(rows - own, 8)
    for part in range(N_PART):
        out_ref, base = (first_ref, 0) if part == 0 else (rest_ref, (part - 1) * (cols + d_model))
        out_ref[pl.ds(own, rows), base:base + cols] = keep_ref[part]
        out_ref[pl.ds(oth, rows), base:base + cols] = recv_ref[part]
        out_ref[:, base + cols:base + cols + d_model] = wd_ref[part * 2 * rows:(part + 1) * 2 * rows, :].astype(BF16)
    n_extra = extra_ref.shape[0]
    first_ref[:n_extra, cols + d_model:] = extra_ref[...]
    first_ref[n_extra:, cols + d_model:] = jnp.zeros((2 * rows - n_extra, extra_ref.shape[1]), BF16)


def stack_up(keep, recv, w_down, extra):
    _, rows, cols = keep.shape
    width = cols + w_down.shape[1]
    outs = [jax.ShapeDtypeStruct((2 * rows, width + extra.shape[1]), BF16), jax.ShapeDtypeStruct((2 * rows, (N_PART - 1) * width), BF16)]
    return pl.pallas_call(stack_kernel, out_shape=outs, name='stack_up')(keep, recv, w_down, extra)


def unpack_kernel(own_ref, oth_ref, wqkv_ref, wo_ref):
    core = lax.axis_index('core')
    r_o, r_in = wo_ref.shape[0] // 16, wqkv_ref.shape[0] // 16
    d_model = wo_ref.shape[1]
    rows = own_ref.shape[0] // 8
    for chip in range(8):
        for flip, ref in enumerate((own_ref, oth_ref)):
            dev = 2 * chip + (core ^ flip)
            wo_ref[pl.ds(pl.multiple_of(dev * r_o, 8), r_o), :] = ref[chip * rows:chip * rows + r_o, :d_model]
            wqkv_ref[pl.ds(pl.multiple_of(dev * r_in, 8), r_in), :] = ref[chip * rows + r_o:chip * rows + r_o + r_in, :]


def unpack(own, oth, r_o, r_in, d_model):
    return pl.pallas_call(
        unpack_kernel, name='unpack',
        out_shape=[jax.ShapeDtypeStruct((16 * r_in, own.shape[1]), BF16), jax.ShapeDtypeStruct((16 * r_o, d_model), BF16)],
    )(own, oth)


def join_kernel(*refs):
    own_refs, recv_refs, (w1_ref, w2_ref, wd_ref) = refs[:N_PART], refs[N_PART:2 * N_PART], refs[2 * N_PART:]
    core = lax.axis_index('core')
    rows = w1_ref.shape[0]
    d_model = wd_ref.shape[1]
    sub = d_model // 8

    def put(even_of, odd_of):
        for i, w_ref in enumerate((w1_ref, w2_ref)):
            pieces = []
            for j in range(8):
                for of in (even_of, odd_of):
                    for part in range(N_PART):
                        pieces.append(of(part)[:, i * d_model + j * sub:i * d_model + (j + 1) * sub])
            w_ref[...] = jnp.concatenate(pieces, axis=1)

    pl.when(core == 0)(lambda: put(lambda p: own_refs[p][:rows, :2 * d_model], lambda p: recv_refs[p][...]))
    pl.when(core == 1)(lambda: put(lambda p: recv_refs[p][...], lambda p: own_refs[p][rows:, :2 * d_model]))
    for part in range(N_PART):
        wd_ref[part * 2 * rows:(part + 1) * 2 * rows, :] = own_refs[part][:, 2 * d_model:3 * d_model]


def join_up(owns, recvs):
    rows, cols = recvs[0].shape
    d_model = cols // 2
    up = jax.ShapeDtypeStruct((rows, N_PART * cols), F32)
    return pl.pallas_call(
        join_kernel, out_shape=[up, up, jax.ShapeDtypeStruct((N_PART * 2 * rows, d_model), F32)], name='join_up',
    )(*owns, *recvs)


GELU_C = 0.7978845608028654
GELU_A = 0.044715


def hidden_kernel(mode, own_ref, oth_ref, w_ref, b1_ref, b2_ref, *refs):
    extra_refs = refs[:2] if mode == 'extra' else ()
    act_ref, dh_ref, *dw_refs, db_ref, h_s, da_s, ng_s, acc_s, side_s, sems = refs[len(extra_refs):]
    dw_ref = dw_refs[0]
    step = pl.program_id(0)
    last = pl.num_programs(0) - 1
    rows, d_model = da_s.shape
    own = step < pl.num_programs(0) // 2
    ng_s[...] = jnp.where(own, own_ref[...], oth_ref[...])

    @pl.when(step == 0)
    def _():
        acc_s[...] = jnp.zeros_like(acc_s)
        db_ref[...] = jnp.zeros_like(db_ref)

    def leave(which, act):
        cols = slice(0, 2 * d_model) if which == 0 else slice(2 * d_model, 3 * d_model)
        sem = sems.at[(0, 3)[which]]
        if mode != 'halves':
            pl.when(step == last)(lambda: act(pltpu.make_async_copy(acc_s.at[:, cols], dw_ref.at[:, cols], sem)))
            return
        x_index = lax.axis_index('x')
        block = d_model // 8
        for chip in range(8):
            for ref, flip in zip(dw_refs, (0, 1)):
                @pl.when((step == last) & ((x_index ^ flip) == chip % 2))
                def _():
                    act(pltpu.make_async_copy(acc_s.at[chip * block:(chip + 1) * block, cols], ref.at[chip // 2, :, cols], sem))

    n_sub = 2
    sub = rows // n_sub
    w12 = w_ref[:, :2 * d_model]
    for i in range(n_sub):
        sl = slice(i * sub, (i + 1) * sub)
        h_s[sl, :] = dot_nn(ng_s[sl, :d_model], w12)
        da_s[sl, :] = dot_nt(ng_s[sl, d_model:], w_ref[:, 2 * d_model:])
    b1 = b1_ref[...]
    b2 = b2_ref[...]
    for i in range(n_sub):
        sl = slice(i * sub, (i + 1) * sub)
        s1 = None
        s2 = None
        for r in range(i * sub, (i + 1) * sub, 64):
            rs = slice(r, r + 64)
            u = h_s[rs, :d_model] + b1
            v = h_s[rs, d_model:] + b2
            da = da_s[rs, :]
            u2 = u * u
            t = jnp.tanh(u * (GELU_C + (GELU_C * GELU_A) * u2))
            half = 0.5 + 0.5 * t
            gelu = u * half
            slope = half + (half * (1.0 - t)) * (u * (GELU_C + (3.0 * GELU_C * GELU_A) * u2))
            d1 = da * v * slope
            d2 = da * gelu
            act_ref[rs, :] = (gelu * v).astype(BF16)
            dh_ref[rs, :d_model] = d1.astype(BF16)
            dh_ref[rs, d_model:] = d2.astype(BF16)
            p1 = jnp.sum(d1.reshape(8, 8, d_model), axis=0)
            p2 = jnp.sum(d2.reshape(8, 8, d_model), axis=0)
            s1 = p1 if s1 is None else s1 + p1
            s2 = p2 if s2 is None else s2 + p2
        db_ref[:8, :] += s1
        db_ref[8:, :] += s2
        acc_s[:, :2 * d_model] += dot_tn(ng_s[sl, :d_model], dh_ref[sl, :])
        if i == n_sub - 1:
            leave(0, lambda copy: copy.start())
        acc_s[:, 2 * d_model:] += dot_tn(act_ref[sl, :], ng_s[sl, d_model:])

    if extra_refs:
        keep_ref, got_ref = extra_refs
        block = side_s.shape[1]
        n_extra = keep_ref.shape[1]
        slot = lax.rem(step, 2)

        def side_copy(at_slot, at_step):
            place = dw_ref.at[pl.ds(pl.multiple_of(at_step * block, 8), block), 3 * d_model:]
            return pltpu.make_async_copy(side_s.at[at_slot], place, sems.at[1 + at_slot])

        @pl.when(step >= 2)
        def _():
            side_copy(slot, step - 2).wait()

        side_s[slot, :n_extra, :] = keep_ref[0] + got_ref[0]
        side_s[slot, n_extra:, :] = jnp.zeros((block - n_extra, keep_ref.shape[2]), F32)
        side_copy(slot, step).start()

        @pl.when(step == last)
        def _():
            side_copy(1 - slot, step - 1).wait()
            side_copy(slot, step).wait()

    leave(1, lambda copy: copy.start())
    leave(0, lambda copy: copy.wait())
    leave(1, lambda copy: copy.wait())


def hidden_part(ng_own, ng_oth, weight, b1, b2, extra=(), halves=False):
    w_part, w_col = weight
    t_len, both = ng_own.shape
    d_model = both // 2
    rows = 512
    steps = 2 * t_len // rows
    half = steps // 2
    own_spec = pl.BlockSpec((rows, both), lambda i: (jnp.minimum(i, half - 1), 0))
    oth_spec = pl.BlockSpec((rows, both), lambda i: (jnp.maximum(i - half, 0), 0))
    full = lambda a, width, col=0: pl.BlockSpec((a.shape[0], width), lambda i: (0, col), pipeline_mode=pl.Buffered(1))
    row = lambda width: pl.BlockSpec((rows, width), lambda i: (i, 0))
    blk = [pl.BlockSpec((1,) + a.shape[1:], lambda i: (i, 0, 0)) for a in extra]
    side = (2, d_model // 8, extra[0].shape[2]) if extra else (2, 8, 128)
    mode = 'halves' if halves else 'extra' if extra else 'plain'
    if halves:
        grads = [jax.ShapeDtypeStruct((4, d_model // 8, 3 * d_model), F32)] * 2
    else:
        grads = [jax.ShapeDtypeStruct((d_model, 3 * d_model + (extra[0].shape[2] if extra else 0)), F32)]
    return pl.pallas_call(
        functools.partial(hidden_kernel, mode),
        grid=(steps,),
        in_specs=[own_spec, oth_spec, full(w_part, 3 * d_model, w_col), full(b1, d_model), full(b2, d_model)] + blk,
        out_specs=[row(d_model), row(2 * d_model)] + [pl.BlockSpec(memory_space=pl.ANY)] * len(grads) + [pl.BlockSpec((16, d_model), lambda i: (0, 0))],
        out_shape=[jax.ShapeDtypeStruct((2 * t_len, d_model), BF16), jax.ShapeDtypeStruct((2 * t_len, 2 * d_model), BF16),
                   *grads, jax.ShapeDtypeStruct((16, d_model), F32)],
        scratch_shapes=[pltpu.VMEM((rows, 2 * d_model), F32), pltpu.VMEM((rows, d_model), F32), pltpu.VMEM((rows, both), BF16),
                        pltpu.VMEM((d_model, 3 * d_model), F32), pltpu.VMEM(side, F32), pltpu.SemaphoreType.DMA((4,))],
        compiler_params=pltpu.CompilerParams(vmem_limit_bytes=63 * 1024 * 1024, dimension_semantics=('arbitrary',)),
        cost_estimate=pl.CostEstimate(flops=65_000_000_000, bytes_accessed=70_000_000, transcendentals=4_700_000),
        name='hidden',
    )(ng_own, ng_oth, w_part, b1, b2, *extra)


A_SHARE = 14


def fold_first_kernel(keep_ref, got_ref, keep_a, send_a, keep_b, send_b):
    z_at, y_at = pl.program_id(0) // 2, lax.rem(pl.program_id(0), 2)
    cols = keep_a.shape[2]
    a = keep_ref[0, :, :cols] + got_ref[0, :, :cols]
    b = keep_ref[0, :, cols:] + got_ref[0, :, cols:]
    z_own = z_at == lax.axis_index('z')
    y_own = y_at == lax.axis_index('y')
    for ref, hit, at, value in ((keep_a, z_own, y_at, a), (send_a, jnp.logical_not(z_own), y_at, a), (keep_b, y_own, z_at, b), (send_b, jnp.logical_not(y_own), z_at, b)):
        @pl.when(hit)
        def _():
            ref[at] = value


def fold_first(keep, got):
    _, rows, width = keep.shape
    cols = A_SHARE * 128
    block = pl.BlockSpec((1, rows, width), lambda i: (i, 0, 0))
    shapes = [(2, rows, cols)] * 2 + [(2, rows, width - cols)] * 2
    return pl.pallas_call(
        fold_first_kernel, grid=(4,), in_specs=[block, block], name='fold_first',
        out_specs=[pl.BlockSpec(shape, lambda i: (0, 0, 0)) for shape in shapes],
        out_shape=[jax.ShapeDtypeStruct(shape, F32) for shape in shapes],
        compiler_params=pltpu.CompilerParams(vmem_limit_bytes=48 * 1024 * 1024, dimension_semantics=('arbitrary',)),
        cost_estimate=pl.CostEstimate(flops=6_000_000_000, bytes_accessed=24_000_000, transcendentals=0),
    )(keep, got)


def fold_second_kernel(a_ref, got_a_ref, b_ref, got_b_ref, keep_a, send_a, keep_b, send_b):
    for ref, got_ref, keep, send, own in ((a_ref, got_a_ref, keep_a, send_a, lax.axis_index('y')), (b_ref, got_b_ref, keep_b, send_b, lax.axis_index('z'))):
        keep[...] = ref[own] + got_ref[own]
        send[...] = ref[1 - own] + got_ref[1 - own]


def fold_second(*parts):
    shapes = [part.shape[1:] for part in parts]
    return pl.pallas_call(
        fold_second_kernel, out_shape=[jax.ShapeDtypeStruct(shape, F32) for shape in shapes], name='fold_second',
        compiler_params=pltpu.CompilerParams(vmem_limit_bytes=48 * 1024 * 1024),
        cost_estimate=pl.CostEstimate(flops=3_000_000_000, bytes_accessed=12_000_000, transcendentals=0),
    )(*parts)


def fold_third_kernel(a_ref, got_a_ref, b_ref, got_b_ref, out_ref):
    cols = a_ref.shape[1]
    out_ref[:, :cols] = a_ref[...] + got_a_ref[...]
    out_ref[:, cols:] = b_ref[...] + got_b_ref[...]


def fold_third(a, got_a, b, got_b):
    return pl.pallas_call(
        fold_third_kernel, out_shape=jax.ShapeDtypeStruct((a.shape[0], a.shape[1] + b.shape[1]), F32), name='fold_third',
        cost_estimate=pl.CostEstimate(flops=2_000_000_000, bytes_accessed=6_000_000, transcendentals=0),
    )(a, got_a, b, got_b)


def attn_grad_kernel(cp_ref, own_ref, n1_ref, n2_ref, n3_ref, g1_ref, g2_ref, g3_ref, dqkv_ref, o_lo_ref, o_hi_ref, keep_ref, send_ref):
    step = pl.program_id(0)
    core = lax.axis_index('core')
    d_model = own_ref.shape[2] // 2
    r_o, r_in = o_lo_ref.shape[1] // 8, d_model // 16
    width = dqkv_ref.shape[1]
    rows = own_ref.shape[1]
    place = [pl.ds(pl.multiple_of((cp_ref[0] ^ flip) * rows, rows), rows) for flip in range(4)]

    def put(at, cols, value_of):
        for dev in range(16):
            for ref, flip in ((keep_ref, 0), (send_ref, 1)):
                @pl.when((core ^ flip) == dev % 2)
                def _():
                    ref[dev // 2, at, cols] = value_of(dev)

    d_wqkv = dot_tn(own_ref[0, :, :d_model], dqkv_ref[place[0], :])
    for flip, n_ref in ((1, n1_ref), (2, n2_ref), (3, n3_ref)):
        d_wqkv = d_wqkv + dot_tn(n_ref[0], dqkv_ref[place[flip], :])
    put(slice(r_o, r_o + r_in), slice(0, width), lambda dev: d_wqkv[dev * r_in:(dev + 1) * r_in])

    def low(first_col, used):
        d_wo = []
        for o_ref in (o_lo_ref, o_hi_ref):
            total = dot_tn(o_ref[place[0], :], own_ref[0, :, d_model + first_col:d_model + first_col + used])
            for flip, g_ref in ((1, g1_ref), (2, g2_ref), (3, g3_ref)):
                total = total + dot_tn(o_ref[place[flip], :], g_ref[0, :, first_col:first_col + used])
            d_wo.append(total)
        put(slice(0, r_o), slice(0, used), lambda dev: d_wo[dev // 8][dev % 8 * r_o:(dev % 8 + 1) * r_o])
        if used < width:
            put(slice(0, r_o), slice(used, width), lambda dev: jnp.zeros((r_o, width - used), F32))

    for i in range(-(-d_model // width)):
        pl.when(step == i)(functools.partial(low, i * width, min(width, d_model - i * width)))


def attn_grad(cp_index, ng_blocks, n_got, g_got, od_seq, r_o, r_in):
    _, rows, both = ng_blocks.shape
    t_len = od_seq.shape[0]
    width = 512
    total = (N_HEADS + 2) * HEAD_DIM
    out = jax.ShapeDtypeStruct((8, r_o + r_in, total), F32)
    out_spec = pl.BlockSpec((8, r_o + r_in, width), lambda i, cp: (0, 0, i))
    one = pl.Buffered(1)
    full = lambda a: pl.BlockSpec(a.shape, lambda i, cp: (0, 0, 0), pipeline_mode=one)
    return pl.pallas_call(
        attn_grad_kernel,
        grid_spec=pltpu.PrefetchScalarGridSpec(
            num_scalar_prefetch=1,
            grid=(total // width,),
            in_specs=[pl.BlockSpec((1, rows, both), lambda i, cp: (cp[0], 0, 0), pipeline_mode=one)] + [full(a) for a in n_got + g_got]
                     + [pl.BlockSpec((t_len, width), lambda i, cp: (0, i)),
                        pl.BlockSpec((t_len, width), lambda i, cp: (0, total // width), pipeline_mode=one),
                        pl.BlockSpec((t_len, width), lambda i, cp: (0, total // width + 1), pipeline_mode=one)],
            out_specs=[out_spec, out_spec]),
        out_shape=[out, out],
        compiler_params=pltpu.CompilerParams(vmem_limit_bytes=60 * 1024 * 1024, dimension_semantics=('arbitrary',)),
        cost_estimate=pl.CostEstimate(flops=12_000_000_000, bytes_accessed=33_000_000, transcendentals=0),
        name='attn_grad',
    )(cp_index[None], ng_blocks, *n_got, *g_got, od_seq, od_seq, od_seq)


def small_kernel(in_ref, out_ref, got_s, send_sems, recv_sems):
    at = [lax.axis_index(axis) for axis in ALL_AXES]
    me = ((at[0] * 2 + at[1]) * 2 + at[2]) * 2 + at[3]

    def peer(flip):
        return tuple(index ^ ((flip >> (3 - i)) & 1) for i, index in enumerate(at))

    barrier = pltpu.get_barrier_semaphore()
    for flip in range(1, 16):
        pl.semaphore_signal(barrier, inc=1, device_id=peer(flip), device_id_type=pl.DeviceIdType.MESH)
    pl.semaphore_wait(barrier, 15)
    copies = []
    for flip in range(1, 16):
        copies.append(pltpu.make_async_remote_copy(
            src_ref=in_ref.at[me ^ flip], dst_ref=got_s.at[flip], send_sem=send_sems.at[flip], recv_sem=recv_sems.at[flip],
            device_id=peer(flip), device_id_type=pl.DeviceIdType.MESH))
        copies[-1].start()
    for copy in copies:
        copy.wait()
    total = in_ref[me]
    for flip in range(1, 16):
        total = total + got_s[flip]
    out_ref[...] = total


def small_sum(values):
    return pl.pallas_call(
        small_kernel, out_shape=jax.ShapeDtypeStruct(values.shape[1:], F32), name='small_sum',
        in_specs=[pl.BlockSpec(memory_space=pltpu.VMEM)], out_specs=pl.BlockSpec(memory_space=pltpu.VMEM),
        scratch_shapes=[pltpu.VMEM(values.shape, F32), pltpu.SemaphoreType.DMA((16,)), pltpu.SemaphoreType.DMA((16,))],
        compiler_params=pltpu.CompilerParams(collective_id=0, has_side_effects=True),
        cost_estimate=pl.CostEstimate(flops=8_000_000_000, bytes_accessed=130_000, transcendentals=0),
    )(values)


def fetch_weights(w_refs, cols, w_s, sems):
    first = pl.program_id(0) == 0
    copies = [pltpu.make_async_copy(ref.at[:, at:at + w_s.shape[2]], w_s.at[i], sems.at[i]) for i, (ref, at) in enumerate(zip(w_refs, cols))]
    for copy in copies:
        pl.when(first)(copy.start)
    return lambda i: pl.when(first)(copies[i].wait)


def fwd_product(act_refs, w_s, ready):
    out = None
    for i, act_ref in enumerate(act_refs):
        ready(i)
        part = dot_nn(act_ref[...], w_s[i])
        out = part if out is None else out + part
    return out


def bwd_product(dh_refs, w_s, ready):
    out = None
    for i, dh_ref in enumerate(dh_refs):
        ready(i)
        part = dot_nt(dh_ref[...], w_s[i])
        out = part if out is None else out + part
    return out


def other_kernel(product, cols, *refs):
    out_ref, w_s, sems = refs[-3:]
    out_ref[...] = product(refs[:N_PART], w_s, fetch_weights(refs[N_PART:2 * N_PART], cols, w_s, sems))


OUT_ROWS = 256


def out_specs_of(width, first_block):
    tile = pl.BlockSpec((OUT_ROWS, width), lambda i, *_: (i + first_block, 0))
    return [tile] * N_PART + [pl.BlockSpec(memory_space=pl.ANY)] * N_PART


def weight_scratch(weights, w_width):
    return [pltpu.VMEM((N_PART, weights[0][0].shape[0], w_width), BF16), pltpu.SemaphoreType.DMA((N_PART,))]


def out_other(parts, weights, product, w_width, w_off):
    t_len, width = parts[0].shape[0] // 2, parts[0].shape[1]
    d_model = weights[0][0].shape[0]
    return pl.pallas_call(
        functools.partial(other_kernel, product, [w_off(col) for _, col in weights]),
        grid=(t_len // OUT_ROWS,),
        scratch_shapes=weight_scratch(weights, w_width),
        in_specs=out_specs_of(width, t_len // OUT_ROWS),
        out_specs=pl.BlockSpec((OUT_ROWS, d_model), lambda i: (i, 0)),
        out_shape=jax.ShapeDtypeStruct((t_len, d_model), F32),
        compiler_params=pltpu.CompilerParams(vmem_limit_bytes=60 * 1024 * 1024, dimension_semantics=('arbitrary',)),
        cost_estimate=pl.CostEstimate(flops=2 * t_len * d_model * width * N_PART, bytes_accessed=50_000_000, transcendentals=0),
    )(*parts, *[array for array, _ in weights])


def fwd_own_kernel(cols, cp_ref, *refs):
    o_refs = refs[2 * N_PART:2 * N_PART + 8]
    wo_ref, x_ref, got_ref, bias_ref, out_ref, o_s, w_s, sems = refs[2 * N_PART + 8:]
    ready = fetch_weights(refs[N_PART:2 * N_PART], cols, w_s, sems)
    flip = (pl.program_id(0) // 2) ^ cp_ref[0]
    half = o_s.shape[1] // 2
    for i in range(4):
        @pl.when(flip == i)
        def _():
            o_s[:, :half] = o_refs[2 * i][0]
            o_s[:, half:] = o_refs[2 * i + 1][0]
    out = dot_nn(o_s[...], wo_ref[...]) + fwd_product(refs[:N_PART], w_s, ready)
    out_ref[...] = (x_ref[...].astype(F32) + out + got_ref[...] + bias_ref[...]).astype(BF16)


def bwd_own_kernel(cols, cp_ref, *refs):
    d_refs = refs[2 * N_PART:2 * N_PART + 4]
    wqkv_ref, x_ref, g_ref, got_ref, scale_ref, d_x_ref, sums_ref, d_s, w_s, sems = refs[2 * N_PART + 4:]
    ready = fetch_weights(refs[N_PART:2 * N_PART], cols, w_s, sems)
    flip = (pl.program_id(0) // 2) ^ cp_ref[0]
    for i in range(4):
        @pl.when(flip == i)
        def _():
            d_s[...] = d_refs[i][0]

    @pl.when(pl.program_id(0) == 0)
    def _():
        sums_ref[...] = jnp.zeros_like(sums_ref)

    d_n = dot_nt(d_s[...], wqkv_ref[...]) + got_ref[...] + bwd_product(refs[:N_PART], w_s, ready)
    x_f = x_ref[...].astype(F32)
    g_f = g_ref[...].astype(F32)
    inv = lax.rsqrt(jnp.mean(x_f * x_f, axis=1, keepdims=True) + 1e-6)
    scaled = d_n * (1.0 + scale_ref[...])
    xn = x_f * inv
    proj = jnp.mean(scaled * xn, axis=1, keepdims=True)
    d_x_ref[...] = (g_f + inv * (scaled - xn * proj)).astype(BF16)
    rows, d_model = x_f.shape
    sums_ref[:8, :] += jnp.sum((d_n * xn).reshape(rows // 8, 8, d_model), axis=0)
    sums_ref[8:, :] += jnp.sum(g_f.reshape(rows // 8, 8, d_model), axis=0)


def own_call(kernel, cp_index, parts, weights, w_width, w_off, od_blocks, od_got, od_cols, od_width, rest, rest_specs, out_specs, out_shape, scratch):
    t_len, width = parts[0].shape[0] // 2, parts[0].shape[1]
    specs = out_specs_of(width, 0)
    args = list(parts) + [array for array, _ in weights]
    for i, source in enumerate([od_blocks] + od_got):
        for col in od_cols:
            if i == 0:
                specs.append(pl.BlockSpec((1, OUT_ROWS, od_width), lambda j, cp, col=col: (cp[0], jnp.clip(j - 2 * cp[0], 0, 1), col)))
            else:
                specs.append(pl.BlockSpec((1, OUT_ROWS, od_width), lambda j, cp, col=col, i=i: (0, jnp.clip(j - 2 * (cp[0] ^ i), 0, 1), col)))
            args.append(source)
    return pl.pallas_call(
        functools.partial(kernel, [w_off(col) for _, col in weights]),
        grid_spec=pltpu.PrefetchScalarGridSpec(
            num_scalar_prefetch=1, grid=(t_len // OUT_ROWS,), in_specs=specs + rest_specs, out_specs=out_specs, scratch_shapes=scratch + weight_scratch(weights, w_width)),
        out_shape=out_shape,
        compiler_params=pltpu.CompilerParams(vmem_limit_bytes=62 * 1024 * 1024, dimension_semantics=('arbitrary',)),
        cost_estimate=pl.CostEstimate(flops=2 * t_len * weights[0][0].shape[0] * (width * N_PART + 1024), bytes_accessed=80_000_000, transcendentals=0),
    )(cp_index[None], *args, *rest)


def pack_kernel(wq_ref, wk_ref, wv_ref, wo_ref, out_ref):
    r_o, d_model = wo_ref.shape
    qk = wq_ref.shape[1]
    out_ref[:r_o, :d_model] = wo_ref[...].astype(BF16)
    out_ref[:r_o, d_model:] = jnp.zeros((r_o, out_ref.shape[1] - d_model), BF16)
    out_ref[r_o:, :qk] = wq_ref[...].astype(BF16)
    out_ref[r_o:, qk:qk + HEAD_DIM] = wk_ref[...].astype(BF16)
    out_ref[r_o:, qk + HEAD_DIM:] = wv_ref[...].astype(BF16)


def pack(w_q, w_k, w_v, w_o):
    out = jax.ShapeDtypeStruct((w_o.shape[0] + w_q.shape[0], w_q.shape[1] + 2 * HEAD_DIM), BF16)
    return pl.pallas_call(pack_kernel, out_shape=out, name='pack')(w_q, w_k, w_v, w_o)


def vector_kernel(scale_ref, bo_ref, bd_ref, b1_ref, b2_ref, out_ref, side_s):
    side_s[...] = jnp.zeros_like(side_s)
    for row, ref in enumerate((scale_ref, bo_ref, bd_ref, b1_ref, b2_ref)):
        side_s[row:row + 1, :ref.shape[1]] = ref[...]
    out_ref[...] = side_s[...].astype(BF16)


def vectors(*parts):
    width = -(-max(part.shape[0] for part in parts) // 128) * 128
    return pl.pallas_call(
        vector_kernel, out_shape=jax.ShapeDtypeStruct((8, width), BF16), scratch_shapes=[pltpu.VMEM((8, width), F32)], name='vectors',
    )(*[part[None] for part in parts])


def solution(mesh):
    mesh4 = Mesh(mesh.devices.reshape(2, 2, 2, 2), ALL_AXES)
    tok_spec = P(('x', 'core'), ('z', 'y'), None)
    pos_spec = P(('x', 'core'), ('z', 'y'))
    vec_spec = P(ALL_AXES)
    mat_spec = P(ALL_AXES, None)
    param_specs = (vec_spec, mat_spec, mat_spec, mat_spec, mat_spec, vec_spec, mat_spec, vec_spec, mat_spec, vec_spec, mat_spec, vec_spec)

    def swap_core(values):
        return lax.ppermute(values, 'core', [(0, 1), (1, 0)])

    def scatter_by_hand(keep, send):
        def shift(values, axis):
            return lax.ppermute(values, axis, [(0, 1), (1, 0)])

        keep_a, send_a, keep_b, send_b = fold_first(keep, shift(send, 'x'))
        keep_a, send_a, keep_b, send_b = fold_second(keep_a, shift(send_a, 'z'), keep_b, shift(send_b, 'y'))
        return fold_third(keep_a, shift(send_a, 'y'), keep_b, shift(send_b, 'z'))

    def after(value, *deps):
        return lax.optimization_barrier((value,) + deps)[0]

    def send_blocks(values, cp_index, width=None):
        got = []
        for flip in (1, 2, 3):
            sent = lax.dynamic_index_in_dim(values, cp_index ^ flip, 0, keepdims=True)[..., :width]
            got.append(lax.ppermute(sent, ('z', 'y'), [(i, i ^ flip) for i in range(4)]))
        return got

    def local_step(x_in, grad_out, seg_id, seg_pos, norm_scale, w_q, w_k, w_v, w_o, b_o, w_up1, b_up1, w_up2, b_up2, w_down, b_down):
        n_seq, piece, d_model = x_in.shape
        t_len = n_seq * piece
        core = lax.axis_index('core')
        cp_index = lax.axis_index('z') * 2 + lax.axis_index('y')
        first = core == 0
        r_in = w_q.shape[0]
        r_o = w_o.shape[0]
        f_blk = b_up1.shape[0]
        sub = f_blk // N_PART
        qk = N_HEADS * HEAD_DIM

        seg_pack = jnp.stack([seg_id, seg_pos], axis=1)
        seg_got = send_blocks(seg_pack, cp_index)
        g_got = send_blocks(grad_out, cp_index)

        keep, send = split_up(w_up1, w_up2)
        shards = stack_up(keep, swap_core(send), w_down, pack(w_q, w_k, w_v, w_o))

        def gather(shard):
            return lax.all_gather(shard, CHIPS, axis=0, tiled=True)

        whole = [gather(shards[0]), gather(shards[1])]
        weights = [(whole[0], 0), (whole[1], 0), (whole[1], 1)]

        vec_all = lax.all_gather(vectors(norm_scale, b_o, b_down, b_up1, b_up2), ALL_AXES, axis=0)
        scale_f, bo_f, bd_f = [vec_all[:, i, :r_in].reshape(1, d_model).astype(F32) for i in range(3)]
        b_ups = []
        for row in (3, 4):
            both = vec_all[:, row, :f_blk].reshape(8, 2, N_PART, sub)
            mine = jnp.where(first, both[:, 0], both[:, 1]).astype(F32)
            b_ups.append([mine[:, part].reshape(1, d_model) for part in range(N_PART)])

        x_loc = x_in.reshape(t_len, d_model)
        ng_own = norm_and_grad(x_loc, grad_out.reshape(t_len, d_model), scale_f)
        ng_oth = swap_core(ng_own)
        ng_blocks = ng_own.reshape(n_seq, piece, 2 * d_model)
        n_got = send_blocks(ng_blocks, cp_index, d_model)

        seg_all = jnp.zeros_like(seg_pack)
        for flip, got in enumerate([lax.dynamic_index_in_dim(seg_pack, cp_index, 0, keepdims=True)] + seg_got):
            seg_all = lax.dynamic_update_slice_in_dim(seg_all, got, cp_index ^ flip, 0)
        seg_own = seg_all[:, 0].reshape(t_len)
        pos_own = seg_all[:, 1].reshape(t_len)
        half = ROPE_DIMS // 2
        inv_freq = 10000.0 ** (-jnp.arange(half, dtype=F32) / half)
        angle = pos_own.astype(F32)[:, None] * inv_freq
        cos_a = jnp.cos(angle)
        sin_a = jnp.sin(angle)
        cos_b = jnp.concatenate([cos_a, cos_a], axis=1)
        sin_b = jnp.concatenate([-sin_a, sin_a], axis=1)

        acts, dhs, dbs, owns, recvs = [], [], [], [], []

        def third(part, ng_in, extra=()):
            act, dh, *d_w, db = hidden_part(ng_in, ng_oth, weights[part], b_ups[0][part], b_ups[1][part], extra, halves=part == 0)
            if part == 0:
                own = scatter_by_hand(*d_w)
            else:
                own = lax.psum_scatter(d_w[0], CHIPS, scatter_dimension=0, tiled=True)
            recvs.append(swap_core(jnp.where(first, own[r_in:, :2 * d_model], own[:r_in, :2 * d_model])))
            acts.append(act)
            dhs.append(dh)
            dbs.append(jnp.sum(db.reshape(2, 8, d_model), axis=1).reshape(2, 8, sub))
            owns.append(own)

        third(0, ng_own)
        extra_own = whole[0][:, 3 * d_model:]
        wqkv, wo = unpack(extra_own, swap_core(extra_own), r_o, r_in, d_model)
        od_seq = attention(cp_index, ng_blocks, n_got, g_got, wqkv, wo, cos_b, sin_b, seg_own)
        third(1, ng_own)
        d_keep, d_send = attn_grad(cp_index, ng_blocks, n_got, g_got, od_seq, r_o, r_in)
        od_blocks = od_seq.reshape(n_seq, piece, -1)
        od_got = send_blocks(od_blocks, cp_index)
        third(2, ng_own, (d_keep, swap_core(d_send)))

        wd_off = lambda col: (3 * col + 2) * d_model
        w12_off = lambda col: 3 * col * d_model
        tile = lambda width, col=0: pl.BlockSpec((OUT_ROWS, width), lambda i, *_: (i, col))
        full = lambda a: pl.BlockSpec(a.shape, lambda i, *_: (0, 0), pipeline_mode=pl.Buffered(1))
        out_oth = out_other(acts, weights, fwd_product, d_model, wd_off)
        dn_oth = out_other(after(tuple(dhs), out_oth), weights, bwd_product, 2 * d_model, w12_off)
        bias_f = bo_f + bd_f
        x_out = own_call(fwd_own_kernel, cp_index, after(tuple(acts), dn_oth), weights, d_model, wd_off, od_blocks, od_got, (3, 4), 512,
                         [wo, x_loc, swap_core(out_oth), bias_f], [full(wo), tile(d_model), tile(d_model), full(bias_f)],
                         tile(d_model), jax.ShapeDtypeStruct((t_len, d_model), BF16), [pltpu.VMEM((OUT_ROWS, qk), BF16)])
        d_x, sums = own_call(bwd_own_kernel, cp_index, after(tuple(dhs), x_out), weights, 2 * d_model, w12_off, od_blocks, od_got, (0,), qk + 2 * HEAD_DIM,
                             [wqkv, x_loc, ng_own, swap_core(dn_oth), scale_f],
                             [full(wqkv), tile(d_model), tile(d_model, 1), tile(d_model), full(scale_f)],
                             [tile(d_model), pl.BlockSpec((16, d_model), lambda i, *_: (0, 0))],
                             [jax.ShapeDtypeStruct((t_len, d_model), BF16), jax.ShapeDtypeStruct((16, d_model), F32)],
                             [pltpu.VMEM((OUT_ROWS, qk + 2 * HEAD_DIM), BF16)])
        x_out = x_out.reshape(n_seq, piece, d_model)
        d_x = d_x.reshape(n_seq, piece, d_model)

        sums = jnp.sum(sums.reshape(2, 8, d_model), axis=1).reshape(2, 16, r_in)
        db = jnp.stack(dbs, axis=2).reshape(2, 8, f_blk)
        zero = jnp.zeros_like(db)
        db = jnp.where(first, jnp.stack([db, zero], axis=2), jnp.stack([zero, db], axis=2)).reshape(2, 16, f_blk)
        small = jnp.concatenate([sums[0], sums[1], db[0], db[1]], axis=1)
        small = jnp.pad(small, ((0, 0), (0, 1024 - small.shape[1]))).reshape(16, 8, 128)
        small = small_sum(small).reshape(1024)
        g_scale, g_bias, g_b1, g_b2 = small[:r_in], small[r_in:2 * r_in], small[2 * r_in:2 * r_in + f_blk], small[2 * r_in + f_blk:2 * r_in + 2 * f_blk]

        g_w1, g_w2, g_wd = join_up(owns, recvs)
        g_attn = owns[2][:r_o + r_in, 3 * d_model:]
        g_wo, g_wq, g_wk, g_wv = g_attn[:r_o, :d_model], g_attn[r_o:, :qk], g_attn[r_o:, qk:qk + HEAD_DIM], g_attn[r_o:, qk + HEAD_DIM:]
        return (x_out, d_x, g_scale, g_wq, g_wk, g_wv, g_wo, g_bias, g_w1, g_b1, g_w2, g_b2, g_wd, g_bias)

    in_specs = (tok_spec, tok_spec, pos_spec, pos_spec) + param_specs
    out_specs = (tok_spec, tok_spec) + param_specs
    return jax.shard_map(local_step, mesh=mesh4, in_specs=in_specs, out_specs=out_specs, check_vma=False)
```

```python
import functools
import jax
import jax.numpy as jnp
from jax import lax
from jax.experimental import pallas as pl
from jax.experimental.pallas import tpu as pltpu
from jax.sharding import Mesh, PartitionSpec as P


ROPE_DIMS = 128
HEAD_DIM = 256
N_HEADS = 4
MASKED = -1.6e31
EXP_SCALE = 1.4426950408889634 / 16.0
CHIPS = ('z', 'y', 'x')
ALL_AXES = ('z', 'y', 'x', 'core')
F32 = jnp.float32
BF16 = jnp.bfloat16


def dot_nn(a, b):
    return lax.dot_general(a, b, (((1,), (0,)), ((), ())), preferred_element_type=F32)


def dot_nt(a, b):
    return lax.dot_general(a, b, (((1,), (1,)), ((), ())), preferred_element_type=F32)


def dot_tn(a, b):
    return lax.dot_general(a, b, (((0,), (0,)), ((), ())), preferred_element_type=F32)


def rotate(values, cos_b, sin_b):
    return values * cos_b + pltpu.roll(values, ROPE_DIMS // 2, axis=1) * sin_b


def attn_kernel(cp_ref, own_ref, n1_ref, n2_ref, n3_ref, g1_ref, g2_ref, g3_ref, wqkv_ref, wo_ref, cos_ref, sin_ref, cosk_ref, sink_ref, segq_ref, segk_ref, out_ref,
                n_buf, g_buf, sems, q_s, do_s, k_s, v_s, kt_s, vt_s, mask_s, s_s, p_s, dk_s, dv_s):
    step = pl.program_id(0)
    n_blocks = pl.num_programs(0)
    rows, d_model = n_buf.shape[1:]
    qk = N_HEADS * HEAD_DIM
    base = pl.multiple_of(step * rows, rows)
    cos_b = cos_ref[...]
    sin_b = sin_ref[...]
    slot = lax.rem(step, 2)

    def fetch(at_step):
        flip = at_step ^ cp_ref[0]
        to = lax.rem(at_step, 2)
        own = own_ref.at[cp_ref[0]]
        sources = ((own.at[:, :d_model], own.at[:, d_model:]), (n1_ref.at[0], g1_ref.at[0]), (n2_ref.at[0], g2_ref.at[0]), (n3_ref.at[0], g3_ref.at[0]))
        for i, (n_src, g_src) in enumerate(sources):
            @pl.when(flip == i)
            def _():
                pltpu.make_async_copy(n_src, n_buf.at[to], sems.at[0, to]).start()
                pltpu.make_async_copy(g_src, g_buf.at[to], sems.at[1, to]).start()

    pl.when(step == 0)(lambda: fetch(step))
    pl.when(step + 1 < n_blocks)(lambda: fetch(step + 1))
    pltpu.make_async_copy(n1_ref.at[0], n_buf.at[slot], sems.at[0, slot]).wait()
    pltpu.make_async_copy(g1_ref.at[0], g_buf.at[slot], sems.at[1, slot]).wait()
    n_blk = n_buf[slot]
    g_blk = g_buf[slot]

    @pl.when(step == 0)
    def _():
        dk_s[...] = jnp.zeros_like(dk_s)
        dv_s[...] = jnp.zeros_like(dv_s)

    for h in range(N_HEADS):
        lin = dot_nn(n_blk, wqkv_ref[:, h * HEAD_DIM:(h + 1) * HEAD_DIM])
        q_s[h, :, :ROPE_DIMS] = rotate(lin[:, :ROPE_DIMS], cos_b, sin_b).astype(BF16)
        q_s[h, :, ROPE_DIMS:] = lin[:, ROPE_DIMS:].astype(BF16)
        do_s[h] = dot_nt(g_blk, wo_ref[h * HEAD_DIM:(h + 1) * HEAD_DIM, :]).astype(BF16)
    k_lin = dot_nn(n_blk, wqkv_ref[:, qk:qk + HEAD_DIM])
    k_blk = jnp.concatenate([rotate(k_lin[:, :ROPE_DIMS], cos_b, sin_b), k_lin[:, ROPE_DIMS:]], axis=1)
    v_blk = dot_nn(n_blk, wqkv_ref[:, qk + HEAD_DIM:])
    k_s[pl.ds(base, rows), :] = k_blk.astype(BF16)
    v_s[pl.ds(base, rows), :] = v_blk.astype(BF16)
    kt_s[:, pl.ds(base, rows)] = k_blk.T.astype(BF16)
    vt_s[:, pl.ds(base, rows)] = v_blk.T.astype(BF16)

    def block(blk):
        n_chunk = blk + 1
        seg_q = segq_ref[:, :1]
        for c in range(n_chunk):
            same = seg_q == segk_ref[:1, c * rows:(c + 1) * rows]
            if c == blk:
                r_id = lax.broadcasted_iota(jnp.int32, (rows, rows), 0)
                c_id = lax.broadcasted_iota(jnp.int32, (rows, rows), 1)
                same = same & (c_id <= r_id)
            mask_s[:, c * rows:(c + 1) * rows] = jnp.where(same, 1.0, 0.0)

        def head(h, carry):
            q = q_s[h]
            do = do_s[h]
            m_run = None
            for c in range(n_chunk):
                sl = slice(c * rows, (c + 1) * rows)
                s = jnp.where(mask_s[:, sl] > 0.5, dot_nn(q, kt_s[:, sl]), MASKED)
                s_s[:, sl] = s
                m_c = jnp.max(s, axis=1, keepdims=True)
                m_run = m_c if m_run is None else jnp.maximum(m_run, m_c)
            l_run = None
            for c in range(n_chunk):
                sl = slice(c * rows, (c + 1) * rows)
                e = jnp.exp2((s_s[:, sl] - m_run) * EXP_SCALE)
                s_s[:, sl] = e
                l_c = jnp.sum(e, axis=1, keepdims=True)
                l_run = l_c if l_run is None else l_run + l_c
            inv = 1.0 / l_run
            for c in range(n_chunk):
                sl = slice(c * rows, (c + 1) * rows)
                p = s_s[:, sl] * inv
                s_s[:, sl] = p
                p_s[:, sl] = p.astype(BF16)
            o = dot_nn(p_s[:, :n_chunk * rows], v_s[:n_chunk * rows, :])
            delta = jnp.sum(o * do.astype(F32), axis=1, keepdims=True)
            out_ref[pl.ds(base, rows), pl.ds(pl.multiple_of(qk + 2 * HEAD_DIM + h * HEAD_DIM, HEAD_DIM), HEAD_DIM)] = o.astype(BF16)
            dq = None
            for c in range(n_chunk):
                sl = slice(c * rows, (c + 1) * rows)
                ds = (s_s[:, sl] * (dot_nn(do, vt_s[:, sl]) - delta)).astype(BF16)
                dq_c = dot_nn(ds, k_s[sl, :])
                dq = dq_c if dq is None else dq + dq_c
                dk_s[sl, :] += dot_tn(ds, q)
                dv_s[sl, :] += dot_tn(p_s[:, sl], do)
            dq = dq * 0.0625
            dq = jnp.concatenate([rotate(dq[:, :ROPE_DIMS], cos_b, -sin_b), dq[:, ROPE_DIMS:]], axis=1)
            out_ref[pl.ds(base, rows), pl.ds(pl.multiple_of(h * HEAD_DIM, HEAD_DIM), HEAD_DIM)] = dq.astype(BF16)
            return carry

        lax.fori_loop(0, N_HEADS, head, 0)

    for blk in range(4):
        pl.when(step == blk)(functools.partial(block, blk))

    @pl.when(step == n_blocks - 1)
    def _():
        dk = dk_s[...] * 0.0625
        dk = jnp.concatenate([rotate(dk[:, :ROPE_DIMS], cosk_ref[...], -sink_ref[...]), dk[:, ROPE_DIMS:]], axis=1)
        out_ref[:, qk:qk + HEAD_DIM] = dk.astype(BF16)
        out_ref[:, qk + HEAD_DIM:qk + 2 * HEAD_DIM] = dv_s[...].astype(BF16)


def attention(cp_index, ng_blocks, n_got, g_got, wqkv, wo, cos_b, sin_b, seg_own):
    _, rows, both = ng_blocks.shape
    t_len = 4 * rows
    qk = N_HEADS * HEAD_DIM
    segq = jnp.broadcast_to(seg_own[:, None], (t_len, 128))
    segk = jnp.broadcast_to(seg_own[None, :], (8, t_len))
    row_spec = lambda width: pl.BlockSpec((rows, width), lambda i, cp: (i, 0))
    full = lambda a: pl.BlockSpec(a.shape, lambda i, cp: (0,) * a.ndim, pipeline_mode=pl.Buffered(1))
    anywhere = pl.BlockSpec(memory_space=pl.ANY)
    width = 2 * (qk + HEAD_DIM)
    return pl.pallas_call(
        attn_kernel,
        grid_spec=pltpu.PrefetchScalarGridSpec(
            num_scalar_prefetch=1,
            grid=(4,),
            in_specs=[anywhere] * 7 + [full(wqkv), full(wo), row_spec(ROPE_DIMS), row_spec(ROPE_DIMS), full(cos_b), full(sin_b), row_spec(128), full(segk)],
            out_specs=pl.BlockSpec((t_len, width), lambda i, cp: (0, 0)),
            scratch_shapes=[
                pltpu.VMEM((2, rows, both // 2), BF16), pltpu.VMEM((2, rows, both // 2), BF16), pltpu.SemaphoreType.DMA((2, 2)),
                pltpu.VMEM((N_HEADS, rows, HEAD_DIM), BF16), pltpu.VMEM((N_HEADS, rows, HEAD_DIM), BF16),
                pltpu.VMEM((t_len, HEAD_DIM), BF16), pltpu.VMEM((t_len, HEAD_DIM), BF16),
                pltpu.VMEM((HEAD_DIM, t_len), BF16), pltpu.VMEM((HEAD_DIM, t_len), BF16),
                pltpu.VMEM((rows, t_len), F32), pltpu.VMEM((rows, t_len), F32), pltpu.VMEM((rows, t_len), BF16),
                pltpu.VMEM((t_len, HEAD_DIM), F32), pltpu.VMEM((t_len, HEAD_DIM), F32)]),
        out_shape=jax.ShapeDtypeStruct((t_len, width), BF16),
        compiler_params=pltpu.CompilerParams(vmem_limit_bytes=62 * 1024 * 1024, dimension_semantics=('arbitrary',)),
        cost_estimate=pl.CostEstimate(flops=45_000_000_000, bytes_accessed=40_000_000, transcendentals=10_000_000),
        name='attn',
    )(cp_index[None], ng_blocks, *n_got, *g_got, wqkv, wo, cos_b, sin_b, cos_b, sin_b, segq, segk)


def norm_kernel(x_ref, g_ref, scale_ref, out_ref):
    d_model = x_ref.shape[1]
    for part in range(0, x_ref.shape[0], 128):
        sl = slice(part, part + 128)
        x_f = x_ref[sl, :].astype(F32)
        inv = lax.rsqrt(jnp.mean(x_f * x_f, axis=1, keepdims=True) + 1e-6)
        out_ref[sl, :d_model] = (x_f * inv * (1.0 + scale_ref[...])).astype(BF16)
        out_ref[sl, d_model:] = g_ref[sl, :]


def norm_and_grad(x_loc, g_loc, scale_f):
    t_len, d_model = x_loc.shape
    rows = 512
    tile = pl.BlockSpec((rows, d_model), lambda i: (i, 0))
    return pl.pallas_call(
        norm_kernel, grid=(t_len // rows,), name='norm',
        in_specs=[tile, tile, pl.BlockSpec(scale_f.shape, lambda i: (0, 0))],
        out_specs=pl.BlockSpec((rows, 2 * d_model), lambda i: (i, 0)),
        out_shape=jax.ShapeDtypeStruct((t_len, 2 * d_model), BF16),
        cost_estimate=pl.CostEstimate(flops=4_000_000_000, bytes_accessed=19_000_000, transcendentals=2048),
    )(x_loc, g_loc, scale_f)


N_PART = 3


def split_kernel(w1_ref, w2_ref, keep_ref, send_ref):
    core = lax.axis_index('core')
    d_model = keep_ref.shape[2] // 2
    sub = d_model // 8
    for part in range(N_PART):
        for i, w_ref in enumerate((w1_ref, w2_ref)):
            even, odd = [
                jnp.concatenate([w_ref[:, ((2 * j + k) * N_PART + part) * sub:((2 * j + k) * N_PART + part + 1) * sub] for j in range(8)], axis=1).astype(BF16)
                for k in range(2)]

            @pl.when(core == 0)
            def _():
                keep_ref[part, :, i * d_model:(i + 1) * d_model] = even
                send_ref[part, :, i * d_model:(i + 1) * d_model] = odd

            @pl.when(core == 1)
            def _():
                keep_ref[part, :, i * d_model:(i + 1) * d_model] = odd
                send_ref[part, :, i * d_model:(i + 1) * d_model] = even


def split_up(w1, w2):
    rows, cols = w1.shape
    out = jax.ShapeDtypeStruct((N_PART, rows, cols // N_PART), BF16)
    return pl.pallas_call(split_kernel, out_shape=[out, out], name='split_up')(w1, w2)


def stack_kernel(keep_ref, recv_ref, wd_ref, extra_ref, first_ref, rest_ref):
    core = lax.axis_index('core')
    rows, cols = keep_ref.shape[1:]
    d_model = wd_ref.shape[1]
    own = pl.multiple_of(core * rows, 8)
    oth = pl.multiple_of(rows - own, 8)
    for part in range(N_PART):
        out_ref, base = (first_ref, 0) if part == 0 else (rest_ref, (part - 1) * (cols + d_model))
        out_ref[pl.ds(own, rows), base:base + cols] = keep_ref[part]
        out_ref[pl.ds(oth, rows), base:base + cols] = recv_ref[part]
        out_ref[:, base + cols:base + cols + d_model] = wd_ref[part * 2 * rows:(part + 1) * 2 * rows, :].astype(BF16)
    n_extra = extra_ref.shape[0]
    first_ref[:n_extra, cols + d_model:] = extra_ref[...]
    first_ref[n_extra:, cols + d_model:] = jnp.zeros((2 * rows - n_extra, extra_ref.shape[1]), BF16)


def stack_up(keep, recv, w_down, extra):
    _, rows, cols = keep.shape
    width = cols + w_down.shape[1]
    outs = [jax.ShapeDtypeStruct((2 * rows, width + extra.shape[1]), BF16), jax.ShapeDtypeStruct((2 * rows, (N_PART - 1) * width), BF16)]
    return pl.pallas_call(stack_kernel, out_shape=outs, name='stack_up')(keep, recv, w_down, extra)


def unpack_kernel(own_ref, oth_ref, wqkv_ref, wo_ref):
    core = lax.axis_index('core')
    r_o, r_in = wo_ref.shape[0] // 16, wqkv_ref.shape[0] // 16
    d_model = wo_ref.shape[1]
    rows = own_ref.shape[0] // 8
    for chip in range(8):
        for flip, ref in enumerate((own_ref, oth_ref)):
            dev = 2 * chip + (core ^ flip)
            wo_ref[pl.ds(pl.multiple_of(dev * r_o, 8), r_o), :] = ref[chip * rows:chip * rows + r_o, :d_model]
            wqkv_ref[pl.ds(pl.multiple_of(dev * r_in, 8), r_in), :] = ref[chip * rows + r_o:chip * rows + r_o + r_in, :]


def unpack(own, oth, r_o, r_in, d_model):
    return pl.pallas_call(
        unpack_kernel, name='unpack',
        out_shape=[jax.ShapeDtypeStruct((16 * r_in, own.shape[1]), BF16), jax.ShapeDtypeStruct((16 * r_o, d_model), BF16)],
    )(own, oth)


def join_kernel(*refs):
    own_refs, recv_refs, (w1_ref, w2_ref, wd_ref) = refs[:N_PART], refs[N_PART:2 * N_PART], refs[2 * N_PART:]
    core = lax.axis_index('core')
    rows = w1_ref.shape[0]
    d_model = wd_ref.shape[1]
    sub = d_model // 8

    def put(even_of, odd_of):
        for i, w_ref in enumerate((w1_ref, w2_ref)):
            pieces = []
            for j in range(8):
                for of in (even_of, odd_of):
                    for part in range(N_PART):
                        pieces.append(of(part)[:, i * d_model + j * sub:i * d_model + (j + 1) * sub])
            w_ref[...] = jnp.concatenate(pieces, axis=1)

    pl.when(core == 0)(lambda: put(lambda p: own_refs[p][:rows, :2 * d_model], lambda p: recv_refs[p][...]))
    pl.when(core == 1)(lambda: put(lambda p: recv_refs[p][...], lambda p: own_refs[p][rows:, :2 * d_model]))
    for part in range(N_PART):
        wd_ref[part * 2 * rows:(part + 1) * 2 * rows, :] = own_refs[part][:, 2 * d_model:3 * d_model]


def join_up(owns, recvs):
    rows, cols = recvs[0].shape
    d_model = cols // 2
    up = jax.ShapeDtypeStruct((rows, N_PART * cols), F32)
    return pl.pallas_call(
        join_kernel, out_shape=[up, up, jax.ShapeDtypeStruct((N_PART * 2 * rows, d_model), F32)], name='join_up',
    )(*owns, *recvs)


GELU_C = 0.7978845608028654
GELU_A = 0.044715


def hidden_kernel(own_ref, oth_ref, w_ref, b1_ref, b2_ref, *refs):
    extra_refs = refs[:-10]
    act_ref, dh_ref, dw_ref, db_ref, h_s, da_s, ng_s, acc_s, side_s, sems = refs[-10:]
    step = pl.program_id(0)
    last = pl.num_programs(0) - 1
    rows, d_model = da_s.shape
    own = step < pl.num_programs(0) // 2
    ng_s[...] = jnp.where(own, own_ref[...], oth_ref[...])

    @pl.when(step == 0)
    def _():
        acc_s[...] = jnp.zeros_like(acc_s)
        db_ref[...] = jnp.zeros_like(db_ref)

    n_sub = 2
    sub = rows // n_sub
    w12 = w_ref[:, :2 * d_model]
    for i in range(n_sub):
        sl = slice(i * sub, (i + 1) * sub)
        h_s[sl, :] = dot_nn(ng_s[sl, :d_model], w12)
        da_s[sl, :] = dot_nt(ng_s[sl, d_model:], w_ref[:, 2 * d_model:])
    b1 = b1_ref[...]
    b2 = b2_ref[...]
    for i in range(n_sub):
        sl = slice(i * sub, (i + 1) * sub)
        s1 = None
        s2 = None
        for r in range(i * sub, (i + 1) * sub, 64):
            rs = slice(r, r + 64)
            u = h_s[rs, :d_model] + b1
            v = h_s[rs, d_model:] + b2
            da = da_s[rs, :]
            u2 = u * u
            t = jnp.tanh(u * (GELU_C + (GELU_C * GELU_A) * u2))
            half = 0.5 + 0.5 * t
            gelu = u * half
            slope = half + (half * (1.0 - t)) * (u * (GELU_C + (3.0 * GELU_C * GELU_A) * u2))
            d1 = da * v * slope
            d2 = da * gelu
            act_ref[rs, :] = (gelu * v).astype(BF16)
            dh_ref[rs, :d_model] = d1.astype(BF16)
            dh_ref[rs, d_model:] = d2.astype(BF16)
            p1 = jnp.sum(d1.reshape(8, 8, d_model), axis=0)
            p2 = jnp.sum(d2.reshape(8, 8, d_model), axis=0)
            s1 = p1 if s1 is None else s1 + p1
            s2 = p2 if s2 is None else s2 + p2
        db_ref[:8, :] += s1
        db_ref[8:, :] += s2
        acc_s[:, :2 * d_model] += dot_tn(ng_s[sl, :d_model], dh_ref[sl, :])
        acc_s[:, 2 * d_model:] += dot_tn(act_ref[sl, :], ng_s[sl, d_model:])

    if extra_refs:
        keep_ref, got_ref = extra_refs
        block = side_s.shape[1]
        n_extra = keep_ref.shape[1]
        slot = lax.rem(step, 2)

        def side_copy(at_slot, at_step):
            place = dw_ref.at[pl.ds(pl.multiple_of(at_step * block, 8), block), 3 * d_model:]
            return pltpu.make_async_copy(side_s.at[at_slot], place, sems.at[1 + at_slot])

        @pl.when(step >= 2)
        def _():
            side_copy(slot, step - 2).wait()

        side_s[slot, :n_extra, :] = keep_ref[0] + got_ref[0]
        side_s[slot, n_extra:, :] = jnp.zeros((block - n_extra, keep_ref.shape[2]), F32)
        side_copy(slot, step).start()

        @pl.when(step == last)
        def _():
            side_copy(1 - slot, step - 1).wait()
            side_copy(slot, step).wait()

    @pl.when(step == last)
    def _():
        copy = pltpu.make_async_copy(acc_s, dw_ref.at[:, :3 * d_model], sems.at[0])
        copy.start()
        copy.wait()


def hidden_part(ng_own, ng_oth, weight, b1, b2, extra=()):
    w_part, w_col = weight
    t_len, both = ng_own.shape
    d_model = both // 2
    rows = 512
    steps = 2 * t_len // rows
    half = steps // 2
    own_spec = pl.BlockSpec((rows, both), lambda i: (jnp.minimum(i, half - 1), 0))
    oth_spec = pl.BlockSpec((rows, both), lambda i: (jnp.maximum(i - half, 0), 0))
    full = lambda a, width, col=0: pl.BlockSpec((a.shape[0], width), lambda i: (0, col), pipeline_mode=pl.Buffered(1))
    row = lambda width: pl.BlockSpec((rows, width), lambda i: (i, 0))
    blk = [pl.BlockSpec((1,) + a.shape[1:], lambda i: (i, 0, 0)) for a in extra]
    side = (2, d_model // 8, extra[0].shape[2]) if extra else (2, 8, 128)
    return pl.pallas_call(
        hidden_kernel,
        grid=(steps,),
        in_specs=[own_spec, oth_spec, full(w_part, 3 * d_model, w_col), full(b1, d_model), full(b2, d_model)] + blk,
        out_specs=[row(d_model), row(2 * d_model), pl.BlockSpec(memory_space=pl.ANY), pl.BlockSpec((16, d_model), lambda i: (0, 0))],
        out_shape=[jax.ShapeDtypeStruct((2 * t_len, d_model), BF16), jax.ShapeDtypeStruct((2 * t_len, 2 * d_model), BF16),
                   jax.ShapeDtypeStruct((d_model, 3 * d_model + (extra[0].shape[2] if extra else 0)), F32), jax.ShapeDtypeStruct((16, d_model), F32)],
        scratch_shapes=[pltpu.VMEM((rows, 2 * d_model), F32), pltpu.VMEM((rows, d_model), F32), pltpu.VMEM((rows, both), BF16),
                        pltpu.VMEM((d_model, 3 * d_model), F32), pltpu.VMEM(side, F32), pltpu.SemaphoreType.DMA((3,))],
        compiler_params=pltpu.CompilerParams(vmem_limit_bytes=63 * 1024 * 1024, dimension_semantics=('arbitrary',)),
        cost_estimate=pl.CostEstimate(flops=65_000_000_000, bytes_accessed=70_000_000, transcendentals=4_700_000),
        name='hidden',
    )(ng_own, ng_oth, w_part, b1, b2, *extra)


def attn_grad_kernel(cp_ref, own_ref, n1_ref, n2_ref, n3_ref, g1_ref, g2_ref, g3_ref, dqkv_ref, o_lo_ref, o_hi_ref, keep_ref, send_ref):
    step = pl.program_id(0)
    core = lax.axis_index('core')
    d_model = own_ref.shape[2] // 2
    r_o, r_in = o_lo_ref.shape[1] // 8, d_model // 16
    width = dqkv_ref.shape[1]
    rows = own_ref.shape[1]
    place = [pl.ds(pl.multiple_of((cp_ref[0] ^ flip) * rows, rows), rows) for flip in range(4)]

    def put(at, cols, value_of):
        for dev in range(16):
            for ref, flip in ((keep_ref, 0), (send_ref, 1)):
                @pl.when((core ^ flip) == dev % 2)
                def _():
                    ref[dev // 2, at, cols] = value_of(dev)

    d_wqkv = dot_tn(own_ref[0, :, :d_model], dqkv_ref[place[0], :])
    for flip, n_ref in ((1, n1_ref), (2, n2_ref), (3, n3_ref)):
        d_wqkv = d_wqkv + dot_tn(n_ref[0], dqkv_ref[place[flip], :])
    put(slice(r_o, r_o + r_in), slice(0, width), lambda dev: d_wqkv[dev * r_in:(dev + 1) * r_in])

    def low(first_col, used):
        d_wo = []
        for o_ref in (o_lo_ref, o_hi_ref):
            total = dot_tn(o_ref[place[0], :], own_ref[0, :, d_model + first_col:d_model + first_col + used])
            for flip, g_ref in ((1, g1_ref), (2, g2_ref), (3, g3_ref)):
                total = total + dot_tn(o_ref[place[flip], :], g_ref[0, :, first_col:first_col + used])
            d_wo.append(total)
        put(slice(0, r_o), slice(0, used), lambda dev: d_wo[dev // 8][dev % 8 * r_o:(dev % 8 + 1) * r_o])
        if used < width:
            put(slice(0, r_o), slice(used, width), lambda dev: jnp.zeros((r_o, width - used), F32))

    for i in range(-(-d_model // width)):
        pl.when(step == i)(functools.partial(low, i * width, min(width, d_model - i * width)))


def attn_grad(cp_index, ng_blocks, n_got, g_got, od_seq, r_o, r_in):
    _, rows, both = ng_blocks.shape
    t_len = od_seq.shape[0]
    width = 512
    total = (N_HEADS + 2) * HEAD_DIM
    out = jax.ShapeDtypeStruct((8, r_o + r_in, total), F32)
    out_spec = pl.BlockSpec((8, r_o + r_in, width), lambda i, cp: (0, 0, i))
    one = pl.Buffered(1)
    full = lambda a: pl.BlockSpec(a.shape, lambda i, cp: (0, 0, 0), pipeline_mode=one)
    return pl.pallas_call(
        attn_grad_kernel,
        grid_spec=pltpu.PrefetchScalarGridSpec(
            num_scalar_prefetch=1,
            grid=(total // width,),
            in_specs=[pl.BlockSpec((1, rows, both), lambda i, cp: (cp[0], 0, 0), pipeline_mode=one)] + [full(a) for a in n_got + g_got]
                     + [pl.BlockSpec((t_len, width), lambda i, cp: (0, i)),
                        pl.BlockSpec((t_len, width), lambda i, cp: (0, total // width), pipeline_mode=one),
                        pl.BlockSpec((t_len, width), lambda i, cp: (0, total // width + 1), pipeline_mode=one)],
            out_specs=[out_spec, out_spec]),
        out_shape=[out, out],
        compiler_params=pltpu.CompilerParams(vmem_limit_bytes=60 * 1024 * 1024, dimension_semantics=('arbitrary',)),
        cost_estimate=pl.CostEstimate(flops=12_000_000_000, bytes_accessed=33_000_000, transcendentals=0),
        name='attn_grad',
    )(cp_index[None], ng_blocks, *n_got, *g_got, od_seq, od_seq, od_seq)


def small_kernel(in_ref, out_ref, got_s, send_sems, recv_sems):
    at = [lax.axis_index(axis) for axis in ALL_AXES]
    me = ((at[0] * 2 + at[1]) * 2 + at[2]) * 2 + at[3]

    def peer(flip):
        return tuple(index ^ ((flip >> (3 - i)) & 1) for i, index in enumerate(at))

    barrier = pltpu.get_barrier_semaphore()
    for flip in range(1, 16):
        pl.semaphore_signal(barrier, inc=1, device_id=peer(flip), device_id_type=pl.DeviceIdType.MESH)
    pl.semaphore_wait(barrier, 15)
    copies = []
    for flip in range(1, 16):
        copies.append(pltpu.make_async_remote_copy(
            src_ref=in_ref.at[me ^ flip], dst_ref=got_s.at[flip], send_sem=send_sems.at[flip], recv_sem=recv_sems.at[flip],
            device_id=peer(flip), device_id_type=pl.DeviceIdType.MESH))
        copies[-1].start()
    for copy in copies:
        copy.wait()
    total = in_ref[me]
    for flip in range(1, 16):
        total = total + got_s[flip]
    out_ref[...] = total


def small_sum(values):
    return pl.pallas_call(
        small_kernel, out_shape=jax.ShapeDtypeStruct(values.shape[1:], F32), name='small_sum',
        in_specs=[pl.BlockSpec(memory_space=pltpu.VMEM)], out_specs=pl.BlockSpec(memory_space=pltpu.VMEM),
        scratch_shapes=[pltpu.VMEM(values.shape, F32), pltpu.SemaphoreType.DMA((16,)), pltpu.SemaphoreType.DMA((16,))],
        compiler_params=pltpu.CompilerParams(collective_id=0, has_side_effects=True),
        cost_estimate=pl.CostEstimate(flops=8_000_000_000, bytes_accessed=130_000, transcendentals=0),
    )(values)


def fwd_product(act_refs, w_refs):
    out = dot_nn(act_refs[0][...], w_refs[0][...])
    for act_ref, w_ref in zip(act_refs[1:], w_refs[1:]):
        out = out + dot_nn(act_ref[...], w_ref[...])
    return out


def bwd_product(dh_refs, w_refs):
    out = dot_nt(dh_refs[0][...], w_refs[0][:, :dh_refs[0].shape[1]])
    for dh_ref, w_ref in zip(dh_refs[1:], w_refs[1:]):
        out = out + dot_nt(dh_ref[...], w_ref[:, :dh_ref.shape[1]])
    return out


def other_kernel(product, *refs):
    refs[-1][...] = product(refs[:N_PART], refs[N_PART:2 * N_PART])


OUT_ROWS = 256


def out_specs_of(width, weights, w_width, w_off, first_block):
    tile = pl.BlockSpec((OUT_ROWS, width), lambda i, *_: (i + first_block, 0))
    specs = [tile] * N_PART
    for array, col in weights:
        specs.append(pl.BlockSpec((array.shape[0], w_width), lambda i, *_, at=w_off(col): (0, at), pipeline_mode=pl.Buffered(1)))
    return specs


def out_other(parts, weights, product, w_width, w_off):
    t_len, width = parts[0].shape[0] // 2, parts[0].shape[1]
    d_model = weights[0][0].shape[0]
    return pl.pallas_call(
        functools.partial(other_kernel, product),
        grid=(t_len // OUT_ROWS,),
        in_specs=out_specs_of(width, weights, w_width, w_off, t_len // OUT_ROWS),
        out_specs=pl.BlockSpec((OUT_ROWS, d_model), lambda i: (i, 0)),
        out_shape=jax.ShapeDtypeStruct((t_len, d_model), F32),
        compiler_params=pltpu.CompilerParams(vmem_limit_bytes=60 * 1024 * 1024, dimension_semantics=('arbitrary',)),
        cost_estimate=pl.CostEstimate(flops=2 * t_len * d_model * width * N_PART, bytes_accessed=50_000_000, transcendentals=0),
    )(*parts, *[array for array, _ in weights])


def fwd_own_kernel(cp_ref, *refs):
    o_refs = refs[2 * N_PART:2 * N_PART + 8]
    wo_ref, x_ref, got_ref, bias_ref, out_ref, o_s = refs[2 * N_PART + 8:]
    flip = (pl.program_id(0) // 2) ^ cp_ref[0]
    half = o_s.shape[1] // 2
    for i in range(4):
        @pl.when(flip == i)
        def _():
            o_s[:, :half] = o_refs[2 * i][0]
            o_s[:, half:] = o_refs[2 * i + 1][0]
    out = fwd_product(refs[:N_PART], refs[N_PART:2 * N_PART]) + dot_nn(o_s[...], wo_ref[...])
    out_ref[...] = (x_ref[...].astype(F32) + out + got_ref[...] + bias_ref[...]).astype(BF16)


def bwd_own_kernel(cp_ref, *refs):
    d_refs = refs[2 * N_PART:2 * N_PART + 4]
    wqkv_ref, x_ref, g_ref, got_ref, scale_ref, d_x_ref, sums_ref, d_s = refs[2 * N_PART + 4:]
    flip = (pl.program_id(0) // 2) ^ cp_ref[0]
    for i in range(4):
        @pl.when(flip == i)
        def _():
            d_s[...] = d_refs[i][0]

    @pl.when(pl.program_id(0) == 0)
    def _():
        sums_ref[...] = jnp.zeros_like(sums_ref)

    d_n = bwd_product(refs[:N_PART], refs[N_PART:2 * N_PART]) + dot_nt(d_s[...], wqkv_ref[...]) + got_ref[...]
    x_f = x_ref[...].astype(F32)
    g_f = g_ref[...].astype(F32)
    inv = lax.rsqrt(jnp.mean(x_f * x_f, axis=1, keepdims=True) + 1e-6)
    scaled = d_n * (1.0 + scale_ref[...])
    xn = x_f * inv
    proj = jnp.mean(scaled * xn, axis=1, keepdims=True)
    d_x_ref[...] = (g_f + inv * (scaled - xn * proj)).astype(BF16)
    rows, d_model = x_f.shape
    sums_ref[:8, :] += jnp.sum((d_n * xn).reshape(rows // 8, 8, d_model), axis=0)
    sums_ref[8:, :] += jnp.sum(g_f.reshape(rows // 8, 8, d_model), axis=0)


def own_call(kernel, cp_index, parts, weights, w_width, w_off, od_blocks, od_got, od_cols, od_width, rest, rest_specs, out_specs, out_shape, scratch):
    t_len, width = parts[0].shape[0] // 2, parts[0].shape[1]
    specs = out_specs_of(width, weights, w_width, w_off, 0)
    args = list(parts) + [array for array, _ in weights]
    for i, source in enumerate([od_blocks] + od_got):
        for col in od_cols:
            if i == 0:
                specs.append(pl.BlockSpec((1, OUT_ROWS, od_width), lambda j, cp, col=col: (cp[0], jnp.clip(j - 2 * cp[0], 0, 1), col)))
            else:
                specs.append(pl.BlockSpec((1, OUT_ROWS, od_width), lambda j, cp, col=col, i=i: (0, jnp.clip(j - 2 * (cp[0] ^ i), 0, 1), col)))
            args.append(source)
    return pl.pallas_call(
        kernel,
        grid_spec=pltpu.PrefetchScalarGridSpec(
            num_scalar_prefetch=1, grid=(t_len // OUT_ROWS,), in_specs=specs + rest_specs, out_specs=out_specs, scratch_shapes=scratch),
        out_shape=out_shape,
        compiler_params=pltpu.CompilerParams(vmem_limit_bytes=62 * 1024 * 1024, dimension_semantics=('arbitrary',)),
        cost_estimate=pl.CostEstimate(flops=2 * t_len * weights[0][0].shape[0] * (width * N_PART + 1024), bytes_accessed=80_000_000, transcendentals=0),
    )(cp_index[None], *args, *rest)


def pack_kernel(wq_ref, wk_ref, wv_ref, wo_ref, out_ref):
    r_o, d_model = wo_ref.shape
    qk = wq_ref.shape[1]
    out_ref[:r_o, :d_model] = wo_ref[...].astype(BF16)
    out_ref[:r_o, d_model:] = jnp.zeros((r_o, out_ref.shape[1] - d_model), BF16)
    out_ref[r_o:, :qk] = wq_ref[...].astype(BF16)
    out_ref[r_o:, qk:qk + HEAD_DIM] = wk_ref[...].astype(BF16)
    out_ref[r_o:, qk + HEAD_DIM:] = wv_ref[...].astype(BF16)


def pack(w_q, w_k, w_v, w_o):
    out = jax.ShapeDtypeStruct((w_o.shape[0] + w_q.shape[0], w_q.shape[1] + 2 * HEAD_DIM), BF16)
    return pl.pallas_call(pack_kernel, out_shape=out, name='pack')(w_q, w_k, w_v, w_o)


def vector_kernel(scale_ref, bo_ref, bd_ref, b1_ref, b2_ref, out_ref, side_s):
    side_s[...] = jnp.zeros_like(side_s)
    for row, ref in enumerate((scale_ref, bo_ref, bd_ref, b1_ref, b2_ref)):
        side_s[row:row + 1, :ref.shape[1]] = ref[...]
    out_ref[...] = side_s[...].astype(BF16)


def vectors(*parts):
    width = -(-max(part.shape[0] for part in parts) // 128) * 128
    return pl.pallas_call(
        vector_kernel, out_shape=jax.ShapeDtypeStruct((8, width), BF16), scratch_shapes=[pltpu.VMEM((8, width), F32)], name='vectors',
    )(*[part[None] for part in parts])


def solution(mesh):
    mesh4 = Mesh(mesh.devices.reshape(2, 2, 2, 2), ALL_AXES)
    tok_spec = P(('x', 'core'), ('z', 'y'), None)
    pos_spec = P(('x', 'core'), ('z', 'y'))
    vec_spec = P(ALL_AXES)
    mat_spec = P(ALL_AXES, None)
    param_specs = (vec_spec, mat_spec, mat_spec, mat_spec, mat_spec, vec_spec, mat_spec, vec_spec, mat_spec, vec_spec, mat_spec, vec_spec)

    def swap_core(values):
        return lax.ppermute(values, 'core', [(0, 1), (1, 0)])

    def after(value, *deps):
        return lax.optimization_barrier((value,) + deps)[0]

    def send_blocks(values, cp_index, width=None):
        got = []
        for flip in (1, 2, 3):
            sent = lax.dynamic_index_in_dim(values, cp_index ^ flip, 0, keepdims=True)[..., :width]
            got.append(lax.ppermute(sent, ('z', 'y'), [(i, i ^ flip) for i in range(4)]))
        return got

    def local_step(x_in, grad_out, seg_id, seg_pos, norm_scale, w_q, w_k, w_v, w_o, b_o, w_up1, b_up1, w_up2, b_up2, w_down, b_down):
        n_seq, piece, d_model = x_in.shape
        t_len = n_seq * piece
        core = lax.axis_index('core')
        cp_index = lax.axis_index('z') * 2 + lax.axis_index('y')
        first = core == 0
        r_in = w_q.shape[0]
        r_o = w_o.shape[0]
        f_blk = b_up1.shape[0]
        sub = f_blk // N_PART
        qk = N_HEADS * HEAD_DIM

        seg_pack = jnp.stack([seg_id, seg_pos], axis=1)
        seg_got = send_blocks(seg_pack, cp_index)
        g_got = send_blocks(grad_out, cp_index)

        keep, send = split_up(w_up1, w_up2)
        shards = stack_up(keep, swap_core(send), w_down, pack(w_q, w_k, w_v, w_o))

        def gather(shard):
            return lax.all_gather(shard, CHIPS, axis=0, tiled=True)

        whole = [gather(shards[0]), gather(shards[1])]
        weights = [(whole[0], 0), (whole[1], 0), (whole[1], 1)]

        vec_all = lax.all_gather(vectors(norm_scale, b_o, b_down, b_up1, b_up2), ALL_AXES, axis=0)
        scale_f, bo_f, bd_f = [vec_all[:, i, :r_in].reshape(1, d_model).astype(F32) for i in range(3)]
        b_ups = []
        for row in (3, 4):
            both = vec_all[:, row, :f_blk].reshape(8, 2, N_PART, sub)
            mine = jnp.where(first, both[:, 0], both[:, 1]).astype(F32)
            b_ups.append([mine[:, part].reshape(1, d_model) for part in range(N_PART)])

        x_loc = x_in.reshape(t_len, d_model)
        ng_own = norm_and_grad(x_loc, grad_out.reshape(t_len, d_model), scale_f)
        ng_oth = swap_core(ng_own)
        ng_blocks = ng_own.reshape(n_seq, piece, 2 * d_model)
        n_got = send_blocks(ng_blocks, cp_index, d_model)

        seg_all = jnp.zeros_like(seg_pack)
        for flip, got in enumerate([lax.dynamic_index_in_dim(seg_pack, cp_index, 0, keepdims=True)] + seg_got):
            seg_all = lax.dynamic_update_slice_in_dim(seg_all, got, cp_index ^ flip, 0)
        seg_own = seg_all[:, 0].reshape(t_len)
        pos_own = seg_all[:, 1].reshape(t_len)
        half = ROPE_DIMS // 2
        inv_freq = 10000.0 ** (-jnp.arange(half, dtype=F32) / half)
        angle = pos_own.astype(F32)[:, None] * inv_freq
        cos_a = jnp.cos(angle)
        sin_a = jnp.sin(angle)
        cos_b = jnp.concatenate([cos_a, cos_a], axis=1)
        sin_b = jnp.concatenate([-sin_a, sin_a], axis=1)

        acts, dhs, dbs, owns, recvs = [], [], [], [], []

        def third(part, ng_in, extra=()):
            act, dh, d_w, db = hidden_part(ng_in, ng_oth, weights[part], b_ups[0][part], b_ups[1][part], extra)
            own = lax.psum_scatter(d_w, CHIPS, scatter_dimension=0, tiled=True)
            recvs.append(swap_core(jnp.where(first, own[r_in:, :2 * d_model], own[:r_in, :2 * d_model])))
            acts.append(act)
            dhs.append(dh)
            dbs.append(jnp.sum(db.reshape(2, 8, d_model), axis=1).reshape(2, 8, sub))
            owns.append(own)

        third(0, ng_own)
        extra_own = whole[0][:, 3 * d_model:]
        wqkv, wo = unpack(extra_own, swap_core(extra_own), r_o, r_in, d_model)
        od_seq = attention(cp_index, ng_blocks, n_got, g_got, wqkv, wo, cos_b, sin_b, seg_own)
        d_keep, d_send = attn_grad(cp_index, ng_blocks, n_got, g_got, od_seq, r_o, r_in)
        od_blocks = od_seq.reshape(n_seq, piece, -1)
        od_got = send_blocks(od_blocks, cp_index)
        third(1, ng_own, (d_keep, swap_core(d_send)))
        third(2, ng_own)

        wd_off = lambda col: 3 * col + 2
        w12_off = lambda col: col
        tile = lambda width, col=0: pl.BlockSpec((OUT_ROWS, width), lambda i, *_: (i, col))
        full = lambda a: pl.BlockSpec(a.shape, lambda i, *_: (0, 0), pipeline_mode=pl.Buffered(1))
        out_oth = out_other(acts, weights, fwd_product, d_model, wd_off)
        dn_oth = out_other(after(tuple(dhs), out_oth), weights, bwd_product, 3 * d_model, w12_off)
        bias_f = bo_f + bd_f
        x_out = own_call(fwd_own_kernel, cp_index, after(tuple(acts), dn_oth), weights, d_model, wd_off, od_blocks, od_got, (3, 4), 512,
                         [wo, x_loc, swap_core(out_oth), bias_f], [full(wo), tile(d_model), tile(d_model), full(bias_f)],
                         tile(d_model), jax.ShapeDtypeStruct((t_len, d_model), BF16), [pltpu.VMEM((OUT_ROWS, qk), BF16)])
        d_x, sums = own_call(bwd_own_kernel, cp_index, after(tuple(dhs), x_out), weights, 3 * d_model, w12_off, od_blocks, od_got, (0,), qk + 2 * HEAD_DIM,
                             [wqkv, x_loc, ng_own, swap_core(dn_oth), scale_f],
                             [full(wqkv), tile(d_model), tile(d_model, 1), tile(d_model), full(scale_f)],
                             [tile(d_model), pl.BlockSpec((16, d_model), lambda i, *_: (0, 0))],
                             [jax.ShapeDtypeStruct((t_len, d_model), BF16), jax.ShapeDtypeStruct((16, d_model), F32)],
                             [pltpu.VMEM((OUT_ROWS, qk + 2 * HEAD_DIM), BF16)])
        x_out = x_out.reshape(n_seq, piece, d_model)
        d_x = d_x.reshape(n_seq, piece, d_model)

        sums = jnp.sum(sums.reshape(2, 8, d_model), axis=1).reshape(2, 16, r_in)
        db = jnp.stack(dbs, axis=2).reshape(2, 8, f_blk)
        zero = jnp.zeros_like(db)
        db = jnp.where(first, jnp.stack([db, zero], axis=2), jnp.stack([zero, db], axis=2)).reshape(2, 16, f_blk)
        small = jnp.concatenate([sums[0], sums[1], db[0], db[1]], axis=1)
        small = jnp.pad(small, ((0, 0), (0, 1024 - small.shape[1]))).reshape(16, 8, 128)
        small = small_sum(small).reshape(1024)
        g_scale, g_bias, g_b1, g_b2 = small[:r_in], small[r_in:2 * r_in], small[2 * r_in:2 * r_in + f_blk], small[2 * r_in + f_blk:2 * r_in + 2 * f_blk]

        g_w1, g_w2, g_wd = join_up(owns, recvs)
        g_attn = owns[1][:r_o + r_in, 3 * d_model:]
        g_wo, g_wq, g_wk, g_wv = g_attn[:r_o, :d_model], g_attn[r_o:, :qk], g_attn[r_o:, qk:qk + HEAD_DIM], g_attn[r_o:, qk + HEAD_DIM:]
        return (x_out, d_x, g_scale, g_wq, g_wk, g_wv, g_wo, g_bias, g_w1, g_b1, g_w2, g_b2, g_wd, g_bias)

    in_specs = (tok_spec, tok_spec, pos_spec, pos_spec) + param_specs
    out_specs = (tok_spec, tok_spec) + param_specs
    return jax.shard_map(local_step, mesh=mesh4, in_specs=in_specs, out_specs=out_specs, check_vma=False)
```

```python
import functools
import jax
import jax.numpy as jnp
from jax import lax
from jax.experimental import pallas as pl
from jax.experimental.pallas import tpu as pltpu
from jax.sharding import Mesh, PartitionSpec as P


ROPE_DIMS = 128
HEAD_DIM = 256
N_HEADS = 4
MASKED = -1.6e31
EXP_SCALE = 1.4426950408889634 / 16.0
CHIPS = ('z', 'y', 'x')
ALL_AXES = ('z', 'y', 'x', 'core')
F32 = jnp.float32
BF16 = jnp.bfloat16


def dot_nn(a, b):
    return lax.dot_general(a, b, (((1,), (0,)), ((), ())), preferred_element_type=F32)


def dot_nt(a, b):
    return lax.dot_general(a, b, (((1,), (1,)), ((), ())), preferred_element_type=F32)


def dot_tn(a, b):
    return lax.dot_general(a, b, (((0,), (0,)), ((), ())), preferred_element_type=F32)


def rotate(values, cos_b, sin_b):
    return values * cos_b + pltpu.roll(values, ROPE_DIMS // 2, axis=1) * sin_b


def attn_kernel(cp_ref, own_ref, n1_ref, n2_ref, n3_ref, g1_ref, g2_ref, g3_ref, wqkv_ref, wo_ref, cos_ref, sin_ref, cosk_ref, sink_ref, segq_ref, segk_ref, out_ref,
                n_buf, g_buf, sems, q_s, do_s, k_s, v_s, kt_s, vt_s, mask_s, s_s, p_s, dk_s, dv_s):
    step = pl.program_id(0)
    n_blocks = pl.num_programs(0)
    rows, d_model = n_buf.shape[1:]
    qk = N_HEADS * HEAD_DIM
    base = pl.multiple_of(step * rows, rows)
    cos_b = cos_ref[...]
    sin_b = sin_ref[...]
    slot = lax.rem(step, 2)

    def fetch(at_step):
        flip = at_step ^ cp_ref[0]
        to = lax.rem(at_step, 2)
        own = own_ref.at[cp_ref[0]]
        sources = ((own.at[:, :d_model], own.at[:, d_model:]), (n1_ref.at[0], g1_ref.at[0]), (n2_ref.at[0], g2_ref.at[0]), (n3_ref.at[0], g3_ref.at[0]))
        for i, (n_src, g_src) in enumerate(sources):
            @pl.when(flip == i)
            def _():
                pltpu.make_async_copy(n_src, n_buf.at[to], sems.at[0, to]).start()
                pltpu.make_async_copy(g_src, g_buf.at[to], sems.at[1, to]).start()

    pl.when(step == 0)(lambda: fetch(step))
    pl.when(step + 1 < n_blocks)(lambda: fetch(step + 1))
    pltpu.make_async_copy(n1_ref.at[0], n_buf.at[slot], sems.at[0, slot]).wait()
    pltpu.make_async_copy(g1_ref.at[0], g_buf.at[slot], sems.at[1, slot]).wait()
    n_blk = n_buf[slot]
    g_blk = g_buf[slot]

    @pl.when(step == 0)
    def _():
        dk_s[...] = jnp.zeros_like(dk_s)
        dv_s[...] = jnp.zeros_like(dv_s)

    for h in range(N_HEADS):
        lin = dot_nn(n_blk, wqkv_ref[:, h * HEAD_DIM:(h + 1) * HEAD_DIM])
        q_s[h, :, :ROPE_DIMS] = rotate(lin[:, :ROPE_DIMS], cos_b, sin_b).astype(BF16)
        q_s[h, :, ROPE_DIMS:] = lin[:, ROPE_DIMS:].astype(BF16)
        do_s[h] = dot_nt(g_blk, wo_ref[h * HEAD_DIM:(h + 1) * HEAD_DIM, :]).astype(BF16)
    k_lin = dot_nn(n_blk, wqkv_ref[:, qk:qk + HEAD_DIM])
    k_blk = jnp.concatenate([rotate(k_lin[:, :ROPE_DIMS], cos_b, sin_b), k_lin[:, ROPE_DIMS:]], axis=1)
    v_blk = dot_nn(n_blk, wqkv_ref[:, qk + HEAD_DIM:])
    k_s[pl.ds(base, rows), :] = k_blk.astype(BF16)
    v_s[pl.ds(base, rows), :] = v_blk.astype(BF16)
    kt_s[:, pl.ds(base, rows)] = k_blk.T.astype(BF16)
    vt_s[:, pl.ds(base, rows)] = v_blk.T.astype(BF16)

    def block(blk):
        n_chunk = blk + 1
        seg_q = segq_ref[:, :1]
        for c in range(n_chunk):
            same = seg_q == segk_ref[:1, c * rows:(c + 1) * rows]
            if c == blk:
                r_id = lax.broadcasted_iota(jnp.int32, (rows, rows), 0)
                c_id = lax.broadcasted_iota(jnp.int32, (rows, rows), 1)
                same = same & (c_id <= r_id)
            mask_s[:, c * rows:(c + 1) * rows] = jnp.where(same, 1.0, 0.0)

        def head(h, carry):
            q = q_s[h]
            do = do_s[h]
            m_run = None
            for c in range(n_chunk):
                sl = slice(c * rows, (c + 1) * rows)
                s = jnp.where(mask_s[:, sl] > 0.5, dot_nn(q, kt_s[:, sl]), MASKED)
                s_s[:, sl] = s
                m_c = jnp.max(s, axis=1, keepdims=True)
                m_run = m_c if m_run is None else jnp.maximum(m_run, m_c)
            l_run = None
            for c in range(n_chunk):
                sl = slice(c * rows, (c + 1) * rows)
                e = jnp.exp2((s_s[:, sl] - m_run) * EXP_SCALE)
                s_s[:, sl] = e
                l_c = jnp.sum(e, axis=1, keepdims=True)
                l_run = l_c if l_run is None else l_run + l_c
            inv = 1.0 / l_run
            for c in range(n_chunk):
                sl = slice(c * rows, (c + 1) * rows)
                p = s_s[:, sl] * inv
                s_s[:, sl] = p
                p_s[:, sl] = p.astype(BF16)
            o = dot_nn(p_s[:, :n_chunk * rows], v_s[:n_chunk * rows, :])
            delta = jnp.sum(o * do.astype(F32), axis=1, keepdims=True)
            out_ref[pl.ds(base, rows), pl.ds(pl.multiple_of(qk + 2 * HEAD_DIM + h * HEAD_DIM, HEAD_DIM), HEAD_DIM)] = o.astype(BF16)
            dq = None
            for c in range(n_chunk):
                sl = slice(c * rows, (c + 1) * rows)
                ds = (s_s[:, sl] * (dot_nn(do, vt_s[:, sl]) - delta)).astype(BF16)
                dq_c = dot_nn(ds, k_s[sl, :])
                dq = dq_c if dq is None else dq + dq_c
                dk_s[sl, :] += dot_tn(ds, q)
                dv_s[sl, :] += dot_tn(p_s[:, sl], do)
            dq = dq * 0.0625
            dq = jnp.concatenate([rotate(dq[:, :ROPE_DIMS], cos_b, -sin_b), dq[:, ROPE_DIMS:]], axis=1)
            out_ref[pl.ds(base, rows), pl.ds(pl.multiple_of(h * HEAD_DIM, HEAD_DIM), HEAD_DIM)] = dq.astype(BF16)
            return carry

        lax.fori_loop(0, N_HEADS, head, 0)

    for blk in range(4):
        pl.when(step == blk)(functools.partial(block, blk))

    @pl.when(step == n_blocks - 1)
    def _():
        dk = dk_s[...] * 0.0625
        dk = jnp.concatenate([rotate(dk[:, :ROPE_DIMS], cosk_ref[...], -sink_ref[...]), dk[:, ROPE_DIMS:]], axis=1)
        out_ref[:, qk:qk + HEAD_DIM] = dk.astype(BF16)
        out_ref[:, qk + HEAD_DIM:qk + 2 * HEAD_DIM] = dv_s[...].astype(BF16)


def attention(cp_index, ng_blocks, n_got, g_got, wqkv, wo, cos_b, sin_b, seg_own):
    _, rows, both = ng_blocks.shape
    t_len = 4 * rows
    qk = N_HEADS * HEAD_DIM
    segq = jnp.broadcast_to(seg_own[:, None], (t_len, 128))
    segk = jnp.broadcast_to(seg_own[None, :], (8, t_len))
    row_spec = lambda width: pl.BlockSpec((rows, width), lambda i, cp: (i, 0))
    full = lambda a: pl.BlockSpec(a.shape, lambda i, cp: (0,) * a.ndim, pipeline_mode=pl.Buffered(1))
    anywhere = pl.BlockSpec(memory_space=pl.ANY)
    width = 2 * (qk + HEAD_DIM)
    return pl.pallas_call(
        attn_kernel,
        grid_spec=pltpu.PrefetchScalarGridSpec(
            num_scalar_prefetch=1,
            grid=(4,),
            in_specs=[anywhere] * 7 + [full(wqkv), full(wo), row_spec(ROPE_DIMS), row_spec(ROPE_DIMS), full(cos_b), full(sin_b), row_spec(128), full(segk)],
            out_specs=pl.BlockSpec((t_len, width), lambda i, cp: (0, 0)),
            scratch_shapes=[
                pltpu.VMEM((2, rows, both // 2), BF16), pltpu.VMEM((2, rows, both // 2), BF16), pltpu.SemaphoreType.DMA((2, 2)),
                pltpu.VMEM((N_HEADS, rows, HEAD_DIM), BF16), pltpu.VMEM((N_HEADS, rows, HEAD_DIM), BF16),
                pltpu.VMEM((t_len, HEAD_DIM), BF16), pltpu.VMEM((t_len, HEAD_DIM), BF16),
                pltpu.VMEM((HEAD_DIM, t_len), BF16), pltpu.VMEM((HEAD_DIM, t_len), BF16),
                pltpu.VMEM((rows, t_len), F32), pltpu.VMEM((rows, t_len), F32), pltpu.VMEM((rows, t_len), BF16),
                pltpu.VMEM((t_len, HEAD_DIM), F32), pltpu.VMEM((t_len, HEAD_DIM), F32)]),
        out_shape=jax.ShapeDtypeStruct((t_len, width), BF16),
        compiler_params=pltpu.CompilerParams(vmem_limit_bytes=62 * 1024 * 1024, dimension_semantics=('arbitrary',)),
        cost_estimate=pl.CostEstimate(flops=45_000_000_000, bytes_accessed=40_000_000, transcendentals=10_000_000),
        name='attn',
    )(cp_index[None], ng_blocks, *n_got, *g_got, wqkv, wo, cos_b, sin_b, cos_b, sin_b, segq, segk)


def norm_kernel(x_ref, g_ref, scale_ref, out_ref):
    d_model = x_ref.shape[1]
    for part in range(0, x_ref.shape[0], 128):
        sl = slice(part, part + 128)
        x_f = x_ref[sl, :].astype(F32)
        inv = lax.rsqrt(jnp.mean(x_f * x_f, axis=1, keepdims=True) + 1e-6)
        out_ref[sl, :d_model] = (x_f * inv * (1.0 + scale_ref[...])).astype(BF16)
        out_ref[sl, d_model:] = g_ref[sl, :]


def norm_and_grad(x_loc, g_loc, scale_f):
    t_len, d_model = x_loc.shape
    rows = 512
    tile = pl.BlockSpec((rows, d_model), lambda i: (i, 0))
    return pl.pallas_call(
        norm_kernel, grid=(t_len // rows,), name='norm',
        in_specs=[tile, tile, pl.BlockSpec(scale_f.shape, lambda i: (0, 0))],
        out_specs=pl.BlockSpec((rows, 2 * d_model), lambda i: (i, 0)),
        out_shape=jax.ShapeDtypeStruct((t_len, 2 * d_model), BF16),
        cost_estimate=pl.CostEstimate(flops=4_000_000_000, bytes_accessed=19_000_000, transcendentals=2048),
    )(x_loc, g_loc, scale_f)


N_PART = 3


def split_kernel(w1_ref, w2_ref, keep_ref, send_ref):
    core = lax.axis_index('core')
    d_model = keep_ref.shape[2] // 2
    sub = d_model // 8
    for part in range(N_PART):
        for i, w_ref in enumerate((w1_ref, w2_ref)):
            even, odd = [
                jnp.concatenate([w_ref[:, ((2 * j + k) * N_PART + part) * sub:((2 * j + k) * N_PART + part + 1) * sub] for j in range(8)], axis=1).astype(BF16)
                for k in range(2)]

            @pl.when(core == 0)
            def _():
                keep_ref[part, :, i * d_model:(i + 1) * d_model] = even
                send_ref[part, :, i * d_model:(i + 1) * d_model] = odd

            @pl.when(core == 1)
            def _():
                keep_ref[part, :, i * d_model:(i + 1) * d_model] = odd
                send_ref[part, :, i * d_model:(i + 1) * d_model] = even


def split_up(w1, w2):
    rows, cols = w1.shape
    out = jax.ShapeDtypeStruct((N_PART, rows, cols // N_PART), BF16)
    return pl.pallas_call(split_kernel, out_shape=[out, out], name='split_up')(w1, w2)


def stack_kernel(keep_ref, recv_ref, wd_ref, extra_ref, first_ref, rest_ref):
    core = lax.axis_index('core')
    rows, cols = keep_ref.shape[1:]
    d_model = wd_ref.shape[1]
    own = pl.multiple_of(core * rows, 8)
    oth = pl.multiple_of(rows - own, 8)
    for part in range(N_PART):
        out_ref, base = (first_ref, 0) if part == 0 else (rest_ref, (part - 1) * (cols + d_model))
        out_ref[pl.ds(own, rows), base:base + cols] = keep_ref[part]
        out_ref[pl.ds(oth, rows), base:base + cols] = recv_ref[part]
        out_ref[:, base + cols:base + cols + d_model] = wd_ref[part * 2 * rows:(part + 1) * 2 * rows, :].astype(BF16)
    n_extra = extra_ref.shape[0]
    first_ref[:n_extra, cols + d_model:] = extra_ref[...]
    first_ref[n_extra:, cols + d_model:] = jnp.zeros((2 * rows - n_extra, extra_ref.shape[1]), BF16)


def stack_up(keep, recv, w_down, extra):
    _, rows, cols = keep.shape
    width = cols + w_down.shape[1]
    outs = [jax.ShapeDtypeStruct((2 * rows, width + extra.shape[1]), BF16), jax.ShapeDtypeStruct((2 * rows, (N_PART - 1) * width), BF16)]
    return pl.pallas_call(stack_kernel, out_shape=outs, name='stack_up')(keep, recv, w_down, extra)


def unpack_kernel(own_ref, oth_ref, wqkv_ref, wo_ref):
    core = lax.axis_index('core')
    r_o, r_in = wo_ref.shape[0] // 16, wqkv_ref.shape[0] // 16
    d_model = wo_ref.shape[1]
    rows = own_ref.shape[0] // 8
    for chip in range(8):
        for flip, ref in enumerate((own_ref, oth_ref)):
            dev = 2 * chip + (core ^ flip)
            wo_ref[pl.ds(pl.multiple_of(dev * r_o, 8), r_o), :] = ref[chip * rows:chip * rows + r_o, :d_model]
            wqkv_ref[pl.ds(pl.multiple_of(dev * r_in, 8), r_in), :] = ref[chip * rows + r_o:chip * rows + r_o + r_in, :]


def unpack(own, oth, r_o, r_in, d_model):
    return pl.pallas_call(
        unpack_kernel, name='unpack',
        out_shape=[jax.ShapeDtypeStruct((16 * r_in, own.shape[1]), BF16), jax.ShapeDtypeStruct((16 * r_o, d_model), BF16)],
    )(own, oth)


def join_kernel(*refs):
    own_refs, recv_refs, (w1_ref, w2_ref) = refs[:N_PART], refs[N_PART:2 * N_PART], refs[2 * N_PART:]
    core = lax.axis_index('core')
    rows = w1_ref.shape[0]
    d_model = recv_refs[0].shape[1] // 2
    sub = d_model // 8

    def put(even_of, odd_of):
        for i, w_ref in enumerate((w1_ref, w2_ref)):
            pieces = []
            for j in range(8):
                for of in (even_of, odd_of):
                    for part in range(N_PART):
                        pieces.append(of(part)[:, i * d_model + j * sub:i * d_model + (j + 1) * sub])
            w_ref[...] = jnp.concatenate(pieces, axis=1)

    pl.when(core == 0)(lambda: put(lambda p: own_refs[p][:rows, :2 * d_model], lambda p: recv_refs[p][...]))
    pl.when(core == 1)(lambda: put(lambda p: recv_refs[p][...], lambda p: own_refs[p][rows:, :2 * d_model]))


def join_up(owns, recvs):
    rows, cols = recvs[0].shape
    up = jax.ShapeDtypeStruct((rows, N_PART * cols), F32)
    first_cols = pl.BlockSpec((2 * rows, cols), lambda i: (0, 0))
    whole = lambda width: pl.BlockSpec((rows, width), lambda i: (0, 0))
    return pl.pallas_call(
        join_kernel, out_shape=[up, up], name='join_up', grid=(1,),
        in_specs=[first_cols] * N_PART + [whole(cols)] * N_PART, out_specs=[whole(N_PART * cols)] * 2,
    )(*owns, *recvs)


GELU_C = 0.7978845608028654
GELU_A = 0.044715


def hidden_kernel(own_ref, oth_ref, w_ref, b1_ref, b2_ref, *refs):
    extra_refs = refs[:-10]
    act_ref, dh_ref, dw_ref, db_ref, h_s, da_s, ng_s, acc_s, side_s, sems = refs[-10:]
    step = pl.program_id(0)
    last = pl.num_programs(0) - 1
    rows, d_model = da_s.shape
    own = step < pl.num_programs(0) // 2
    ng_s[...] = jnp.where(own, own_ref[...], oth_ref[...])

    @pl.when(step == 0)
    def _():
        acc_s[...] = jnp.zeros_like(acc_s)
        db_ref[...] = jnp.zeros_like(db_ref)

    n_sub = 2
    sub = rows // n_sub
    w12 = w_ref[:, :2 * d_model]
    for i in range(n_sub):
        sl = slice(i * sub, (i + 1) * sub)
        h_s[sl, :] = dot_nn(ng_s[sl, :d_model], w12)
        da_s[sl, :] = dot_nt(ng_s[sl, d_model:], w_ref[:, 2 * d_model:])
    b1 = b1_ref[...]
    b2 = b2_ref[...]
    for i in range(n_sub):
        sl = slice(i * sub, (i + 1) * sub)
        s1 = None
        s2 = None
        for r in range(i * sub, (i + 1) * sub, 64):
            rs = slice(r, r + 64)
            u = h_s[rs, :d_model] + b1
            v = h_s[rs, d_model:] + b2
            da = da_s[rs, :]
            u2 = u * u
            t = jnp.tanh(u * (GELU_C + (GELU_C * GELU_A) * u2))
            half = 0.5 + 0.5 * t
            gelu = u * half
            slope = half + (half * (1.0 - t)) * (u * (GELU_C + (3.0 * GELU_C * GELU_A) * u2))
            d1 = da * v * slope
            d2 = da * gelu
            act_ref[rs, :] = (gelu * v).astype(BF16)
            dh_ref[rs, :d_model] = d1.astype(BF16)
            dh_ref[rs, d_model:] = d2.astype(BF16)
            p1 = jnp.sum(d1.reshape(8, 8, d_model), axis=0)
            p2 = jnp.sum(d2.reshape(8, 8, d_model), axis=0)
            s1 = p1 if s1 is None else s1 + p1
            s2 = p2 if s2 is None else s2 + p2
        db_ref[:8, :] += s1
        db_ref[8:, :] += s2
        acc_s[:, :2 * d_model] += dot_tn(ng_s[sl, :d_model], dh_ref[sl, :])
        acc_s[:, 2 * d_model:] += dot_tn(act_ref[sl, :], ng_s[sl, d_model:])

    if extra_refs:
        keep_ref, got_ref = extra_refs
        block = side_s.shape[1]
        n_extra = keep_ref.shape[1]
        slot = lax.rem(step, 2)

        def side_copy(at_slot, at_step):
            place = dw_ref.at[pl.ds(pl.multiple_of(at_step * block, 8), block), 3 * d_model:]
            return pltpu.make_async_copy(side_s.at[at_slot], place, sems.at[1 + at_slot])

        @pl.when(step >= 2)
        def _():
            side_copy(slot, step - 2).wait()

        side_s[slot, :n_extra, :] = keep_ref[0] + got_ref[0]
        side_s[slot, n_extra:, :] = jnp.zeros((block - n_extra, keep_ref.shape[2]), F32)
        side_copy(slot, step).start()

        @pl.when(step == last)
        def _():
            side_copy(1 - slot, step - 1).wait()
            side_copy(slot, step).wait()

    @pl.when(step == last)
    def _():
        copy = pltpu.make_async_copy(acc_s, dw_ref.at[:, :3 * d_model], sems.at[0])
        copy.start()
        copy.wait()


def hidden_part(ng_own, ng_oth, weight, b1, b2, extra=()):
    w_part, w_col = weight
    t_len, both = ng_own.shape
    d_model = both // 2
    rows = 512
    steps = 2 * t_len // rows
    half = steps // 2
    own_spec = pl.BlockSpec((rows, both), lambda i: (jnp.minimum(i, half - 1), 0))
    oth_spec = pl.BlockSpec((rows, both), lambda i: (jnp.maximum(i - half, 0), 0))
    full = lambda a, width, col=0: pl.BlockSpec((a.shape[0], width), lambda i: (0, col), pipeline_mode=pl.Buffered(1))
    row = lambda width: pl.BlockSpec((rows, width), lambda i: (i, 0))
    blk = [pl.BlockSpec((1,) + a.shape[1:], lambda i: (i, 0, 0)) for a in extra]
    side = (2, d_model // 8, extra[0].shape[2]) if extra else (2, 8, 128)
    return pl.pallas_call(
        hidden_kernel,
        grid=(steps,),
        in_specs=[own_spec, oth_spec, full(w_part, 3 * d_model, w_col), full(b1, d_model), full(b2, d_model)] + blk,
        out_specs=[row(d_model), row(2 * d_model), pl.BlockSpec(memory_space=pl.ANY), pl.BlockSpec((16, d_model), lambda i: (0, 0))],
        out_shape=[jax.ShapeDtypeStruct((2 * t_len, d_model), BF16), jax.ShapeDtypeStruct((2 * t_len, 2 * d_model), BF16),
                   jax.ShapeDtypeStruct((d_model, 3 * d_model + (extra[0].shape[2] if extra else 0)), F32), jax.ShapeDtypeStruct((16, d_model), F32)],
        scratch_shapes=[pltpu.VMEM((rows, 2 * d_model), F32), pltpu.VMEM((rows, d_model), F32), pltpu.VMEM((rows, both), BF16),
                        pltpu.VMEM((d_model, 3 * d_model), F32), pltpu.VMEM(side, F32), pltpu.SemaphoreType.DMA((3,))],
        compiler_params=pltpu.CompilerParams(vmem_limit_bytes=63 * 1024 * 1024, dimension_semantics=('arbitrary',)),
        cost_estimate=pl.CostEstimate(flops=65_000_000_000, bytes_accessed=70_000_000, transcendentals=4_700_000),
        name='hidden',
    )(ng_own, ng_oth, w_part, b1, b2, *extra)


def attn_grad_kernel(cp_ref, own_ref, n1_ref, n2_ref, n3_ref, g1_ref, g2_ref, g3_ref, dqkv_ref, o_lo_ref, o_hi_ref, keep_ref, send_ref):
    step = pl.program_id(0)
    core = lax.axis_index('core')
    d_model = own_ref.shape[2] // 2
    r_o, r_in = o_lo_ref.shape[1] // 8, d_model // 16
    width = dqkv_ref.shape[1]
    rows = own_ref.shape[1]
    place = [pl.ds(pl.multiple_of((cp_ref[0] ^ flip) * rows, rows), rows) for flip in range(4)]

    def put(at, cols, value_of):
        for dev in range(16):
            for ref, flip in ((keep_ref, 0), (send_ref, 1)):
                @pl.when((core ^ flip) == dev % 2)
                def _():
                    ref[dev // 2, at, cols] = value_of(dev)

    d_wqkv = dot_tn(own_ref[0, :, :d_model], dqkv_ref[place[0], :])
    for flip, n_ref in ((1, n1_ref), (2, n2_ref), (3, n3_ref)):
        d_wqkv = d_wqkv + dot_tn(n_ref[0], dqkv_ref[place[flip], :])
    put(slice(r_o, r_o + r_in), slice(0, width), lambda dev: d_wqkv[dev * r_in:(dev + 1) * r_in])

    def low(first_col, used):
        d_wo = []
        for o_ref in (o_lo_ref, o_hi_ref):
            total = dot_tn(o_ref[place[0], :], own_ref[0, :, d_model + first_col:d_model + first_col + used])
            for flip, g_ref in ((1, g1_ref), (2, g2_ref), (3, g3_ref)):
                total = total + dot_tn(o_ref[place[flip], :], g_ref[0, :, first_col:first_col + used])
            d_wo.append(total)
        put(slice(0, r_o), slice(0, used), lambda dev: d_wo[dev // 8][dev % 8 * r_o:(dev % 8 + 1) * r_o])
        if used < width:
            put(slice(0, r_o), slice(used, width), lambda dev: jnp.zeros((r_o, width - used), F32))

    for i in range(-(-d_model // width)):
        pl.when(step == i)(functools.partial(low, i * width, min(width, d_model - i * width)))


def attn_grad(cp_index, ng_blocks, n_got, g_got, od_seq, r_o, r_in):
    _, rows, both = ng_blocks.shape
    t_len = od_seq.shape[0]
    width = 512
    total = (N_HEADS + 2) * HEAD_DIM
    out = jax.ShapeDtypeStruct((8, r_o + r_in, total), F32)
    out_spec = pl.BlockSpec((8, r_o + r_in, width), lambda i, cp: (0, 0, i))
    one = pl.Buffered(1)
    full = lambda a: pl.BlockSpec(a.shape, lambda i, cp: (0, 0, 0), pipeline_mode=one)
    return pl.pallas_call(
        attn_grad_kernel,
        grid_spec=pltpu.PrefetchScalarGridSpec(
            num_scalar_prefetch=1,
            grid=(total // width,),
            in_specs=[pl.BlockSpec((1, rows, both), lambda i, cp: (cp[0], 0, 0), pipeline_mode=one)] + [full(a) for a in n_got + g_got]
                     + [pl.BlockSpec((t_len, width), lambda i, cp: (0, i)),
                        pl.BlockSpec((t_len, width), lambda i, cp: (0, total // width), pipeline_mode=one),
                        pl.BlockSpec((t_len, width), lambda i, cp: (0, total // width + 1), pipeline_mode=one)],
            out_specs=[out_spec, out_spec]),
        out_shape=[out, out],
        compiler_params=pltpu.CompilerParams(vmem_limit_bytes=60 * 1024 * 1024, dimension_semantics=('arbitrary',)),
        cost_estimate=pl.CostEstimate(flops=12_000_000_000, bytes_accessed=33_000_000, transcendentals=0),
        name='attn_grad',
    )(cp_index[None], ng_blocks, *n_got, *g_got, od_seq, od_seq, od_seq)


def small_kernel(in_ref, out_ref, got_s, send_sems, recv_sems):
    at = [lax.axis_index(axis) for axis in ALL_AXES]
    me = ((at[0] * 2 + at[1]) * 2 + at[2]) * 2 + at[3]

    def peer(flip):
        return tuple(index ^ ((flip >> (3 - i)) & 1) for i, index in enumerate(at))

    barrier = pltpu.get_barrier_semaphore()
    for flip in range(1, 16):
        pl.semaphore_signal(barrier, inc=1, device_id=peer(flip), device_id_type=pl.DeviceIdType.MESH)
    pl.semaphore_wait(barrier, 15)
    copies = []
    for flip in range(1, 16):
        copies.append(pltpu.make_async_remote_copy(
            src_ref=in_ref.at[me ^ flip], dst_ref=got_s.at[flip], send_sem=send_sems.at[flip], recv_sem=recv_sems.at[flip],
            device_id=peer(flip), device_id_type=pl.DeviceIdType.MESH))
        copies[-1].start()
    for copy in copies:
        copy.wait()
    total = in_ref[me]
    for flip in range(1, 16):
        total = total + got_s[flip]
    out_ref[...] = total


def small_sum(values):
    return pl.pallas_call(
        small_kernel, out_shape=jax.ShapeDtypeStruct(values.shape[1:], F32), name='small_sum',
        in_specs=[pl.BlockSpec(memory_space=pltpu.VMEM)], out_specs=pl.BlockSpec(memory_space=pltpu.VMEM),
        scratch_shapes=[pltpu.VMEM(values.shape, F32), pltpu.SemaphoreType.DMA((16,)), pltpu.SemaphoreType.DMA((16,))],
        compiler_params=pltpu.CompilerParams(collective_id=0, has_side_effects=True),
        cost_estimate=pl.CostEstimate(flops=8_000_000_000, bytes_accessed=130_000, transcendentals=0),
    )(values)


def fwd_product(act_refs, w_refs):
    out = dot_nn(act_refs[0][...], w_refs[0][...])
    for act_ref, w_ref in zip(act_refs[1:], w_refs[1:]):
        out = out + dot_nn(act_ref[...], w_ref[...])
    return out


def bwd_product(dh_refs, w_refs):
    out = dot_nt(dh_refs[0][...], w_refs[0][:, :dh_refs[0].shape[1]])
    for dh_ref, w_ref in zip(dh_refs[1:], w_refs[1:]):
        out = out + dot_nt(dh_ref[...], w_ref[:, :dh_ref.shape[1]])
    return out


def other_kernel(product, *refs):
    refs[-1][...] = product(refs[:N_PART], refs[N_PART:2 * N_PART])


OUT_ROWS = 256


def out_specs_of(width, weights, w_width, w_off, first_block):
    tile = pl.BlockSpec((OUT_ROWS, width), lambda i, *_: (i + first_block, 0))
    specs = [tile] * N_PART
    for array, col in weights:
        specs.append(pl.BlockSpec((array.shape[0], w_width), lambda i, *_, at=w_off(col): (0, at), pipeline_mode=pl.Buffered(1)))
    return specs


def out_other(parts, weights, product, w_width, w_off):
    t_len, width = parts[0].shape[0] // 2, parts[0].shape[1]
    d_model = weights[0][0].shape[0]
    return pl.pallas_call(
        functools.partial(other_kernel, product),
        grid=(t_len // OUT_ROWS,),
        in_specs=out_specs_of(width, weights, w_width, w_off, t_len // OUT_ROWS),
        out_specs=pl.BlockSpec((OUT_ROWS, d_model), lambda i: (i, 0)),
        out_shape=jax.ShapeDtypeStruct((t_len, d_model), F32),
        compiler_params=pltpu.CompilerParams(vmem_limit_bytes=60 * 1024 * 1024, dimension_semantics=('arbitrary',)),
        cost_estimate=pl.CostEstimate(flops=2 * t_len * d_model * width * N_PART, bytes_accessed=50_000_000, transcendentals=0),
    )(*parts, *[array for array, _ in weights])


def fwd_own_kernel(cp_ref, *refs):
    o_refs = refs[2 * N_PART:2 * N_PART + 8]
    wo_ref, x_ref, got_ref, bias_ref, out_ref, o_s = refs[2 * N_PART + 8:]
    flip = (pl.program_id(0) // 2) ^ cp_ref[0]
    half = o_s.shape[1] // 2
    for i in range(4):
        @pl.when(flip == i)
        def _():
            o_s[:, :half] = o_refs[2 * i][0]
            o_s[:, half:] = o_refs[2 * i + 1][0]
    out = fwd_product(refs[:N_PART], refs[N_PART:2 * N_PART]) + dot_nn(o_s[...], wo_ref[...])
    out_ref[...] = (x_ref[...].astype(F32) + out + got_ref[...] + bias_ref[...]).astype(BF16)


def bwd_own_kernel(cp_ref, *refs):
    d_refs = refs[2 * N_PART:2 * N_PART + 4]
    wqkv_ref, x_ref, g_ref, got_ref, scale_ref, d_x_ref, sums_ref, d_s = refs[2 * N_PART + 4:]
    flip = (pl.program_id(0) // 2) ^ cp_ref[0]
    for i in range(4):
        @pl.when(flip == i)
        def _():
            d_s[...] = d_refs[i][0]

    @pl.when(pl.program_id(0) == 0)
    def _():
        sums_ref[...] = jnp.zeros_like(sums_ref)

    d_n = bwd_product(refs[:N_PART], refs[N_PART:2 * N_PART]) + dot_nt(d_s[...], wqkv_ref[...]) + got_ref[...]
    x_f = x_ref[...].astype(F32)
    g_f = g_ref[...].astype(F32)
    inv = lax.rsqrt(jnp.mean(x_f * x_f, axis=1, keepdims=True) + 1e-6)
    scaled = d_n * (1.0 + scale_ref[...])
    xn = x_f * inv
    proj = jnp.mean(scaled * xn, axis=1, keepdims=True)
    d_x_ref[...] = (g_f + inv * (scaled - xn * proj)).astype(BF16)
    rows, d_model = x_f.shape
    sums_ref[:8, :] += jnp.sum((d_n * xn).reshape(rows // 8, 8, d_model), axis=0)
    sums_ref[8:, :] += jnp.sum(g_f.reshape(rows // 8, 8, d_model), axis=0)


def own_call(kernel, cp_index, parts, weights, w_width, w_off, od_blocks, od_got, od_cols, od_width, rest, rest_specs, out_specs, out_shape, scratch):
    t_len, width = parts[0].shape[0] // 2, parts[0].shape[1]
    specs = out_specs_of(width, weights, w_width, w_off, 0)
    args = list(parts) + [array for array, _ in weights]
    for i, source in enumerate([od_blocks] + od_got):
        for col in od_cols:
            if i == 0:
                specs.append(pl.BlockSpec((1, OUT_ROWS, od_width), lambda j, cp, col=col: (cp[0], jnp.clip(j - 2 * cp[0], 0, 1), col)))
            else:
                specs.append(pl.BlockSpec((1, OUT_ROWS, od_width), lambda j, cp, col=col, i=i: (0, jnp.clip(j - 2 * (cp[0] ^ i), 0, 1), col)))
            args.append(source)
    return pl.pallas_call(
        kernel,
        grid_spec=pltpu.PrefetchScalarGridSpec(
            num_scalar_prefetch=1, grid=(t_len // OUT_ROWS,), in_specs=specs + rest_specs, out_specs=out_specs, scratch_shapes=scratch),
        out_shape=out_shape,
        compiler_params=pltpu.CompilerParams(vmem_limit_bytes=62 * 1024 * 1024, dimension_semantics=('arbitrary',)),
        cost_estimate=pl.CostEstimate(flops=2 * t_len * weights[0][0].shape[0] * (width * N_PART + 1024), bytes_accessed=80_000_000, transcendentals=0),
    )(cp_index[None], *args, *rest)


def pack_kernel(wq_ref, wk_ref, wv_ref, wo_ref, out_ref):
    r_o, d_model = wo_ref.shape
    qk = wq_ref.shape[1]
    out_ref[:r_o, :d_model] = wo_ref[...].astype(BF16)
    out_ref[:r_o, d_model:] = jnp.zeros((r_o, out_ref.shape[1] - d_model), BF16)
    out_ref[r_o:, :qk] = wq_ref[...].astype(BF16)
    out_ref[r_o:, qk:qk + HEAD_DIM] = wk_ref[...].astype(BF16)
    out_ref[r_o:, qk + HEAD_DIM:] = wv_ref[...].astype(BF16)


def pack(w_q, w_k, w_v, w_o):
    out = jax.ShapeDtypeStruct((w_o.shape[0] + w_q.shape[0], w_q.shape[1] + 2 * HEAD_DIM), BF16)
    return pl.pallas_call(pack_kernel, out_shape=out, name='pack')(w_q, w_k, w_v, w_o)


def vector_kernel(scale_ref, bo_ref, bd_ref, b1_ref, b2_ref, out_ref, side_s):
    side_s[...] = jnp.zeros_like(side_s)
    for row, ref in enumerate((scale_ref, bo_ref, bd_ref, b1_ref, b2_ref)):
        side_s[row:row + 1, :ref.shape[1]] = ref[...]
    out_ref[...] = side_s[...].astype(BF16)


def vectors(*parts):
    width = -(-max(part.shape[0] for part in parts) // 128) * 128
    return pl.pallas_call(
        vector_kernel, out_shape=jax.ShapeDtypeStruct((8, width), BF16), scratch_shapes=[pltpu.VMEM((8, width), F32)], name='vectors',
    )(*[part[None] for part in parts])


def solution(mesh):
    mesh4 = Mesh(mesh.devices.reshape(2, 2, 2, 2), ALL_AXES)
    tok_spec = P(('x', 'core'), ('z', 'y'), None)
    pos_spec = P(('x', 'core'), ('z', 'y'))
    vec_spec = P(ALL_AXES)
    mat_spec = P(ALL_AXES, None)
    param_specs = (vec_spec, mat_spec, mat_spec, mat_spec, mat_spec, vec_spec, mat_spec, vec_spec, mat_spec, vec_spec, mat_spec, vec_spec)

    def swap_core(values):
        return lax.ppermute(values, 'core', [(0, 1), (1, 0)])

    def after(value, *deps):
        return lax.optimization_barrier((value,) + deps)[0]

    def send_blocks(values, cp_index, width=None):
        got = []
        for flip in (1, 2, 3):
            sent = lax.dynamic_index_in_dim(values, cp_index ^ flip, 0, keepdims=True)[..., :width]
            got.append(lax.ppermute(sent, ('z', 'y'), [(i, i ^ flip) for i in range(4)]))
        return got

    def local_step(x_in, grad_out, seg_id, seg_pos, norm_scale, w_q, w_k, w_v, w_o, b_o, w_up1, b_up1, w_up2, b_up2, w_down, b_down):
        n_seq, piece, d_model = x_in.shape
        t_len = n_seq * piece
        core = lax.axis_index('core')
        cp_index = lax.axis_index('z') * 2 + lax.axis_index('y')
        first = core == 0
        r_in = w_q.shape[0]
        r_o = w_o.shape[0]
        f_blk = b_up1.shape[0]
        sub = f_blk // N_PART
        qk = N_HEADS * HEAD_DIM

        seg_pack = jnp.stack([seg_id, seg_pos], axis=1)
        seg_got = send_blocks(seg_pack, cp_index)
        g_got = send_blocks(grad_out, cp_index)

        keep, send = split_up(w_up1, w_up2)
        shards = stack_up(keep, swap_core(send), w_down, pack(w_q, w_k, w_v, w_o))

        def gather(shard):
            return lax.all_gather(shard, CHIPS, axis=0, tiled=True)

        whole = [gather(shards[0]), gather(shards[1])]
        weights = [(whole[0], 0), (whole[1], 0), (whole[1], 1)]

        vec_all = lax.all_gather(vectors(norm_scale, b_o, b_down, b_up1, b_up2), ALL_AXES, axis=0)
        scale_f, bo_f, bd_f = [vec_all[:, i, :r_in].reshape(1, d_model).astype(F32) for i in range(3)]
        b_ups = []
        for row in (3, 4):
            both = vec_all[:, row, :f_blk].reshape(8, 2, N_PART, sub)
            mine = jnp.where(first, both[:, 0], both[:, 1]).astype(F32)
            b_ups.append([mine[:, part].reshape(1, d_model) for part in range(N_PART)])

        x_loc = x_in.reshape(t_len, d_model)
        ng_own = norm_and_grad(x_loc, grad_out.reshape(t_len, d_model), scale_f)
        ng_oth = swap_core(ng_own)
        ng_blocks = ng_own.reshape(n_seq, piece, 2 * d_model)
        n_got = send_blocks(ng_blocks, cp_index, d_model)

        seg_all = jnp.zeros_like(seg_pack)
        for flip, got in enumerate([lax.dynamic_index_in_dim(seg_pack, cp_index, 0, keepdims=True)] + seg_got):
            seg_all = lax.dynamic_update_slice_in_dim(seg_all, got, cp_index ^ flip, 0)
        seg_own = seg_all[:, 0].reshape(t_len)
        pos_own = seg_all[:, 1].reshape(t_len)
        half = ROPE_DIMS // 2
        inv_freq = 10000.0 ** (-jnp.arange(half, dtype=F32) / half)
        angle = pos_own.astype(F32)[:, None] * inv_freq
        cos_a = jnp.cos(angle)
        sin_a = jnp.sin(angle)
        cos_b = jnp.concatenate([cos_a, cos_a], axis=1)
        sin_b = jnp.concatenate([-sin_a, sin_a], axis=1)

        acts, dhs, dbs, owns, recvs = [], [], [], [], []

        def third(part, ng_in, extra=()):
            act, dh, d_w, db = hidden_part(ng_in, ng_oth, weights[part], b_ups[0][part], b_ups[1][part], extra)
            own = lax.psum_scatter(d_w, CHIPS, scatter_dimension=0, tiled=True)
            recvs.append(swap_core(jnp.where(first, own[r_in:, :2 * d_model], own[:r_in, :2 * d_model])))
            acts.append(act)
            dhs.append(dh)
            dbs.append(jnp.sum(db.reshape(2, 8, d_model), axis=1).reshape(2, 8, sub))
            owns.append(own)

        third(0, ng_own)
        extra_own = whole[0][:, 3 * d_model:]
        wqkv, wo = unpack(extra_own, swap_core(extra_own), r_o, r_in, d_model)
        od_seq = attention(cp_index, ng_blocks, n_got, g_got, wqkv, wo, cos_b, sin_b, seg_own)
        d_keep, d_send = attn_grad(cp_index, ng_blocks, n_got, g_got, od_seq, r_o, r_in)
        od_blocks = od_seq.reshape(n_seq, piece, -1)
        od_got = send_blocks(od_blocks, cp_index)
        third(1, ng_own, (d_keep, swap_core(d_send)))
        third(2, ng_own)

        wd_off = lambda col: 3 * col + 2
        w12_off = lambda col: col
        tile = lambda width, col=0: pl.BlockSpec((OUT_ROWS, width), lambda i, *_: (i, col))
        full = lambda a: pl.BlockSpec(a.shape, lambda i, *_: (0, 0), pipeline_mode=pl.Buffered(1))
        out_oth = out_other(acts, weights, fwd_product, d_model, wd_off)
        dn_oth = out_other(after(tuple(dhs), out_oth), weights, bwd_product, 3 * d_model, w12_off)
        bias_f = bo_f + bd_f
        x_out = own_call(fwd_own_kernel, cp_index, after(tuple(acts), dn_oth), weights, d_model, wd_off, od_blocks, od_got, (3, 4), 512,
                         [wo, x_loc, swap_core(out_oth), bias_f], [full(wo), tile(d_model), tile(d_model), full(bias_f)],
                         tile(d_model), jax.ShapeDtypeStruct((t_len, d_model), BF16), [pltpu.VMEM((OUT_ROWS, qk), BF16)])
        d_x, sums = own_call(bwd_own_kernel, cp_index, after(tuple(dhs), x_out), weights, 3 * d_model, w12_off, od_blocks, od_got, (0,), qk + 2 * HEAD_DIM,
                             [wqkv, x_loc, ng_own, swap_core(dn_oth), scale_f],
                             [full(wqkv), tile(d_model), tile(d_model, 1), tile(d_model), full(scale_f)],
                             [tile(d_model), pl.BlockSpec((16, d_model), lambda i, *_: (0, 0))],
                             [jax.ShapeDtypeStruct((t_len, d_model), BF16), jax.ShapeDtypeStruct((16, d_model), F32)],
                             [pltpu.VMEM((OUT_ROWS, qk + 2 * HEAD_DIM), BF16)])
        x_out = x_out.reshape(n_seq, piece, d_model)
        d_x = d_x.reshape(n_seq, piece, d_model)

        sums = jnp.sum(sums.reshape(2, 8, d_model), axis=1).reshape(2, 16, r_in)
        db = jnp.stack(dbs, axis=2).reshape(2, 8, f_blk)
        zero = jnp.zeros_like(db)
        db = jnp.where(first, jnp.stack([db, zero], axis=2), jnp.stack([zero, db], axis=2)).reshape(2, 16, f_blk)
        small = jnp.concatenate([sums[0], sums[1], db[0], db[1]], axis=1)
        small = jnp.pad(small, ((0, 0), (0, 1024 - small.shape[1]))).reshape(16, 8, 128)
        small = small_sum(small).reshape(1024)
        g_scale, g_bias, g_b1, g_b2 = small[:r_in], small[r_in:2 * r_in], small[2 * r_in:2 * r_in + f_blk], small[2 * r_in + f_blk:2 * r_in + 2 * f_blk]

        g_w1, g_w2 = join_up(owns, recvs)
        g_wd = jnp.concatenate([own[:, 2 * d_model:3 * d_model] for own in owns], axis=0)
        g_attn = owns[1][:r_o + r_in, 3 * d_model:]
        g_wo, g_wq, g_wk, g_wv = g_attn[:r_o, :d_model], g_attn[r_o:, :qk], g_attn[r_o:, qk:qk + HEAD_DIM], g_attn[r_o:, qk + HEAD_DIM:]
        return (x_out, d_x, g_scale, g_wq, g_wk, g_wv, g_wo, g_bias, g_w1, g_b1, g_w2, g_b2, g_wd, g_bias)

    in_specs = (tok_spec, tok_spec, pos_spec, pos_spec) + param_specs
    out_specs = (tok_spec, tok_spec) + param_specs
    return jax.shard_map(local_step, mesh=mesh4, in_specs=in_specs, out_specs=out_specs, check_vma=False)
```
